256 devices in a mesh: depth: 8 (over z), col: 4 (over y), row: 8 (over x, core).
Axes of the slice: x: 4, y: 4, z: 8, core: 2. Of those that a mesh axis runs over, the one named last changes fastest.
Arguments:
- tokens: bfloat16 [32768, 3072], P(('depth', 'row'), 'col')
- w_up: bfloat16 [3072, 8192], P('row', 'col')
- w_down: bfloat16 [8192, 3072], P('row', 'col')
- grad_out: bfloat16 [32768, 3072], P(('depth', 'row'), 'col')
Outputs:
- output 1: bfloat16 [32768, 3072], P(('depth', 'row'), 'col')
- output 2: bfloat16 [32768, 3072], P(('depth', 'row'), 'col')
- output 3: float32 [3072, 8192], P('row', 'col')
- output 4: float32 [8192, 3072], P('row', 'col')
All inputs are finite; a program needn't handle non-finite values.
Results may differ from the reference program's by a relative error of at most 0.00114.
Values are sent between devices in bfloat16 or wider.
A program may use at most 768 MiB of HBM per device.

```python
import jax
import jax.numpy as jnp
from jax import lax

H = 3072
F = 8192
ROWS = 512
SHARDS = 64
TOKENS = ROWS * SHARDS


def gelu_fn(pre_act):
    return jax.nn.gelu(pre_act, approximate=True)


def setup_inputs(seed: int = 0) -> dict:
    root_key = jax.random.key(seed)
    key_tok, key_up, key_down, key_grad = jax.random.split(root_key, 4)
    tokens = jax.random.normal(key_tok, (TOKENS, H), jnp.float32)
    w_up = jax.random.normal(key_up, (H, F), jnp.float32) * H ** -0.5
    w_down = jax.random.normal(key_down, (F, H), jnp.float32) * F ** -0.5
    grad_out = jax.random.normal(key_grad, (TOKENS, H), jnp.float32)
    return {"tokens": tokens.astype(jnp.bfloat16), "w_up": w_up.astype(jnp.bfloat16), "w_down": w_down.astype(jnp.bfloat16), "grad_out": grad_out.astype(jnp.bfloat16)}


def reference(tokens, w_up, w_down, grad_out):
    tok_blocks = tokens.reshape(SHARDS, ROWS, H)
    grad_blocks = grad_out.reshape(SHARDS, ROWS, H)

    def shard_step(acc_pair, blocks):
        acc_up, acc_down = acc_pair
        tok_blk, grad_blk = blocks
        pre_act = jnp.dot(tok_blk, w_up, preferred_element_type=jnp.float32)
        hidden, gelu_vjp = jax.vjp(gelu_fn, pre_act)
        hidden = hidden.astype(jnp.bfloat16)
        out_blk = jnp.dot(hidden, w_down, preferred_element_type=jnp.float32).astype(jnp.bfloat16)
        d_hidden = jnp.dot(grad_blk, w_down.T, preferred_element_type=jnp.float32)
        d_pre = gelu_vjp(d_hidden)[0].astype(jnp.bfloat16)
        dx_blk = jnp.dot(d_pre, w_up.T, preferred_element_type=jnp.float32).astype(jnp.bfloat16)
        acc_up = acc_up + jnp.dot(tok_blk.T, d_pre, preferred_element_type=jnp.float32)
        acc_down = acc_down + jnp.dot(hidden.T, grad_blk, preferred_element_type=jnp.float32)
        return (acc_up, acc_down), (out_blk, dx_blk)

    init_pair = (jnp.zeros((H, F), jnp.float32), jnp.zeros((F, H), jnp.float32))
    (dw_up, dw_down), (out_blocks, dx_blocks) = lax.scan(shard_step, init_pair, (tok_blocks, grad_blocks))
    return out_blocks.reshape(TOKENS, H), dx_blocks.reshape(TOKENS, H), dw_up, dw_down
```

```python
import functools
import itertools

import jax
import jax.numpy as jnp
from jax import lax
from jax.experimental import pallas as pl
from jax.experimental.pallas import tpu as pltpu
from jax.sharding import PartitionSpec as P

MESH = pl.DeviceIdType.MESH
ANY = pl.BlockSpec(memory_space=pl.ANY)
F32 = jnp.float32
BF16 = jnp.bfloat16

CHUNKS_UP = [(0, 0, 1), (1, 3, 1), (0, 1, 1), (1, 4, 1), (0, 2, 1), (1, 5, 1)]
CHUNKS_DOWN_X = [(0, 0, 2), (1, 4, 2), (0, 2, 2), (1, 6, 2)]
CHUNKS_DOWN_Z = [(0, 8, 2), (1, 12, 2), (0, 10, 2), (1, 14, 2)]


def gelu_fn(pre_act):
    return jax.nn.gelu(pre_act, approximate=True)


class Plan:
    def __init__(self, rates, window):
        self.rates, self.window = rates, window
        self.tasks, self.size, self.link = [], {}, {}

    def msg(self, key, link, nbytes):
        self.size[key], self.link[key] = nbytes, link

    def task(self, prio, waits, sends, run, cost=0.3, stage=None):
        self.tasks.append((prio, tuple(waits), tuple(sends), run, cost, stage))

    def order(self):
        free, arrive, out = {}, {}, []
        now, left = 0.0, list(range(len(self.tasks)))
        while left:
            best = None
            for i in left:
                prio, waits, sends, _, _, _ = self.tasks[i]
                if any(w not in arrive for w in waits):
                    continue
                ready = max([arrive[w] for w in waits], default=0.0)
                if not waits:
                    ready = max([free.get(self.link[s], 0.0) - self.window for s in sends], default=0.0)
                key = (max(ready, now), prio, i)
                if best is None or key < best:
                    best = key
            at, _, i = best
            left.remove(i)
            out.append(i)
            now = at + self.tasks[i][4]
            for s in self.tasks[i][2]:
                rate, lat = self.rates[self.link[s][0]]
                done = max(now, free.get(self.link[s], 0.0)) + self.size[s] / rate
                free[self.link[s]] = done
                arrive[s] = done + lat
        self.end = max(now, max(arrive.values()))
        return out


RATES = {"x": (44e3, 2.5), "y": (44e3, 2.5), "z": (44e3, 2.5), "d": (300e3, 1.5), "t": (40e3, 5.0), "l": (1e12, 0.0)}
WINDOW = 8.0


class Comm:
    def __init__(self, plan, ssem, rsem):
        self.plan, self.ssem, self.rsem = plan, ssem, rsem
        self.make, self.slot, self.remote_if = {}, {}, {}

    def msg(self, key, link, src, dst, to):
        i = len(self.slot)
        self.slot[key] = i
        self.make[key] = lambda: pltpu.make_async_remote_copy(
            src_ref=src(), dst_ref=dst(), send_sem=self.ssem.at[i], recv_sem=self.rsem.at[i], device_id=to, device_id_type=MESH)
        shape = src().shape
        nbytes = functools.reduce(lambda a, b: a * b, shape, 1) * src().dtype.itemsize
        self.plan.msg(key, link, nbytes)

    def each(self, keys, act):
        for key in keys:
            if key not in self.make:
                continue
            if key in self.remote_if:
                pl.when(self.remote_if[key])(lambda key=key: act(self.make[key]()))
            else:
                act(self.make[key]())

    def start(self, *keys):
        self.each(keys, lambda copy: copy.start())

    def wait(self, *keys):
        self.each(keys, lambda copy: copy.wait_recv())

    def finish(self):
        self.each(list(self.make), lambda copy: copy.wait_send())


def where_am_i():
    z, y, r = lax.axis_index("depth"), lax.axis_index("col"), lax.axis_index("row")
    return z, y, lax.div(r, 2), lax.rem(r, 2)


def gather_kernel(dims, x_ref, g_ref, w1_ref, w2_ref, xf, gf, w1c, w2c, vx, vg, vw1, vw2, lsem, ssem, rsem):
    nz, ny, nx = dims
    z, y, x, c = where_am_i()
    tk, hb = x_ref.shape
    fc = w2_ref.shape[0]
    hr = hb // 2
    fz = fc // nz
    r = 2 * x + c

    def col(d):
        return {"col": lax.rem(y + d + ny, ny)}

    def row(d):
        return {"row": 2 * lax.rem(x + d + nx, nx) + c}

    def dep(d):
        return {"depth": lax.rem(z + d + nz, nz)}

    partner = {"row": 2 * x + (1 - c)}

    def target(t):
        return {"row": 2 * lax.rem(x + t, nx) + c, "col": x}

    loads = [
        pltpu.make_async_copy(w2_ref.at[pl.ds(z * fz, fz), :], vw2, lsem.at[0]),
        pltpu.make_async_copy(w1_ref, vw1, lsem.at[1]),
        pltpu.make_async_copy(x_ref, vx, lsem.at[2]),
        pltpu.make_async_copy(g_ref, vg, lsem.at[3]),
    ]
    for copy in loads:
        copy.start()

    barrier = pltpu.get_barrier_semaphore()

    def tell(to):
        pl.semaphore_signal(barrier, inc=1, device_id=to, device_id_type=MESH)

    for to in (col(1), col(-1), row(1), row(-1), dep(1), dep(-1), partner):
        tell(to)
    for b in range(1, ny):
        tell({"row": 2 * y + c, "col": lax.rem(y + b, ny)})

    @pl.when(x != y)
    def _():
        tell({"row": 2 * y + c, "col": y})

    pl.semaphore_wait(barrier, 10 + jnp.where(x != y, 1, 0))

    def xblock(full, k, lo, n):
        return full.at[pl.ds(c * tk + lo, n), pl.ds(pl.multiple_of(k * hb, hb), hb)]

    def wblock(k):
        return w1c.at[pl.ds(k * hr, hr), :]

    def wpiece(k, b):
        return w2c.at[pl.ds(k * fz, fz), pl.ds(pl.multiple_of(b * hb, hb), hb)]

    ym, yp, yo = lax.rem(y + ny - 1, ny), lax.rem(y + 1, ny), lax.rem(y + 2, ny)
    half = tk // 2
    started = []

    def send(i, src, dst, to):
        copy = pltpu.make_async_remote_copy(src_ref=src, dst_ref=dst, send_sem=ssem.at[i], recv_sem=rsem.at[i], device_id=to, device_id_type=MESH)
        copy.start()
        started.append(copy)

    def got(i, dst):
        pltpu.make_async_remote_copy(src_ref=dst, dst_ref=dst, send_sem=ssem.at[i], recv_sem=rsem.at[i], device_id=partner, device_id_type=MESH).wait_recv()

    def slice_copy(t):
        return pltpu.make_async_remote_copy(src_ref=vw2, dst_ref=wpiece(z, y), send_sem=ssem.at[t], recv_sem=rsem.at[y], device_id=target(t), device_id_type=MESH)

    loads[0].wait()
    for t in (1, 3, 2):
        slice_copy(t).start()

    @pl.when(x != y)
    def _():
        slice_copy(0).start()

    self_copy = pltpu.make_async_copy(vw2, wpiece(z, y), lsem.at[4])

    @pl.when(x == y)
    def _():
        self_copy.start()

    c0 = pl.multiple_of(c * fc, fc)
    c1 = pl.multiple_of((1 - c) * fc, fc)
    loads[1].wait()
    send(36, vw1.at[:, pl.ds(c1, fc)], wblock(r), partner)
    for i, d in ((37, 1), (38, -1)):
        send(i, vw1.at[:, pl.ds(c0, fc)], wblock(r), row(d))
    keep = [pltpu.make_async_copy(vw1.at[:, pl.ds(c0, fc)], wblock(r), lsem.at[5])]
    loads[2].wait()
    loads[3].wait()
    base = {0: 44, 1: 53}
    for a, (v, full) in enumerate(((vx, xf), (vg, gf))):
        send(base[a], v, xblock(full, y, 0, tk), col(1))
        send(base[a] + 1, v, xblock(full, y, 0, tk), col(-1))
    for a, (v, full) in enumerate(((vx, xf), (vg, gf))):
        send(base[a] + 4, v, xblock(full, y, 0, tk), partner)
        keep.append(pltpu.make_async_copy(v, xblock(full, y, 0, tk), lsem.at[6 + a]))
    for copy in keep:
        copy.start()

    rp = 2 * x + 1 - c
    got(36, wblock(rp))
    for i, d in ((39, 1), (40, -1)):
        send(i, wblock(rp), wblock(rp), row(d))

    def z_index(o, step, sign):
        return 4 + o * 8 + (step if sign > 0 else 4 + step)

    def z_send(o, step, sign):
        b = lax.rem(y + o, ny)
        k = lax.rem(z - sign * step + nz, nz)
        src = wpiece(k, b)
        send(z_index(o, step, sign), src, wpiece(k, b), dep(sign))

    def z_got(o, step, sign):
        b = lax.rem(y + o, ny)
        got(z_index(o, step, sign), wpiece(lax.rem(z - sign * (step + 1) + nz, nz), b))

    def z_steps(o, sign):
        return 4 if (sign > 0) == (o % 2 == 0) else 3

    def z_first(o):
        b = lax.rem(y + o, ny)
        if o == 0:
            @pl.when(x != y)
            def _():
                got(b, wpiece(z, b))

            @pl.when(x == y)
            def _():
                self_copy.wait()
        else:
            got(b, wpiece(z, b))
        for sign in (1, -1):
            z_send(o, 0, sign)

    def z_forward(step):
        for o in range(ny):
            for sign in (1, -1):
                if step < z_steps(o, sign):
                    z_got(o, step, sign)
                    if step + 1 < z_steps(o, sign):
                        z_send(o, step + 1, sign)

    def x_arrived(a, full):
        got(base[a], xblock(full, ym, 0, tk))
        send(base[a] + 2, xblock(full, ym, 0, half), xblock(full, ym, 0, half), col(1))
        got(base[a] + 1, xblock(full, yp, 0, tk))
        send(base[a] + 3, xblock(full, yp, half, half), xblock(full, yp, half, half), col(-1))
        send(base[a] + 5, xblock(full, ym, 0, tk), xblock(full, ym, 0, tk), partner)
        send(base[a] + 6, xblock(full, yp, 0, tk), xblock(full, yp, 0, tk), partner)

    def x_opposite(a, full):
        got(base[a] + 2, xblock(full, yo, 0, half))
        send(base[a] + 7, xblock(full, yo, 0, half), xblock(full, yo, 0, half), partner)
        got(base[a] + 3, xblock(full, yo, half, half))
        send(base[a] + 8, xblock(full, yo, half, half), xblock(full, yo, half, half), partner)

    z_first(0)
    z_first(1)
    z_first(3)
    z_first(2)
    x_arrived(0, xf)
    z_forward(0)
    xm, xp = lax.rem(x + nx - 1, nx), lax.rem(x + 1, nx)
    xo = lax.rem(x + 2, nx)
    got(37, wblock(2 * xm + c))
    send(41, wblock(2 * xm + c), wblock(2 * xm + c), row(1))
    got(38, wblock(2 * xp + c))
    x_arrived(1, gf)
    z_forward(1)
    x_opposite(0, xf)
    got(39, wblock(2 * xm + 1 - c))
    got(40, wblock(2 * xp + 1 - c))
    send(42, wblock(2 * xp + 1 - c), wblock(2 * xp + 1 - c), row(-1))
    z_forward(2)
    x_opposite(1, gf)
    got(41, wblock(2 * xo + c))
    got(42, wblock(2 * xo + 1 - c))
    z_forward(3)

    pc = 1 - c
    for a, full in ((0, xf), (1, gf)):
        def pblock(k, lo, n):
            return full.at[pl.ds(pc * tk + lo, n), pl.ds(pl.multiple_of(k * hb, hb), hb)]
        got(base[a] + 4, pblock(y, 0, tk))
        got(base[a] + 5, pblock(ym, 0, tk))
        got(base[a] + 6, pblock(yp, 0, tk))
        got(base[a] + 7, pblock(yo, 0, half))
        got(base[a] + 8, pblock(yo, half, half))
    for copy in keep:
        copy.wait()
    for copy in started:
        copy.wait_send()
    for t in (1, 3, 2):
        slice_copy(t).wait_send()

    @pl.when(x != y)
    def _():
        slice_copy(0).wait_send()


def gather(dims, tok, grad, up, down):
    tk, hb = tok.shape
    fc = down.shape[0]
    nz, ny, nx = dims
    return pl.pallas_call(
        functools.partial(gather_kernel, dims),
        out_shape=[
            jax.ShapeDtypeStruct((2 * tk, ny * hb), BF16),
            jax.ShapeDtypeStruct((2 * tk, ny * hb), BF16),
            jax.ShapeDtypeStruct((nx * hb, fc), BF16),
            jax.ShapeDtypeStruct((fc, ny * hb), BF16),
        ],
        in_specs=[ANY] * 4,
        out_specs=[ANY] * 4,
        scratch_shapes=[
            pltpu.VMEM((tk, hb), BF16),
            pltpu.VMEM((tk, hb), BF16),
            pltpu.VMEM(up.shape, BF16),
            pltpu.VMEM((fc // nz, hb), BF16),
            pltpu.SemaphoreType.DMA((8,)),
            pltpu.SemaphoreType.DMA((64,)),
            pltpu.SemaphoreType.DMA((64,)),
        ],
        compiler_params=pltpu.CompilerParams(collective_id=0, has_side_effects=True),
        name="gather",
    )(tok, grad, up, down)


def each(shape, fn):
    lead = shape[:-2]
    big = max(range(len(lead)), key=lambda d: lead[d])
    looped = lead[big] >= 8

    def rest(k):
        for ix in itertools.product(*[range(n) if not (looped and d == big) else (k,) for d, n in enumerate(lead)]):
            fn(ix)

    if looped:
        pl.loop(0, lead[big])(rest)
    else:
        rest(None)


def accumulate(dst, others):
    def one(ix):
        total = dst[ix]
        for o in others:
            total = total + o[ix]
        dst[ix] = total

    each(dst.shape, one)


def reduce_kernel(dims, yp, dxp, dw1, dw2, y_out, dx_out, dw1_out, dw2_out, *scratch):
    nz, ny, nx = dims
    z, y, x, c = where_am_i()
    fc = dw1.shape[-1]
    hb = y_out.shape[-1]
    sgn = (1, -1)
    scratch = list(scratch)

    def grab(n):
        return [scratch.pop(0) for _ in range(n)]

    n1, n2, n3 = len(CHUNKS_UP), len(CHUNKS_DOWN_X), len(CHUNKS_DOWN_Z)
    ux, uz, us = grab(n1), grab(n1), grab(n1)
    vx, vz, vt = grab(n2), grab(n2), grab(n2)
    wz, wx, wt = grab(n3), grab(n3), grab(n3)
    o1, o2, pair, yr, yo = grab(5)
    pools = grab(4)
    ssem, rsem, lsem, osem = grab(4)

    plan = Plan(RATES, WINDOW)
    comm = Comm(plan, ssem, rsem)

    def idx(axis, d):
        at, n = {"z": (z, nz), "y": (y, ny), "x": (x, nx)}[axis]
        return lax.rem(at + (d % n), n)

    def nb(axis, d):
        i = idx(axis, d)
        return {"z": {"depth": i}, "y": {"col": i}, "x": {"row": 2 * i + c}}[axis]

    partner = {"row": 2 * x + (1 - c)}
    across = {"row": 2 * y + c, "col": x}

    def hcol(j):
        return pl.ds(pl.multiple_of(j * hb, hb), hb)

    def fcol(h):
        return pl.ds(pl.multiple_of(h * fc, fc), fc)

    staged, stores = [], []

    def stage(pool, src):
        staged.append((pool, src))
        return len(staged) - 1

    def mark(key):
        plan.msg(key, ("l", key), 0)

    place = {}

    def slot(k):
        return place[k][0]

    def chain(key, axis, n, s, buf, src, pool, prio, end, end_sends, end_waits=()):
        far, near = n // 2, n // 2 - 1
        for t in range(far):
            comm.msg((key, "F", t), (axis, s), (lambda: src(far * s)) if t == 0 else (lambda t=t: buf.at[t - 1]), lambda t=t: buf.at[t], nb(axis, s))
        for t in range(near):
            comm.msg((key, "N", t), (axis, -s), (lambda: src(-near * s)) if t == 0 else (lambda t=t: buf.at[far + t - 1]), lambda t=t: buf.at[far + t], nb(axis, -s))

        def mid(name, t, at, rel, extra):
            k = None if pool is None else stage(pool, lambda: src(rel))

            def run():
                accumulate(buf.at[at], [src(rel) if k is None else slot(k)])
                comm.start((key, name, t + 1))

            plan.task(prio, [(key, name, t), *extra], [(key, name, t + 1)], run, stage=k)

        for t in range(far - 1):
            mid("F", t, t, (far - 1 - t) * s, end_waits[1:2] if end_waits else ())
        for t in range(near - 1):
            mid("N", t, far + t, -(near - 1 - t) * s, ())
        k = None if pool is None else stage(pool, lambda: src(0))
        last = [buf.at[far - 1], buf.at[far + near - 1]]
        plan.task(prio, [(key, "F", far - 1), (key, "N", near - 1), *end_waits[:1]], end_sends,
                  lambda: end(last, src(0) if k is None else slot(k)), stage=k)
        return [(key, "F", 0), (key, "N", 0)]

    def spread(key, s, region, store):
        far, near = nz // 2, nz // 2 - 1
        for name, count, d in (("GF", far, s), ("GN", near, -s)):
            for t in range(count):
                def ref(t=t, d=d):
                    return region(idx("z", -t * d))
                comm.msg((key, name, t), ("z", d), ref, ref, nb("z", d))
        for name, count in (("GF", far), ("GN", near)):
            for t in range(count - 1):
                plan.task(4, [(key, name, t)], [(key, name, t + 1)], lambda name=name, t=t: comm.start((key, name, t + 1)), 0.15)
        plan.task(30, [(key, "GF", far - 1), (key, "GN", near - 1)], [], store, 0.15)
        return [(key, "GF", 0), (key, "GN", 0)]

    def store(src, dst):
        copy = pltpu.make_async_copy(src, dst, osem.at[len(stores)])
        stores.append(copy)
        copy.start()

    for i, (sigma, q, n) in enumerate(CHUNKS_UP):
        s = sgn[sigma]
        res = ux[i].at[1]

        def region(k, q=q, n=n):
            return o1.at[k, pl.ds(q, n)]

        first = spread(("ug", i), s, region, lambda q=q, n=n: store(o1.at[:, pl.ds(q, n)], dw1_out.at[:, pl.ds(q, n)]))
        comm.msg(("sw", i), ("d", 0), lambda i=i: us[i], lambda q=q, n=n: o1.at[z, pl.ds(q, n), :, fcol(c)], partner)
        plan.task(3, [("sw", i)], first, lambda first=first: comm.start(*first))

        def z_end(last, own, i=i, q=q, n=n):
            for m in range(n):
                o1[z, q + m, :, fcol(c)] = own[c, m] + last[0][c, m] + last[1][c, m]
                us[i][m] = own[1 - c, m] + last[0][1 - c, m] + last[1][1 - c, m]
            comm.start(("sw", i))

        raws = chain(("uz", i), "z", nz, s, uz[i], lambda rel, res=res: res.at[:, idx("z", rel)], None, 5, z_end, [("sw", i)])

        def x_end(last, own, raws=raws):
            accumulate(last[0], [last[1], own])
            comm.start(*raws)

        raws = chain(("ux", i), "x", nx, s, ux[i], lambda rel, q=q, n=n: dw1.at[idx("x", rel), :, :, pl.ds(q, n)], 0, 10, x_end, raws)
        plan.task(20 + i, [], raws, lambda raws=raws: comm.start(*raws))

    def deliver(key, i, s, u, n, tb):
        def region(k):
            return o2.at[k, pl.ds(u, n)]

        first = spread((key, "g", i), s, region, lambda: store(o2.at[:, pl.ds(u, n)], dw2_out.at[:, pl.ds(u, n)]))
        tr = (key, "tr", i)
        comm.msg(tr, ("t", 0), lambda: tb, lambda: region(z), across)
        comm.remote_if[tr] = x != y
        plan.task(3, [tr], first, lambda: comm.start(*first))

        def end(last, own):
            for m in range(n):
                tb[m] = own[m] + last[0][m] + last[1][m]
            comm.start(tr)

            @pl.when(x == y)
            def _():
                for m in range(n):
                    o2[z, u + m] = tb[m]

        return end, [tr]

    for i, (sigma, u, n) in enumerate(CHUNKS_DOWN_X):
        s = sgn[sigma]
        res = vx[i].at[1]
        end, sends = deliver("v", i, s, u, n, vt[i])
        raws = chain(("vz", i), "z", nz, s, vz[i], lambda rel, res=res: res.at[idx("z", rel)], None, 5, end, sends)

        def x_end(last, own, raws=raws):
            accumulate(last[0], [last[1], own])
            comm.start(*raws)

        raws = chain(("vx", i), "x", nx, s, vx[i], lambda rel, u=u, n=n: dw2.at[:, pl.ds(u, n), :, hcol(idx("x", rel))], 1, 10, x_end, raws)
        plan.task(20 + n1 + i, [], raws, lambda raws=raws: comm.start(*raws))

    for i, (sigma, u, n) in enumerate(CHUNKS_DOWN_Z):
        s = sgn[sigma]
        res = wz[i].at[nz // 2 - 1]
        end, sends = deliver("w", i, s, u, n, wt[i])
        raws = chain(("wx", i), "x", nx, s, wx[i], lambda rel, res=res: res.at[:, :, hcol(idx("x", rel))], None, 8, end, sends)

        def z_end(last, own, raws=raws):
            accumulate(last[0], [last[1], own])
            comm.start(*raws)

        raws = chain(("wz", i), "z", nz, s, wz[i], lambda rel, u=u, n=n: dw2.at[idx("z", rel), pl.ds(u, n)], 2, 9, z_end, raws)
        plan.task(20 + i, [], raws, lambda raws=raws: comm.start(*raws))

    rows = yo.shape[1] // 2
    for a, (part, out) in enumerate(((yp, y_out), (dxp, dx_out))):
        raw_of = {2: [], 3: [], 1: [], 0: []}
        for sigma in range(2):
            s = sgn[sigma]
            half = pl.ds(sigma * rows, rows)

            def y_end(last, own, a=a, half=half, sigma=sigma, out=out):
                @pl.loop(0, rows)
                def _(k):
                    yo[a, sigma * rows + k] = (own[k] + last[0][k] + last[1][k]).astype(BF16)

                store(yo.at[a, half], out.at[half])

            raws = chain(("y", a, sigma), "y", ny, s, yr.at[a, sigma], lambda rel, a=a, half=half: pair.at[a, rel % ny, half], None, 12, y_end, [],
                         (("pd", a, 0), ("pd", a, s % ny)))
            raw_of[2].append(raws[0])
            raw_of[-s % ny].append(raws[1])
        for n, o in enumerate((2, 3, 1, 0)):
            comm.msg(("p", a, o), ("d", 0), lambda part=part, o=o: part.at[1 - c, :, :, hcol(idx("y", o))], lambda a=a, o=o: pair.at[a, o], partner)
            mark(("pd", a, o))
            plan.task(15, [], [("p", a, o)], lambda a=a, o=o: comm.start(("p", a, o)), 0.15)
            k = stage(3, lambda part=part, o=o: part.at[c, :, :, hcol(idx("y", o))])

            def combine(a=a, o=o, k=k, go=raw_of[o]):
                accumulate(pair.at[a, o], [slot(k)])
                comm.start(*go)

            plan.task(14, [("p", a, o)], [("pd", a, o), *raw_of[o]], combine, 1.0, stage=k)

    order = plan.order()

    uses = {p: [] for p in range(len(pools))}
    for i in order:
        k = plan.tasks[i][5]
        if k is not None:
            uses[staged[k][0]].append(k)
    lbase, fill = 0, {}
    for p, ks in uses.items():
        depth = pools[p].shape[0]
        for n, k in enumerate(ks):
            place[k] = (pools[p].at[n % depth], lsem.at[lbase + n % depth])
            if n + depth < len(ks):
                fill[k] = ks[n + depth]
        lbase += depth

    def load(k):
        return pltpu.make_async_copy(staged[k][1](), *place[k])

    for p, ks in uses.items():
        for k in ks[: pools[p].shape[0]]:
            load(k).start()

    barrier = pltpu.get_barrier_semaphore()

    def tell(to):
        pl.semaphore_signal(barrier, inc=1, device_id=to, device_id_type=MESH)

    for to in (*[nb(axis, d) for axis in "zyx" for d in (1, -1)], partner):
        tell(to)

    @pl.when(x != y)
    def _():
        tell(across)

    pl.semaphore_wait(barrier, 7 + jnp.where(x != y, 1, 0))

    for i in order:
        _, waits, _, run, _, k = plan.tasks[i]
        if k is not None:
            load(k).wait()
        comm.wait(*waits)
        run()
        if k in fill:
            load(fill[k]).start()
    for copy in stores:
        copy.wait()
    comm.finish()


def reduce(dims, yp, dxp, dw1, dw2):
    nz, ny, nx = dims
    fc, hh = dw2.shape
    hb = hh // ny
    tk = yp.shape[0] // 2
    t8 = tk // 8
    nq, nu = hb // (2 * nz * 8), fc // (nz * 8)
    n_msg = 2 * 0
    vm = pltpu.VMEM

    def per(chunks, shape, count):
        return [vm(((count,) if count else ()) + shape(n), F32) for _, _, n in chunks]

    scratch = [
        *per(CHUNKS_UP, lambda n: (2, nz, n, 8, fc), nx - 1),
        *per(CHUNKS_UP, lambda n: (2, n, 8, fc), nz - 1),
        *per(CHUNKS_UP, lambda n: (n, 8, fc), 0),
        *per(CHUNKS_DOWN_X, lambda n: (nz, n, 8, hb), nx - 1),
        *per(CHUNKS_DOWN_X, lambda n: (n, 8, hb), nz - 1),
        *per(CHUNKS_DOWN_X, lambda n: (n, 8, hb), 0),
        *per(CHUNKS_DOWN_Z, lambda n: (n, 8, hh), nz - 1),
        *per(CHUNKS_DOWN_Z, lambda n: (n, 8, hb), nx - 1),
        *per(CHUNKS_DOWN_Z, lambda n: (n, 8, hb), 0),
        vm((nz, nq, 8, 2 * fc), F32),
        vm((nz, nu, 8, hb), F32),
        vm((2, ny, t8, 8, hb), F32),
        vm((2, 2, ny - 1, t8 // 2, 8, hb), F32),
        vm((2, t8, 8, hb), BF16),
        vm((4, 2, nz, CHUNKS_UP[0][2], 8, fc), F32),
        vm((4, nz, CHUNKS_DOWN_X[0][2], 8, hb), F32),
        vm((6, CHUNKS_DOWN_Z[0][2], 8, hh), F32),
        vm((2, t8, 8, hb), F32),
        pltpu.SemaphoreType.DMA((320,)),
        pltpu.SemaphoreType.DMA((320,)),
        pltpu.SemaphoreType.DMA((16,)),
        pltpu.SemaphoreType.DMA((24,)),
    ]
    y, dx, g1, g2 = pl.pallas_call(
        functools.partial(reduce_kernel, dims),
        out_shape=[
            jax.ShapeDtypeStruct((t8, 8, hb), BF16),
            jax.ShapeDtypeStruct((t8, 8, hb), BF16),
            jax.ShapeDtypeStruct((nz, nq, 8, 2 * fc), F32),
            jax.ShapeDtypeStruct((nz, nu, 8, hb), F32),
        ],
        in_specs=[ANY] * 4,
        out_specs=[ANY] * 4,
        scratch_shapes=scratch,
        compiler_params=pltpu.CompilerParams(collective_id=1, has_side_effects=True, vmem_limit_bytes=66_000_000),
        name="reduce",
    )(
        yp.reshape(2, t8, 8, hh),
        dxp.reshape(2, t8, 8, hh),
        dw1.reshape(nx, 2, nz, nq, 8, fc),
        dw2.reshape(nz, nu, 8, hh),
    )
    return y.reshape(tk, hb), dx.reshape(tk, hb), g1.reshape(nz * nq * 8, 2 * fc), g2.reshape(fc, hb)


def solution(mesh):
    act_spec = P(("depth", "row"), "col")
    weight_spec = P("row", "col")
    dims = (mesh.shape["depth"], mesh.shape["col"], mesh.shape["row"] // 2)
    last = (((1,), (1,)), ((), ()))
    first = (((0,), (0,)), ((), ()))

    def local_block(tok_blk, up_blk, down_blk, grad_blk):
        tok, grad, up, down = gather(dims, tok_blk, grad_blk, up_blk, down_blk)
        pre_act = jnp.dot(tok, up, preferred_element_type=F32)
        hidden, gelu_vjp = jax.vjp(gelu_fn, pre_act)
        hidden = hidden.astype(BF16)
        d_hidden = lax.dot_general(grad, down, last, preferred_element_type=F32)
        d_pre = gelu_vjp(d_hidden)[0].astype(BF16)
        dw_down = lax.dot_general(hidden, grad, first, preferred_element_type=F32)
        dw_up = lax.dot_general(tok, d_pre, first, preferred_element_type=F32)
        out_part = jnp.dot(hidden, down, preferred_element_type=F32)
        dx_part = lax.dot_general(d_pre, up, last, preferred_element_type=F32)
        return reduce(dims, out_part, dx_part, dw_up, dw_down)

    return jax.shard_map(local_block, mesh=mesh, in_specs=(act_spec, weight_spec, weight_spec, act_spec), out_specs=(act_spec, act_spec, weight_spec, weight_spec), check_vma=False)
```

```python
import functools
import itertools

import jax
import jax.numpy as jnp
from jax import lax
from jax.experimental import pallas as pl
from jax.experimental.pallas import tpu as pltpu
from jax.sharding import PartitionSpec as P

MESH = pl.DeviceIdType.MESH
ANY = pl.BlockSpec(memory_space=pl.ANY)
F32 = jnp.float32
SUB = 8
BF16 = jnp.bfloat16

CHUNKS = [(1, "z", i % 2, 8 + 2 * i, 2, i) for i in range(4)]
CHUNKS += [(0, "z", i % 2, 12 + 2 * i, 2, 20 + i) for i in range(2)]
CHUNKS += [(1, "x", i % 2, 2 * i, 2, i) for i in range(4)]
CHUNKS += [(0, "x", i % 2, 2 * i, 2, 4 + i) for i in range(6)]
FAR_FIRST = (2, 1, 3, 0)
Y_ORDER = [(a, o) for a in range(2) for o in FAR_FIRST]


def job_list():
    def block(a, u, n, order=FAR_FIRST):
        return [("D", a, o, u, n) for o in order]

    head = block(1, 8, 4, range(4)) + block(1, 0, 4) + block(1, 12, 4, range(4))
    rest = block(1, 4, 4) + block(0, 0, 8) + block(0, 8, 4) + block(0, 12, 4, range(4))
    both = head + rest
    cut = len(both) // 2
    jobs = both[:cut]
    out = [[("Y", a, o, 0), ("Y", a, o, 1)] for a, o in Y_ORDER]
    for job, two in itertools.zip_longest(both[cut:], out):
        jobs += ([job] if job else []) + (two or [])
    return jobs


JOBS = job_list()
LHS_ORDER = (0, 1)
COST = {"D": {2: 0.75, 4: 1.15, 8: 1.57}, "Y": 1.15, "mid": 0.05, "fin": 0.1, "go": 0.03, "U": 3.05, "A3": 1.55, "A": 0.6, "act": 0.63}
SLACK = 40.0
VMEM_LIMIT = 66_500_000


def gelu_fn(pre_act):
    return jax.nn.gelu(pre_act, approximate=True)


class Plan:
    def __init__(self, rates, window):
        self.rates, self.window = rates, window
        self.tasks, self.size, self.link = [], {}, {}

    def msg(self, key, link, nbytes):
        self.size[key], self.link[key] = nbytes, link

    def task(self, prio, waits, sends, run, cost=0.3, stage=(), raw=False):
        self.tasks.append((prio, tuple(waits), tuple(sends), run, cost, tuple(stage), raw))

    def order(self):
        free, arrive, out = {}, {}, []
        self.when, self.arrive = [], arrive
        now, left = 2.5, list(range(len(self.tasks)))
        while left:
            best = None
            for i in left:
                prio, waits, sends, _, _, _, raw = self.tasks[i]
                if any(w not in arrive for w in waits):
                    continue
                ready = max([arrive[w] for w in waits], default=0.0)
                if raw:
                    ready = max([ready] + [free.get(self.link[s], 0.0) - self.window for s in sends])
                key = (max(ready, now), prio, i)
                if best is None or key < best:
                    best = key
            at, _, i = best
            left.remove(i)
            out.append(i)
            now = at + self.tasks[i][4]
            self.when.append(now)
            for s in self.tasks[i][2]:
                rate, lat = self.rates[self.link[s][0]]
                took = self.size[s] / rate
                if self.link[s][0] == "t":
                    ways = [(axis, d) for axis in "xy" for d in (1, -1)]
                    done = max(now, *[free.get(way, 0.0) for way in ways]) + took
                    for way in ways:
                        free[way] = max(now, free.get(way, 0.0)) + took / 2
                else:
                    done = max(now, free.get(self.link[s], 0.0)) + took
                    free[self.link[s]] = done
                arrive[s] = done + lat
        self.end = max(now, max(arrive.values()))
        return out


RATES = {"x": (42e3, 2.2), "y": (44e3, 2.2), "z": (45e3, 2.2), "d": (300e3, 3.0), "t": (42e3, 5.0), "l": (1e12, 0.0), "s": (1e12, 1.5)}
WINDOW = 6.0


class Comm:
    def __init__(self, plan, ssem, rsem):
        self.plan, self.ssem, self.rsem = plan, ssem, rsem
        self.make, self.meet, self.slot, self.remote_if, self.flying = {}, {}, {}, {}, []

    def msg(self, key, link, src, dst, to, mail=None):
        i = len(self.slot)
        self.slot[key] = i
        there, here = mail or (i, i)

        def make(r):
            return pltpu.make_async_remote_copy(
                src_ref=src(), dst_ref=dst(), send_sem=self.ssem.at[i], recv_sem=self.rsem.at[r], device_id=to, device_id_type=MESH)

        self.make[key] = lambda: make(there)
        self.meet[key] = lambda: make(here)
        shape = src().shape
        nbytes = functools.reduce(lambda a, b: a * b, shape, 1) * src().dtype.itemsize
        self.plan.msg(key, link, nbytes)

    def each(self, keys, make, act):
        for key in keys:
            if key in self.remote_if:
                pl.when(self.remote_if[key])(lambda key=key: act(make[key]()))
            elif key in make:
                act(make[key]())

    def start(self, *keys):
        self.flying.extend(keys)
        self.each(keys, self.make, lambda copy: copy.start())

    def wait(self, *keys):
        self.each(keys, self.meet, lambda copy: copy.wait_recv())

    def sent(self, before):
        keys = [key for key in self.flying if self.plan.arrive[key] <= before]
        self.flying = [key for key in self.flying if self.plan.arrive[key] > before]
        self.each(keys, self.make, lambda copy: copy.wait_send())


def run_tasks(plan, comm, order, load=None, fill={}):
    heard = set()
    for n, i in enumerate(order):
        _, waits, _, run, _, ks, _ = plan.tasks[i]
        with jax.named_scope(f"w{n}"):
            comm.wait(*[w for w in waits if w not in heard])
            heard.update(waits)
        with jax.named_scope(f"l{n}"):
            for k in ks:
                load(k).wait()
        with jax.named_scope(f"r{n}"):
            run()
        for k in fill.get(n, ()):
            load(k).start()
        comm.sent(plan.when[n] - SLACK)
    comm.sent(float("inf"))


def where_am_i():
    z, y, r = lax.axis_index("depth"), lax.axis_index("col"), lax.axis_index("row")
    return z, y, lax.div(r, 2), lax.rem(r, 2)


def each(shape, fn):
    lead = shape[:-2]
    big = max(range(len(lead)), key=lambda d: lead[d])
    looped = lead[big] >= 8

    def rest(k):
        for ix in itertools.product(*[range(n) if not (looped and d == big) else (k,) for d, n in enumerate(lead)]):
            fn(ix)

    if looped:
        pl.loop(0, lead[big])(rest)
    else:
        rest(None)


def accumulate(dst, others):
    def one(ix):
        total = dst[ix]
        for o in others:
            total = total + o[ix]
        dst[ix] = total

    each(dst.shape, one)


def mm(a, b):
    return jnp.dot(a, b, preferred_element_type=F32)


def mm_l(a, b):
    return lax.dot_general(a, b, (((0,), (0,)), ((), ())), preferred_element_type=F32)


def mm_t(a, b):
    return lax.dot_general(a, b, (((1,), (1,)), ((), ())), preferred_element_type=F32)


def gather_kernel(dims, x_ref, g_ref, w1_ref, w2_ref, xf, gf, w1f, w2f, hid, dpre,
                  bx, bg, bw1, bw2, vw2, u, da, ha, hd, ssem, rsem, lsem, osem):
    nz, ny, nx = dims
    z, y, x, c = where_am_i()
    tk, hb = x_ref.shape
    fc = w2_ref.shape[0]
    hr, fz, half = hb // 2, fc // nz, tk // 2
    plan = Plan(RATES, WINDOW)
    comm = Comm(plan, ssem, rsem)
    ways = (1, -1)

    def idx(axis, d):
        at, n = {"z": (z, nz), "y": (y, ny), "x": (x, nx)}[axis]
        return lax.rem(at + (d % n), n)

    def nb(axis, d):
        i = idx(axis, d)
        return {"z": {"depth": i}, "y": {"col": i}, "x": {"row": 2 * i + c}}[axis]

    partner = {"row": 2 * x + (1 - c)}

    def at(i, size):
        return pl.ds(pl.multiple_of(i * size, size), size)

    def block(full, core, o, part=None):
        rows = at(core, tk) if part is None else pl.ds(pl.multiple_of(core * tk + part * half, half), half)
        return full.at[rows, at(idx("y", o), hb)]

    def wblock(o, core):
        return bw1.at[at(2 * idx("x", o) + core, hr), :]

    def piece(d, o):
        return bw2.at[at(idx("z", d), fz), at(idx("y", o), hb)]

    stores = []

    def store(src, dst):
        copy = pltpu.make_async_copy(src, dst, osem.at[len(stores)])
        stores.append(copy)
        copy.start()

    def mark(key):
        plan.msg(key, ("l", key), 0)
        return key

    loads = {}

    def load(name, src, dst):
        loads[name] = pltpu.make_async_copy(src, dst, lsem.at[len(loads)])
        plan.task(len(loads) / 10, [], [mark(name)], loads[name].wait, COST["mid"])

    load("s", w2_ref.at[at(z, fz), :], vw2)
    load("w", w1_ref.at[:, at(c, fc)], wblock(0, c))
    load("x", x_ref, block(bx, c, 0))
    load("g", g_ref, block(bg, c, 0))
    self_copy = pltpu.make_async_copy(w2_ref.at[at(z, fz), :], piece(0, 0), lsem.at[len(loads)])

    def raw(prio, waits, keys):
        plan.task(prio, waits, keys, lambda: comm.start(*keys), COST["go"], raw=True)

    def passed(prio, wait, keys, key=None):
        plan.task(prio, [wait], [*keys, mark(("in", *wait) if key is None else key)], lambda: comm.start(*keys), COST["go"])

    for o in (1, -1, 2, 0):
        o = o % ny
        to = {"row": 2 * idx("x", o) + c, "col": x}
        comm.msg(("s", o), ("t", 0), lambda: vw2, lambda: piece(0, 0), to, mail=(y, idx("y", o)))
    comm.remote_if[("s", 0)] = x != y
    plan.task(1, ["s"], [("s", o) for o in range(ny)], lambda: comm.start(*[("s", o) for o in range(ny)]), COST["go"])
    whole = {d: [] for d in range(nz)}
    far = nz // 2
    for o in range(ny):
        for w in ways:
            steps = far if (w > 0) == (o % 2 == 0) else far - 1
            for t in range(steps):
                comm.msg(("z", o, w, t), ("z", w), lambda o=o, w=w, t=t: piece(-w * t, o), lambda o=o, w=w, t=t: piece(-w * t, o), nb("z", w))
                nxt = [("z", o, w, t + 1)] if t + 1 < steps else []
                key = ("w2", o, (-w * (t + 1)) % nz)
                passed(4, ("z", o, w, t), nxt, key)
                whole[key[2]].append(key)
        first = [("z", o, w, 0) for w in ways]

        def slice_in(o=o, first=first):
            if o == 0:
                pl.when(x == y)(self_copy.wait)
            comm.start(*first)

        plan.task(3, [("s", o)], [*first, mark(("w2", o, 0))], slice_in, COST["go"])
        whole[0].append(("w2", o, 0))

    comm.msg(("pw",), ("d", 0), lambda: w1_ref.at[:, at(1 - c, fc)], lambda: wblock(0, c), partner)
    raw(1.1, [], [("pw",)])
    w1_in = {0: ["w"], 1: [], -1: [], 2: []}
    for own in (True, False):
        core = c if own else 1 - c
        for w in ways:
            comm.msg(("wa", own, w), ("x", w), lambda core=core: wblock(0, core), lambda core=core: wblock(0, core), nb("x", w))
    raw(1.2, ["w"], [("wa", True, w) for w in ways])
    passed(5, ("pw",), [("wa", False, w) for w in ways])
    w1_in[0].append(("in", "pw"))
    for own, w in ((True, 1), (False, -1)):
        core = c if own else 1 - c
        comm.msg(("wf", w), ("x", w), lambda core=core, w=w: wblock(-w, core), lambda core=core, w=w: wblock(-w, core), nb("x", w))
        passed(6, ("wa", own, w), [("wf", w)])
        passed(6, ("wa", not own, w), [])
        passed(6, ("wf", w), [])
        w1_in[-w] += [("in", "wa", True, w), ("in", "wa", False, w)]
        w1_in[2].append(("in", "wf", w))

    arrived = {}
    for a, (full, name) in enumerate(((bx, "x"), (bg, "g"))):
        arrived[a] = [name]
        for w in ways:
            for p in range(2):
                comm.msg((name, w, p), ("y", w), lambda full=full, p=p: block(full, c, 0, p), lambda full=full, p=p: block(full, c, 0, p), nb("y", w))
            p = 0 if w > 0 else 1
            comm.msg((name, "f", w), ("y", w), lambda full=full, w=w, p=p: block(full, c, -w, p), lambda full=full, w=w, p=p: block(full, c, -w, p), nb("y", w))

        def share(key, o, p, full=full, name=name, a=a):
            comm.msg((name, "d", *key), ("d", 0), lambda: block(full, c, o, p), lambda: block(full, c, o, p), partner)
            passed(20, (name, "d", *key), [])
            arrived[a].append(("in", name, "d", *key))
            return (name, "d", *key)

        plan.task(2 + a, [name], [share((0,), 0, None)], lambda name=name: comm.start((name, "d", 0)), COST["go"])
        for w in ways:
            p = 0 if w > 0 else 1
            for q in range(2):
                keys = [share((-w, q), -w, q)] + ([(name, "f", w)] if q == p else [])
                passed(7, (name, w, q), keys)
                arrived[a].append(("in", name, w, q))
            passed(7, (name, "f", w), [share((2, p), 2, p)])
            arrived[a].append(("in", name, "f", w))
    for n, (name, late) in enumerate(itertools.product("xg", (False, True))):
        raw(1.3 + n / 100, [name], [(name, w, 1 if (w > 0) == late else 0) for w in ways])
    plan.task(9, arrived[0], [mark("X")], lambda: store(bx, xf), COST["go"])
    near = [key for key in arrived[1] if not (key[:3] == ("in", "g", "f") or key[:4] == ("in", "g", "d", 2))]
    plan.task(9, near, [mark("G3")], lambda: None, COST["go"])
    plan.task(9, arrived[1], [mark("G")], lambda: store(bg, gf), COST["go"])

    tile = 256
    order_u = (0, 1, -1, 2)
    for n, o in enumerate(order_u):
        def up(n=n, o=o):
            j = idx("x", o)
            store(bw1.at[at(j, hb), :], w1f.at[at(j, hb), :])

            @pl.loop(0, 2 * fc // tile)
            def _(i):
                rows, cols = at(lax.rem(i, 2), tk), at(lax.div(i, 2), tile)
                v = mm(bx[rows, at(j, hb)], bw1[at(j, hb), cols])
                u[rows, cols] = v if n == 0 else u[rows, cols] + v

        plan.task(30, ["X", *w1_in[o], *([("U", n - 1)] if n else [])], [mark(("U", n))], up, COST["U"])
    for d in sorted(range(nz), key=lambda d: min(d, nz - d)):
        def down(os, d=d):
            cols = at(idx("z", d), fz)

            @pl.loop(0, 2)
            def _(i):
                rows = at(i, tk)
                v = sum(mm_t(bg[rows, at(idx("y", o), hb)], bw2[cols, at(idx("y", o), hb)]) for o in os)
                da[rows, cols] = v if len(os) > 1 else da[rows, cols] + v

        def act(d=d):
            cols = at(idx("z", d), fz)

            @pl.loop(0, 2 * tk // fz)
            def _(i):
                rows = at(i, fz)
                h, vjp = jax.vjp(gelu_fn, u[rows, cols])
                ha[rows, cols] = h.astype(BF16)
                hd[rows, cols] = vjp(da[rows, cols])[0].astype(BF16)

            store(bw2.at[cols, :], w2f.at[cols, :])
            store(ha.at[:, cols], hid.at[:, cols])
            store(hd.at[:, cols], dpre.at[:, cols])

        plan.task(31, ["G3", *whole[d]], [mark(("A3", d))], functools.partial(down, (0, 1, -1)), COST["A3"])
        plan.task(32, ["G", ("A3", d)], [mark(("A", d))], functools.partial(down, (2,)), COST["A"])
        plan.task(33, [("A", d), ("U", len(order_u) - 1)], [], act, COST["act"])

    order = plan.order()
    for copy in loads.values():
        copy.start()
    pl.when(x == y)(self_copy.start)

    barrier = pltpu.get_barrier_semaphore()

    def tell(to):
        pl.semaphore_signal(barrier, inc=1, device_id=to, device_id_type=MESH)

    for to in (*[nb(axis, d) for axis in "zyx" for d in ways], partner):
        tell(to)
    for o in range(1, ny):
        tell({"row": 2 * y + c, "col": idx("y", o)})
    pl.when(x != y)(lambda: tell({"row": 2 * y + c, "col": y}))
    pl.semaphore_wait(barrier, 6 + ny + jnp.where(x != y, 1, 0))
    run_tasks(plan, comm, order)
    for copy in stores:
        copy.wait()


def gather(dims, tok, grad, up, down):
    tk, hb = tok.shape
    fc = down.shape[0]
    nz, ny, nx = dims
    sds, vm = jax.ShapeDtypeStruct, pltpu.VMEM
    tokens, first, second, mid = (2 * tk, ny * hb), (nx * hb, fc), (fc, ny * hb), (2 * tk, fc)
    return pl.pallas_call(
        functools.partial(gather_kernel, dims),
        out_shape=[sds(shape, BF16) for shape in (tokens, tokens, first, second, mid, mid)],
        in_specs=[ANY] * 4,
        out_specs=[ANY] * 6,
        scratch_shapes=[
            *[vm(shape, BF16) for shape in (tokens, tokens, first, second, (fc // nz, hb))],
            vm(mid, F32),
            vm(mid, F32),
            vm(mid, BF16),
            vm(mid, BF16),
            pltpu.SemaphoreType.DMA((80,)),
            pltpu.SemaphoreType.DMA((80,)),
            pltpu.SemaphoreType.DMA((5,)),
            pltpu.SemaphoreType.DMA((30,)),
        ],
        compiler_params=pltpu.CompilerParams(collective_id=0, has_side_effects=True, vmem_limit_bytes=VMEM_LIMIT),
        name="gather",
    )(tok, grad, up, down)


def reduce_kernel(dims, tok, grad, up, down, hid, dpre,
                  y_out, dx_out, g1_out, g2_out, dwp, yp, wx1, wx2, hx, dx, *scratch):
    nz, ny, nx = dims
    z, y, x, c = where_am_i()
    hb = y_out.shape[-1]
    tk = tok.shape[0] // 2
    hr = hb // 2
    fc = hid.shape[1]
    nu = fc // (nz * 8)
    sgn = (1, -1)
    scratch = list(scratch)

    def grab(n):
        return [scratch.pop(0) for _ in range(n)]

    nc = len(CHUNKS)
    xbuf, zbuf, tbuf = grab(nc), grab(nc), grab(nc)
    o1, o2, yr, yo, lhs, par, tmp = grab(7)
    pools = grab(5)
    ssem, rsem, lsem, osem, isem, tsem = grab(6)
    P_X, P_Z, P_Y, P_R, P_W = range(5)

    plan = Plan(RATES, WINDOW)
    comm = Comm(plan, ssem, rsem)

    def idx(axis, d):
        at, n = {"z": (z, nz), "y": (y, ny), "x": (x, nx)}[axis]
        return lax.rem(at + (d % n), n)

    def nb(axis, d):
        i = idx(axis, d)
        return {"z": {"depth": i}, "y": {"col": i}, "x": {"row": 2 * i + c}}[axis]

    partner = {"row": 2 * x + (1 - c)}
    across = {"row": 2 * y + c, "col": x}

    def hcol(j):
        return pl.ds(pl.multiple_of(j * hb, hb), hb)

    staged, stores, place = [], [], {}

    def stage(pool, src, marks=(), n=None):
        staged.append((pool, src, tuple(marks), n))
        return len(staged) - 1

    def slot(k):
        return place[k][0]

    def mark(key):
        plan.msg(key, ("l", key), 0)
        return key

    def chain(key, axis, n, s, buf, src, pool, marks, prio, end, end_sends, units=None):
        far, near = n // 2, n // 2 - 1
        for t in range(far):
            comm.msg((key, "F", t), (axis, s), (lambda: src(far * s)) if t == 0 else (lambda t=t: buf.at[t - 1]), lambda t=t: buf.at[t], nb(axis, s))
        for t in range(near):
            comm.msg((key, "N", t), (axis, -s), (lambda: src(-near * s)) if t == 0 else (lambda t=t: buf.at[far + t - 1]), lambda t=t: buf.at[far + t], nb(axis, -s))

        def own(rel):
            return [] if pool is None else [stage(pool, lambda: src(rel), marks(rel), units)]

        def mid(name, t, at, rel):
            ks = own(rel)

            def run():
                accumulate(buf.at[at], [slot(ks[0]) if ks else src(rel)])
                comm.start((key, name, t + 1))

            plan.task(prio, [(key, name, t), *marks(rel)], [(key, name, t + 1)], run, COST["mid"], stage=ks)

        for t in range(far - 1):
            mid("F", t, t, (far - 1 - t) * s)
        for t in range(near - 1):
            mid("N", t, far + t, -(near - 1 - t) * s)
        ks = own(0)
        last = [buf.at[far - 1], buf.at[far + near - 1]]
        plan.task(prio, [(key, "F", far - 1), (key, "N", near - 1), *marks(0)], end_sends,
                  lambda: end(last, slot(ks[0]) if ks else src(0)), COST["fin"], stage=ks)
        return [(key, "F", 0), (key, "N", 0)]

    def raw(prio, marks, keys):
        plan.task(prio, marks, keys, lambda: comm.start(*keys), COST["go"], raw=True)

    def spread(key, s, region, finish):
        far, near = nz // 2, nz // 2 - 1
        for name, count, d in (("GF", far, s), ("GN", near, -s)):
            for t in range(count):
                def ref(t=t, d=d):
                    return region(idx("z", -t * d))
                comm.msg((key, name, t), ("z", d), ref, ref, nb("z", d))
        for name, count in (("GF", far), ("GN", near)):
            for t in range(count - 1):
                plan.task(4, [(key, name, t)], [(key, name, t + 1)], lambda name=name, t=t: comm.start((key, name, t + 1)), COST["go"])
        plan.task(30, [(key, "GF", far - 1), (key, "GN", near - 1)], [], finish, COST["go"])
        return [(key, "GF", 0), (key, "GN", 0)]

    def store(src, dst):
        copy = pltpu.make_async_copy(src, dst, osem.at[len(stores)])
        stores.append(copy)
        copy.start()

    def none(rel):
        return ()

    for i, (a, first_axis, sigma, u, n, prio) in enumerate(CHUNKS):
        s = sgn[sigma]

        def done(o, a=a, u=u, n=n):
            return [("D", a, o % nx, v) for v in range(u, u + n)]

        if a == 0:
            def region(k, u=u, n=n):
                return o1.at[:, pl.ds(u, n), k]

            go = spread(("g", i), s, region, lambda u=u, n=n: store(o1.at[:, pl.ds(u, n)], g1_out.at[:, pl.ds(u, n)]))
            over = ("sw", i)
            comm.msg(over, ("d", 0), lambda i=i: tbuf[i], lambda u=u, n=n: o1.at[c, pl.ds(u, n), z], partner)

            def end(last, own, i=i, u=u, n=n, over=over):
                mine = pl.ds(pl.multiple_of(c * hr, hr), hr)
                other = pl.ds(pl.multiple_of((1 - c) * hr, hr), hr)
                for m in range(n):
                    tbuf[i][m] = own[m, :, other] + last[0][m, :, other] + last[1][m, :, other]
                comm.start(over)
                for m in range(n):
                    o1[c, u + m, z] = own[m, :, mine] + last[0][m, :, mine] + last[1][m, :, mine]
        else:
            def region(k, u=u, n=n):
                return o2.at[pl.ds(u, n), k]

            go = spread(("g", i), s, region, lambda u=u, n=n: store(o2.at[pl.ds(u, n)], g2_out.at[pl.ds(u, n)]))
            over = ("tr", i)
            comm.msg(over, ("t", 0), lambda i=i: tbuf[i], lambda region=region: region(z), across)
            comm.remote_if[over] = x != y

            def end(last, own, i=i, u=u, n=n, over=over):
                for m in range(n):
                    tbuf[i][m] = own[m] + last[0][m] + last[1][m]
                comm.start(over)

                @pl.when(x == y)
                def _():
                    for m in range(n):
                        o2[u + m, z] = tbuf[i][m]

        plan.task(3, [over], go, lambda go=go: comm.start(*go), COST["go"])
        if first_axis == "x":
            res = xbuf[i].at[nx // 2 - 1]
            raws = chain(("z", i), "z", nz, s, zbuf[i], lambda rel, res=res: res.at[:, idx("z", rel)], None, none, 5, end, [over])

            def x_end(last, own, raws=raws):
                accumulate(last[0], [last[1], own])
                comm.start(*raws)

            raws = chain(("x", i), "x", nx, s, xbuf[i], lambda rel, a=a, u=u, n=n: dwp.at[a, pl.ds(u, n), :, :, hcol(idx("x", rel))],
                         P_X, lambda rel, done=done: done(rel), 10, x_end, raws, n)
            raw(11 + prio / 100, done(2) + done(-s), raws)
        else:
            res = zbuf[i].at[nz // 2 - 1]
            raws = chain(("x", i), "x", nx, s, xbuf[i], lambda rel, res=res: res.at[:, :, hcol(idx("x", rel))], None, none, 8, end, [over])

            def z_end(last, own, raws=raws):
                accumulate(last[0], [last[1], own])
                comm.start(*raws)

            all_done = [m for o in range(nx) for m in done(o)]
            raws = chain(("z", i), "z", nz, s, zbuf[i], lambda rel, a=a, u=u, n=n: dwp.at[a, pl.ds(u, n), idx("z", rel)],
                         P_Z, lambda rel, all_done=all_done: all_done, 9, z_end, raws, n)
            raw(11 + prio / 100, all_done, raws)

    groups = yo.shape[1]
    for a, out in enumerate((y_out, dx_out)):
        for sigma in range(2):
            s = sgn[sigma]
            half = pl.ds(sigma * (groups // 2), groups // 2)

            def y_end(last, own, a=a, half=half, sigma=sigma, out=out):
                def one(ix):
                    yo[(a, sigma * (groups // 2) + ix[0], ix[1])] = (own[ix] + last[0][ix] + last[1][ix]).astype(BF16)

                each(own.shape, one)
                store(yo.at[a, half], out.at[half])

            raws = chain(("y", a, sigma), "y", ny, s, yr.at[a, sigma], lambda rel, a=a, half=half: yp.at[a, half, :, :, hcol(idx("y", rel))],
                         P_Y, lambda rel, a=a: [("Y", a, rel % ny)], 12, y_end, [])
            raw(11, [("Y", a, 2), ("Y", a, -s % ny)], raws)

    tile = 256

    def rows(o):
        return pl.ds(pl.multiple_of(idx("y", o) * hb, hb), hb)

    def arrive(key, prio=6):
        plan.task(prio, [key], [mark(("got", *key))], lambda: None, 0.01)
        return ("got", *key)

    lhs_loads = [pltpu.make_async_copy(src, lhs.at[n], isem.at[n]) for n, src in enumerate((hid, dpre))]
    for n in (0, 1):
        plan.task(0, [], [mark(("T", n))], lhs_loads[n].wait, 0.3)

    others = pl.ds(pl.multiple_of((1 - c) * tk, tk), tk)
    own_rows = pl.ds(pl.multiple_of(c * tk, tk), tk)
    par_loads = []
    for n, (src, box) in enumerate(((hid, hx), (dpre, dx))):
        comm.msg(("hx", n), ("d", 0), lambda src=src: src.at[others], lambda box=box: box, partner)
        raw(1, [], [("hx", n)])
        par_loads.append(pltpu.make_async_copy(box, par.at[n], isem.at[2 + n]))
        plan.task(6, [("hx", n)], [mark(("P", n))], par_loads[n].start, 0.02)
    for a, o in Y_ORDER:
        if a == 0:
            comm.msg(("w", a, o), ("d", 0), lambda o=o: down.at[:, hcol(idx("y", o))], lambda o=o: wx2.at[:, hcol(idx("y", o))], partner)
        else:
            comm.msg(("w", a, o), ("d", 0), lambda o=o: up.at[rows(o)], lambda o=o: wx1.at[rows(o)], partner)
        raw(2, [], [("w", a, o)])

    par_seen = set()
    last_of, b = {}, 1
    for n, job in enumerate(JOBS):
        opens, closes = job[0] == "D" or job[3] == 0, job[0] == "D" or job[3] == 1
        b = 1 - b if opens else b
        keys = [("Y", job[1], job[2])] if job[0] == "Y" else [("D", job[1], job[2] % nx, v) for v in range(job[3], job[3] + job[4])]
        span = pl.ds(0, yo.shape[1] if job[0] == "Y" else job[4])
        waits = [("C", n - 1)] if n else []
        if opens and b in last_of:
            waits.append(("S", last_of[b]))
        if job[0] == "D":
            _, a, o, u, n_u = job
            waits.append(("T", 1 - a))
            ks = [stage(P_R, lambda a=a, o=o: (tok, grad)[a].at[:, hcol(idx("x", o))])]

            def value(cols, a=a, u=u, n_u=n_u, ks=ks):
                return mm_l(lhs[1 - a, :, u * nz * 8:(u + n_u) * nz * 8], slot(ks[0])[:, cols])

            dst = functools.partial(lambda a, o, u, n_u: dwp.at[a, pl.ds(u, n_u), :, :, hcol(idx("x", o))], a, o, u, n_u)
            cost = COST["D"][n_u]
        else:
            _, a, o, h = job
            waits.append(("T", a))
            marks = []
            if h:
                marks = [arrive(("w", a, o))]
                waits += [("P", a), *marks]
            if a == 0:
                ks = [stage(P_R, lambda o=o, w=(down, wx2)[h]: w.at[:, hcol(idx("y", o))], marks)]
            else:
                ks = [stage(P_W, lambda o=o, w=(up, wx1)[h]: w.at[rows(o)], marks)]

            def value(cols, a=a, h=h, ks=ks):
                left = par[a] if h else lhs[a, own_rows, :]
                return mm(left, slot(ks[0])[:, cols]) if a == 0 else mm_t(left, slot(ks[0])[cols, :])

            dst = functools.partial(lambda a, o: yp.at[a, :, :, :, hcol(idx("y", o))], a, o)
            cost = COST["Y"]

        def save(b=b, dst=dst, span=span):
            return pltpu.make_async_copy(tmp.at[b, span], dst(), tsem.at[b])

        def run(b=b, value=value, save=save, job=job, span=span, opens=opens, closes=closes):
            if job[0] == "Y" and job[3] and job[1] not in par_seen:
                par_loads[job[1]].wait()
                par_seen.add(job[1])

            @pl.loop(0, hb // tile)
            def _(t):
                cols = pl.ds(pl.multiple_of(t * tile, tile), tile)
                v = value(cols).reshape((span.size,) + tmp.shape[2:4] + (tile,))
                tmp[b, span, :, :, cols] = v if opens else tmp[b, span, :, :, cols] + v

            if closes:
                save().start()

        sends = [mark(("C", n))]
        if closes:
            plan.msg(("W", n), ("s", n), 0)
            sends.append(("W", n))
            last_of[b] = n
            plan.task(2, [("W", n)], [mark(("S", n)), *[mark(key) for key in keys]], lambda save=save: save().wait(), 0.03)
        plan.task(40, waits, sends, run, cost, stage=ks)

    order = plan.order()

    at = {}
    for n, i in enumerate(order):
        for w in plan.tasks[i][2]:
            at[w] = n
    uses = {p: [] for p in range(len(pools))}
    user = {}
    for n, i in enumerate(order):
        for k in plan.tasks[i][5]:
            uses[staged[k][0]].append(k)
            user[k] = n
    lbase, fill = 0, {}
    for p, ks in uses.items():
        depth = pools[p].shape[0]
        for n, k in enumerate(ks):
            box = pools[p].at[n % depth] if staged[k][3] is None else pools[p].at[n % depth, pl.ds(0, staged[k][3])]
            place[k] = (box, lsem.at[lbase + n % depth])
            when = -1 if n < depth else user[ks[n - depth]]
            for w in staged[k][2]:
                when = max(when, at[w])
            fill.setdefault(when, []).append(k)
        lbase += depth

    def load(k):
        return pltpu.make_async_copy(staged[k][1](), *place[k])

    for n in LHS_ORDER:
        lhs_loads[n].start()
    for k in fill.get(-1, ()):
        load(k).start()

    barrier = pltpu.get_barrier_semaphore()

    def tell(to):
        pl.semaphore_signal(barrier, inc=1, device_id=to, device_id_type=MESH)

    for to in (*[nb(axis, d) for axis in "zyx" for d in (1, -1)], partner):
        tell(to)

    @pl.when(x != y)
    def _():
        tell(across)

    pl.semaphore_wait(barrier, 7 + jnp.where(x != y, 1, 0))

    run_tasks(plan, comm, order, load, fill)
    for copy in stores:
        copy.wait()


def reduce(dims, tok, grad, up, down, hid, dpre):
    nz, ny, nx = dims
    rows2, hh = tok.shape
    fc = hid.shape[1]
    tk, hb = rows2 // 2, hh // ny
    hr = hb // 2
    nu = fc // (nz * SUB)
    g = tk // (SUB * SUB)
    vm = pltpu.VMEM

    def per(shape):
        return [vm(shape(axis, n), F32) for _, axis, _, _, n, _ in CHUNKS]

    def fin(shape):
        return [vm((n, SUB, hr if a == 0 else hb), F32) for a, _, _, _, n, _ in CHUNKS]

    n0 = max(chunk[4] for chunk in CHUNKS)
    scratch = [
        *per(lambda axis, n: (nx - 1, n, nz, SUB, hb) if axis == "x" else (nx - 1, n, SUB, hb)),
        *per(lambda axis, n: (nz - 1, n, SUB, hb) if axis == "x" else (nz - 1, n, SUB, hh)),
        *fin(0),
        vm((2, nu, nz, SUB, hr), F32),
        vm((nu, nz, SUB, hb), F32),
        vm((2, 2, ny - 1, g // 2, SUB, SUB, hb), F32),
        vm((2, g, SUB, SUB, hb), BF16),
        vm((2, rows2, fc), BF16),
        vm((2, tk, fc), BF16),
        vm((2, g, SUB, SUB, hb), F32),
        vm((3, n0, nz, SUB, hb), F32),
        vm((6, n0, SUB, hh), F32),
        vm((2, g // 2, SUB, SUB, hb), F32),
        vm((3, rows2, hb), BF16),
        vm((3, hb, fc), BF16),
        pltpu.SemaphoreType.DMA((340,)),
        pltpu.SemaphoreType.DMA((340,)),
        pltpu.SemaphoreType.DMA((18,)),
        pltpu.SemaphoreType.DMA((24,)),
        pltpu.SemaphoreType.DMA((6,)),
        pltpu.SemaphoreType.DMA((2,)),
    ]
    sds = jax.ShapeDtypeStruct
    outs = pl.pallas_call(
        functools.partial(reduce_kernel, dims),
        out_shape=[
            sds((g, SUB, SUB, hb), BF16),
            sds((g, SUB, SUB, hb), BF16),
            sds((2, nu, nz, SUB, hr), F32),
            sds((nu, nz, SUB, hb), F32),
            sds((2, nu, nz, SUB, hh), F32),
            sds((2, g, SUB, SUB, hh), F32),
            sds(up.shape, BF16),
            sds(down.shape, BF16),
            sds((tk, fc), BF16),
            sds((tk, fc), BF16),
        ],
        in_specs=[ANY] * 6,
        out_specs=[ANY] * 10,
        scratch_shapes=scratch,
        compiler_params=pltpu.CompilerParams(collective_id=1, has_side_effects=True, vmem_limit_bytes=VMEM_LIMIT),
        name="reduce",
    )(tok, grad, up, down, hid, dpre)
    y, dx, g1, g2 = outs[:4]
    return y.reshape(tk, hb), dx.reshape(tk, hb), g1.reshape(2 * fc, hr).T, g2.reshape(fc, hb)


def solution(mesh):
    act_spec = P(("depth", "row"), "col")
    weight_spec = P("row", "col")
    dims = (mesh.shape["depth"], mesh.shape["col"], mesh.shape["row"] // 2)

    def local_block(tok_blk, up_blk, down_blk, grad_blk):
        return reduce(dims, *gather(dims, tok_blk, grad_blk, up_blk, down_blk))

    return jax.shard_map(local_block, mesh=mesh, in_specs=(act_spec, weight_spec, weight_spec, act_spec), out_specs=(act_spec, act_spec, weight_spec, weight_spec), check_vma=False)
```

```python
import functools
import itertools

import jax
import jax.numpy as jnp
from jax import lax
from jax.experimental import pallas as pl
from jax.experimental.pallas import tpu as pltpu
from jax.sharding import PartitionSpec as P

MESH = pl.DeviceIdType.MESH
ANY = pl.BlockSpec(memory_space=pl.ANY)
F32 = jnp.float32
SUB = 8
BF16 = jnp.bfloat16

def chunk_list():
    def run(a, axis, lo, hi, n, rank):
        return [(a, axis, k % 2, u, n, rank + k) for k, u in enumerate(range(lo, hi, n))]

    return [*run(1, "z", 8, 16, 2, 0), *run(0, "z", 14, 16, 2, 20), *run(1, "x", 0, 8, 2, 0), *run(0, "x", 0, 12, 2, 4), *run(0, "x", 12, 14, 1, 10)]


CHUNKS = chunk_list()
FAR_FIRST = (2, 1, 3, 0)
Y_ORDER = [(a, o) for a in range(2) for o in FAR_FIRST]


def job_list():
    def block(a, u, n, order=FAR_FIRST):
        return [("D", a, o, u, n) for o in order]

    near = range(4)
    both = block(1, 8, 4, near) + block(1, 0, 4) + block(1, 12, 4, near) + block(1, 4, 4) + block(0, 0, 8) + block(0, 8, 6) + block(0, 14, 2, near)
    cut = len(both) // 3
    jobs = both[:cut]
    out = [[("Y", a, o, 0), ("Y", a, o, 1)] for a, o in Y_ORDER]
    for job, two in itertools.zip_longest(both[cut:], out):
        jobs += ([job] if job else []) + (two or [])
    return jobs


JOBS = job_list()
LHS_ORDER = (0, 1)
COST = {"D": {2: 0.75, 4: 1.15, 6: 1.4, 8: 1.57}, "Y": 1.15, "mid": 0.05, "fin": 0.1, "go": 0.03, "U": 4.0, "A": 0.8, "act": 3.0}
SLACK = 40.0
SPREAD, GATED = 11.5, True
VMEM_LIMIT = 66_500_000


def gelu_fn(pre_act):
    return jax.nn.gelu(pre_act, approximate=True)


class Plan:
    def __init__(self, rates, window):
        self.rates, self.window = rates, window
        self.tasks, self.size, self.link = [], {}, {}

    def msg(self, key, link, nbytes):
        self.size[key], self.link[key] = nbytes, link

    def task(self, prio, waits, sends, run, cost=0.3, stage=(), raw=False):
        self.tasks.append((prio, tuple(waits), tuple(sends), run, cost, tuple(stage), raw))

    def order(self):
        free, arrive, out = {}, {}, []
        self.when, self.arrive = [], arrive
        now, left = 2.5, list(range(len(self.tasks)))
        while left:
            best = None
            for i in left:
                prio, waits, sends, _, _, _, raw = self.tasks[i]
                if any(w not in arrive for w in waits):
                    continue
                ready = max([arrive[w] for w in waits], default=0.0)
                if raw:
                    ready = max([ready] + [free.get(self.link[s], 0.0) - self.window for s in sends])
                key = (max(ready, now), prio, i)
                if best is None or key < best:
                    best = key
            at, _, i = best
            left.remove(i)
            out.append(i)
            now = at + self.tasks[i][4]
            self.when.append(now)
            for s in self.tasks[i][2]:
                rate, lat = self.rates[self.link[s][0]]
                took = self.size[s] / rate
                if self.link[s][0] == "t":
                    ways = [(axis, d) for axis in "xy" for d in (1, -1)]
                    done = max(now, *[free.get(way, 0.0) for way in ways]) + took
                    for way in ways:
                        free[way] = max(now, free.get(way, 0.0)) + took / 2
                else:
                    done = max(now, free.get(self.link[s], 0.0)) + took
                    free[self.link[s]] = done
                arrive[s] = done + lat
        self.end = max(now, max(arrive.values()))
        return out


RATES = {axis: (45e3, 2.2) for axis in "xyz"}
RATES.update(d=(450e3, 3.0), t=(45e3, 5.0), l=(1e12, 0.0), s=(1e12, 2.0))
WINDOW = 10.0


class Comm:
    def __init__(self, plan, ssem, rsem):
        self.plan, self.ssem, self.rsem = plan, ssem, rsem
        self.make, self.meet, self.slot, self.remote_if, self.flying = {}, {}, {}, {}, []

    def msg(self, key, link, src, dst, to, mail=None):
        i = len(self.slot)
        self.slot[key] = i
        there, here = mail or (i, i)

        def make(r):
            return pltpu.make_async_remote_copy(
                src_ref=src(), dst_ref=dst(), send_sem=self.ssem.at[i], recv_sem=self.rsem.at[r], device_id=to, device_id_type=MESH)

        self.make[key] = lambda: make(there)
        self.meet[key] = lambda: make(here)
        shape = src().shape
        nbytes = functools.reduce(lambda a, b: a * b, shape, 1) * src().dtype.itemsize
        self.plan.msg(key, link, nbytes)

    def each(self, keys, make, act):
        for key in keys:
            if key in self.remote_if:
                pl.when(self.remote_if[key])(lambda key=key: act(make[key]()))
            elif key in make:
                act(make[key]())

    def start(self, *keys):
        self.flying.extend(keys)
        self.each(keys, self.make, lambda copy: copy.start())

    def wait(self, *keys):
        self.each(keys, self.meet, lambda copy: copy.wait_recv())

    def sent(self, before):
        keys = [key for key in self.flying if self.plan.arrive[key] <= before]
        self.flying = [key for key in self.flying if self.plan.arrive[key] > before]
        self.each(keys, self.make, lambda copy: copy.wait_send())


def run_tasks(plan, comm, order, load=None, fill={}):
    heard = set()
    for n, i in enumerate(order):
        _, waits, _, run, _, ks, _ = plan.tasks[i]
        with jax.named_scope(f"w{n}"):
            comm.wait(*[w for w in waits if w not in heard])
            heard.update(waits)
        with jax.named_scope(f"l{n}"):
            for k in ks:
                load(k).wait()
        with jax.named_scope(f"r{n}"):
            run()
        for k in fill.get(n, ()):
            load(k).start()
        comm.sent(plan.when[n] - SLACK)
    comm.sent(float("inf"))


def where_am_i():
    z, y, r = lax.axis_index("depth"), lax.axis_index("col"), lax.axis_index("row")
    return z, y, lax.div(r, 2), lax.rem(r, 2)


def each(shape, fn):
    lead = shape[:-2]
    big = max(range(len(lead)), key=lambda d: lead[d])
    looped = lead[big] >= 8

    def rest(k):
        for ix in itertools.product(*[range(n) if not (looped and d == big) else (k,) for d, n in enumerate(lead)]):
            fn(ix)

    if looped:
        pl.loop(0, lead[big])(rest)
    else:
        rest(None)


def total(refs, ix):
    return functools.reduce(lambda a, b: a + b, [ref[ix] for ref in refs])


def accumulate(dst, others):
    def one(ix):
        dst[ix] = total([dst, *others], ix)

    each(dst.shape, one)


def mm(a, b):
    return jnp.dot(a, b, preferred_element_type=F32)


def mm_l(a, b):
    return lax.dot_general(a, b, (((0,), (0,)), ((), ())), preferred_element_type=F32)


def mm_t(a, b):
    return lax.dot_general(a, b, (((1,), (1,)), ((), ())), preferred_element_type=F32)


def gather_kernel(dims, x_ref, g_ref, w1_ref, w2_ref, xf, gf, w1f, w2f, hid, dpre,
                  bx, bg, bw1, bw2, vw2, u, da, ha, hd, ssem, rsem, lsem, osem, asem):
    nz, ny, nx = dims
    z, y, x, c = where_am_i()
    tk, hb = x_ref.shape
    fc = w2_ref.shape[0]
    hr, fz, half = hb // 2, fc // nz, tk // 2
    plan = Plan(RATES, WINDOW)
    comm = Comm(plan, ssem, rsem)
    ways = (1, -1)

    def idx(axis, d):
        at, n = {"z": (z, nz), "y": (y, ny), "x": (x, nx)}[axis]
        return lax.rem(at + (d % n), n)

    def nb(axis, d):
        i = idx(axis, d)
        return {"z": {"depth": i}, "y": {"col": i}, "x": {"row": 2 * i + c}}[axis]

    partner = {"row": 2 * x + (1 - c)}

    def at(i, size):
        return pl.ds(pl.multiple_of(i * size, size), size)

    def block(full, core, o, part=None):
        rows = at(core, tk) if part is None else pl.ds(pl.multiple_of(core * tk + part * half, half), half)
        return full.at[rows, at(idx("y", o), hb)]

    def wblock(o, core):
        return bw1.at[at(2 * idx("x", o) + core, hr), :]

    def piece(d, o):
        return bw2.at[at(idx("z", d), fz), at(idx("y", o), hb)]

    stores = []

    def store(src, dst):
        copy = pltpu.make_async_copy(src, dst, osem.at[len(stores)])
        stores.append(copy)
        copy.start()

    def mark(key):
        plan.msg(key, ("l", key), 0)
        return key

    loads = {}

    def load(name, src, dst):
        loads[name] = pltpu.make_async_copy(src, dst, lsem.at[len(loads)])
        plan.task(len(loads) / 10, [], [mark(name)], loads[name].wait, COST["mid"])

    load("s", w2_ref.at[at(z, fz), :], vw2)
    load("w", w1_ref.at[:, at(c, fc)], wblock(0, c))
    load("x", x_ref, block(bx, c, 0))
    load("g", g_ref, block(bg, c, 0))
    self_copy = pltpu.make_async_copy(w2_ref.at[at(z, fz), :], piece(0, 0), lsem.at[len(loads)])

    def raw(prio, waits, keys):
        plan.task(prio, waits, keys, lambda: comm.start(*keys), COST["go"], raw=True)

    def passed(prio, wait, keys, key=None):
        plan.task(prio, [wait], [*keys, mark(("in", *wait) if key is None else key)], lambda: comm.start(*keys), COST["go"])

    for o in (1, -1, 2, 0):
        o = o % ny
        to = {"row": 2 * idx("x", o) + c, "col": x}
        comm.msg(("s", o), ("t", 0), lambda: vw2, lambda: piece(0, 0), to, mail=(y, idx("y", o)))
    comm.remote_if[("s", 0)] = x != y
    plan.task(1, ["s"], [("s", o) for o in range(ny)], lambda: comm.start(*[("s", o) for o in range(ny)]), COST["go"])
    whole = {d: [] for d in range(nz)}
    far = nz // 2
    for o in range(ny):
        for w in ways:
            steps = far if (w > 0) == (o % 2 == 0) else far - 1
            for t in range(steps):
                comm.msg(("z", o, w, t), ("z", w), lambda o=o, w=w, t=t: piece(-w * t, o), lambda o=o, w=w, t=t: piece(-w * t, o), nb("z", w))
                nxt = [("z", o, w, t + 1)] if t + 1 < steps else []
                key = ("w2", o, (-w * (t + 1)) % nz)
                passed(4, ("z", o, w, t), nxt, key)
                whole[key[2]].append(key)
        first = [("z", o, w, 0) for w in ways]

        def slice_in(o=o, first=first):
            if o == 0:
                pl.when(x == y)(self_copy.wait)
            comm.start(*first)

        plan.task(3, [("s", o)], [*first, mark(("w2", o, 0))], slice_in, COST["go"])
        whole[0].append(("w2", o, 0))

    comm.msg(("pw",), ("d", 0), lambda: w1_ref.at[:, at(1 - c, fc)], lambda: wblock(0, c), partner)
    raw(1.1, [], [("pw",)])
    w1_in = {0: ["w"], 1: [], -1: [], 2: []}
    for own in (True, False):
        core = c if own else 1 - c
        for w in ways:
            comm.msg(("wa", own, w), ("x", w), lambda core=core: wblock(0, core), lambda core=core: wblock(0, core), nb("x", w))
    raw(1.2, ["w"], [("wa", True, w) for w in ways])
    passed(5, ("pw",), [("wa", False, w) for w in ways])
    w1_in[0].append(("in", "pw"))
    for own, w in ((True, 1), (False, -1)):
        core = c if own else 1 - c
        comm.msg(("wf", w), ("x", w), lambda core=core, w=w: wblock(-w, core), lambda core=core, w=w: wblock(-w, core), nb("x", w))
        passed(6, ("wa", own, w), [("wf", w)])
        passed(6, ("wa", not own, w), [])
        passed(6, ("wf", w), [])
        w1_in[-w] += [("in", "wa", True, w), ("in", "wa", False, w)]
        w1_in[2].append(("in", "wf", w))

    arrived = {}
    for a, (full, name) in enumerate(((bx, "x"), (bg, "g"))):
        arrived[a] = [name]
        for w in ways:
            for p in range(2):
                comm.msg((name, w, p), ("y", w), lambda full=full, p=p: block(full, c, 0, p), lambda full=full, p=p: block(full, c, 0, p), nb("y", w))
            p = 0 if w > 0 else 1
            comm.msg((name, "f", w), ("y", w), lambda full=full, w=w, p=p: block(full, c, -w, p), lambda full=full, w=w, p=p: block(full, c, -w, p), nb("y", w))

        def share(key, o, p, full=full, name=name, a=a):
            comm.msg((name, "d", *key), ("d", 0), lambda: block(full, c, o, p), lambda: block(full, c, o, p), partner)
            passed(20, (name, "d", *key), [])
            arrived[a].append(("in", name, "d", *key))
            return (name, "d", *key)

        plan.task(2 + a, [name], [share((0,), 0, None)], lambda name=name: comm.start((name, "d", 0)), COST["go"])
        for w in ways:
            p = 0 if w > 0 else 1
            for q in range(2):
                keys = [share((-w, q), -w, q)] + ([(name, "f", w)] if q == p else [])
                passed(7, (name, w, q), keys)
                arrived[a].append(("in", name, w, q))
            passed(7, (name, "f", w), [share((2, p), 2, p)])
            arrived[a].append(("in", name, "f", w))
    for n, (name, late) in enumerate(itertools.product("gx", (False, True))):
        raw(1.3 + n / 100, [name], [(name, w, 1 if (w > 0) == late else 0) for w in ways])
    for name, here, src, dst in (("X", arrived[0], bx, xf), ("G", arrived[1], bg, gf), ("W2", [key for d in whole for key in whole[d]], bw2, w2f),
                                 ("W1", [key for o in w1_in for key in w1_in[o]], bw1, w1f)):
        plan.task(9, here, [mark(name)], functools.partial(store, src, dst), COST["go"])

    tile = 256

    e = lax.rem(y - x + ny, ny)
    early = lax.div(e, 2) * (3 - e), 1 + 2 * lax.div(e, 2)
    late = 2, 4 - early[0] - early[1]

    def up(ts, first):
        js = [lax.rem(x + t, nx) for t in ts]

        @pl.loop(0, fc // tile)
        def _(i):
            cols = at(i, tile)
            v = sum(mm(bx[:, at(j, hb)], bw1[at(j, hb), cols]) for j in js)
            u[:, cols] = v if first else u[:, cols] + v

    near = ["w", *[key for key in w1_in[0] + w1_in[1] + w1_in[-1]], *[key for key in arrived[0] if not (key[:3] == ("in", "x", "f") or key[:4] == ("in", "x", "d", 2))]]
    plan.task(30, near, [mark(("U", 0))], functools.partial(up, early, True), COST["U"])
    plan.task(30, [("U", 0), "X", "W1"], [mark(("U", 1))], functools.partial(up, late, False), COST["U"])

    def down(ds):
        spans = [at(idx("z", d), fz) for d in ds]

        @pl.loop(0, 2)
        def _(i):
            rows = at(i, tk)
            v = mm_t(bg[rows, :], jnp.concatenate([bw2[span, :] for span in spans]))
            for n, span in enumerate(spans):
                da[rows, span] = v[:, n * fz:(n + 1) * fz]

    for d in range(far + 1):
        ds = sorted({d, -d % nz})
        plan.task(31, ["G", *[key for e in ds for key in whole[e]]], [mark(("A", d))], functools.partial(down, ds), COST["A"] * len(ds) + 1)

    parts = 2 * tk // tile
    acts = [pltpu.make_async_copy(src, dst, asem.at[n]) for n, (src, dst) in enumerate(((ha, hid), (hd, dpre)))]

    def act():
        @pl.loop(0, parts * (fc // fz))
        def _(i):
            rows, cols = at(lax.rem(i, parts), tile), at(lax.div(i, parts), fz)
            h, vjp = jax.vjp(gelu_fn, u[rows, cols])
            ha[rows, cols] = h.astype(BF16)
            hd[rows, cols] = vjp(da[rows, cols])[0].astype(BF16)

        for copy in acts:
            copy.start()

    plan.task(32, [("U", 1), *[("A", d) for d in range(far + 1)]], [], act, COST["act"])

    order = plan.order()
    for copy in loads.values():
        copy.start()
    pl.when(x == y)(self_copy.start)

    barrier = pltpu.get_barrier_semaphore()

    def tell(to):
        pl.semaphore_signal(barrier, inc=1, device_id=to, device_id_type=MESH)

    for to in (*[nb(axis, d) for axis in "zyx" for d in ways], partner):
        tell(to)
    for o in range(1, ny):
        tell({"row": 2 * y + c, "col": idx("y", o)})
    pl.when(x != y)(lambda: tell({"row": 2 * y + c, "col": y}))
    pl.semaphore_wait(barrier, 6 + ny + jnp.where(x != y, 1, 0))
    run_tasks(plan, comm, order)
    for copy in [*stores, *acts]:
        copy.wait()


def gather(dims, tok, grad, up, down):
    tk, hb = tok.shape
    fc = down.shape[0]
    nz, ny, nx = dims
    sds, vm = jax.ShapeDtypeStruct, pltpu.VMEM
    tokens, first, second, mid = (2 * tk, ny * hb), (nx * hb, fc), (fc, ny * hb), (2 * tk, fc)
    return pl.pallas_call(
        functools.partial(gather_kernel, dims),
        out_shape=[sds(shape, BF16) for shape in (tokens, tokens, first, second, mid, mid)],
        in_specs=[ANY] * 4,
        out_specs=[ANY] * 6,
        scratch_shapes=[
            *[vm(shape, BF16) for shape in (tokens, tokens, first, second, (fc // nz, hb))],
            vm(mid, F32),
            vm(mid, F32),
            vm(mid, BF16),
            vm(mid, BF16),
            pltpu.SemaphoreType.DMA((80,)),
            pltpu.SemaphoreType.DMA((80,)),
            pltpu.SemaphoreType.DMA((5,)),
            pltpu.SemaphoreType.DMA((9,)),
            pltpu.SemaphoreType.DMA((2,)),
        ],
        compiler_params=pltpu.CompilerParams(collective_id=0, has_side_effects=True, vmem_limit_bytes=VMEM_LIMIT),
        name="gather",
    )(tok, grad, up, down)


def reduce_kernel(dims, tok, grad, up, down, hid, dpre,
                  y_out, dx_out, g1_out, g2_out, dwp, yp, wx1, wx2, hx, dx, *scratch):
    nz, ny, nx = dims
    z, y, x, c = where_am_i()
    hb = y_out.shape[-1]
    tk = tok.shape[0] // 2
    hr = hb // 2
    fc = hid.shape[1]
    nu = fc // (nz * 8)
    sgn = (1, -1)
    scratch = list(scratch)

    def grab(n):
        return [scratch.pop(0) for _ in range(n)]

    nc = len(CHUNKS)
    xbuf, zbuf, tbuf = grab(nc), grab(nc), grab(nc)
    o1, o2, yr, yo, lhs, par, tmp = grab(7)
    pools = grab(5)
    ssem, rsem, lsem, osem, isem, tsem = grab(6)
    P_X, P_Z, P_Y, P_R, P_W = range(5)

    plan = Plan(RATES, WINDOW)
    comm = Comm(plan, ssem, rsem)

    def idx(axis, d):
        at, n = {"z": (z, nz), "y": (y, ny), "x": (x, nx)}[axis]
        return lax.rem(at + (d % n), n)

    def nb(axis, d):
        i = idx(axis, d)
        return {"z": {"depth": i}, "y": {"col": i}, "x": {"row": 2 * i + c}}[axis]

    partner = {"row": 2 * x + (1 - c)}
    across = {"row": 2 * y + c, "col": x}

    def hcol(j):
        return pl.ds(pl.multiple_of(j * hb, hb), hb)

    staged, stores, place = [], [], {}

    def stage(pool, src, marks=(), n=None):
        staged.append((pool, src, tuple(marks), n))
        return len(staged) - 1

    def slot(k):
        return place[k][0]

    def mark(key):
        plan.msg(key, ("l", key), 0)
        return key

    def chain(key, axis, n, s, buf, src, pool, marks, prio, end, end_sends, units=None):
        far, near = n // 2, n // 2 - 1
        for t in range(far):
            comm.msg((key, "F", t), (axis, s), (lambda: src(far * s)) if t == 0 else (lambda t=t: buf.at[t - 1]), lambda t=t: buf.at[t], nb(axis, s))
        for t in range(near):
            comm.msg((key, "N", t), (axis, -s), (lambda: src(-near * s)) if t == 0 else (lambda t=t: buf.at[far + t - 1]), lambda t=t: buf.at[far + t], nb(axis, -s))

        def own(rel):
            return [] if pool is None else [stage(pool, lambda: src(rel), marks(rel), units)]

        def mid(name, t, at, rel):
            ks = own(rel)

            def run():
                accumulate(buf.at[at], [slot(ks[0]) if ks else src(rel)])
                comm.start((key, name, t + 1))

            plan.task(prio, [(key, name, t), *marks(rel)], [(key, name, t + 1)], run, COST["mid"], stage=ks)

        for t in range(far - 1):
            mid("F", t, t, (far - 1 - t) * s)
        for t in range(near - 1):
            mid("N", t, far + t, -(near - 1 - t) * s)
        ks = own(0)
        last = [buf.at[far - 1], buf.at[far + near - 1]]
        plan.task(prio, [(key, "F", far - 1), (key, "N", near - 1), *marks(0)], end_sends,
                  lambda: end(last, slot(ks[0]) if ks else src(0)), COST["fin"], stage=ks)
        return [(key, "F", 0), (key, "N", 0)]

    def raw(prio, marks, keys):
        plan.task(prio, marks, keys, lambda: comm.start(*keys), COST["go"], raw=True)

    def spread(key, s, region, finish):
        far, near = nz // 2, nz // 2 - 1
        for name, count, d in (("GF", far, s), ("GN", near, -s)):
            for t in range(count):
                def ref(t=t, d=d):
                    return region(idx("z", -t * d))
                comm.msg((key, name, t), ("z", d), ref, ref, nb("z", d))
        for name, count in (("GF", far), ("GN", near)):
            for t in range(count - 1):
                plan.task(SPREAD, [(key, name, t)], [(key, name, t + 1)], lambda name=name, t=t: comm.start((key, name, t + 1)), COST["go"], raw=GATED)
        plan.task(30, [(key, "GF", far - 1), (key, "GN", near - 1)], [], finish, COST["go"])
        return [(key, "GF", 0), (key, "GN", 0)]

    def store(src, dst):
        copy = pltpu.make_async_copy(src, dst, osem.at[len(stores)])
        stores.append(copy)
        copy.start()

    def none(rel):
        return ()

    for i, (a, first_axis, sigma, u, n, prio) in enumerate(CHUNKS):
        s = sgn[sigma]

        def done(o, a=a, u=u, n=n):
            return [("D", a, o % nx, v) for v in range(u, u + n)]

        if a == 0:
            def region(k, u=u, n=n):
                return o1.at[:, pl.ds(u, n), k]

            go = spread(("g", i), s, region, lambda u=u, n=n: store(o1.at[:, pl.ds(u, n)], g1_out.at[:, pl.ds(u, n)]))
            over = ("sw", i)
            comm.msg(over, ("d", 0), lambda i=i: tbuf[i], lambda u=u, n=n: o1.at[c, pl.ds(u, n), z], partner)

            def end(last, own, i=i, u=u, n=n, over=over):
                mine = pl.ds(pl.multiple_of(c * hr, hr), hr)
                other = pl.ds(pl.multiple_of((1 - c) * hr, hr), hr)
                for m in range(n):
                    tbuf[i][m] = total([own, *last], (m, slice(None), other))
                comm.start(over)
                for m in range(n):
                    o1[c, u + m, z] = total([own, *last], (m, slice(None), mine))
        else:
            def region(k, u=u, n=n):
                return o2.at[pl.ds(u, n), k]

            go = spread(("g", i), s, region, lambda u=u, n=n: store(o2.at[pl.ds(u, n)], g2_out.at[pl.ds(u, n)]))
            over = ("tr", i)
            comm.msg(over, ("t", 0), lambda i=i: tbuf[i], lambda region=region: region(z), across)
            comm.remote_if[over] = x != y

            def end(last, own, i=i, u=u, n=n, over=over):
                for m in range(n):
                    tbuf[i][m] = total([own, *last], m)
                comm.start(over)

                @pl.when(x == y)
                def _():
                    for m in range(n):
                        o2[u + m, z] = tbuf[i][m]

        plan.task(SPREAD, [over], go, lambda go=go: comm.start(*go), COST["go"], raw=GATED)
        if first_axis == "x":
            res = xbuf[i].at[nx // 2 - 1]
            pieces = functools.partial(lambda res, rel: res.at[:, idx("z", rel)], res)
            raws = chain(("z", i), "z", nz, s, zbuf[i], pieces, None, none, 5, end, [over])

            def x_end(last, own, raws=raws):
                accumulate(last[0], [last[1], own])
                comm.start(*raws)

            raws = chain(("x", i), "x", nx, s, xbuf[i], lambda rel, a=a, u=u, n=n: dwp.at[a, pl.ds(u, n), :, :, hcol(idx("x", rel))],
                         P_X, lambda rel, done=done: done(rel), 10, x_end, raws, n)
            raw(11 + prio / 100, done(2) + done(-s), raws)
        else:
            res = zbuf[i].at[nz // 2 - 1]
            raws = chain(("x", i), "x", nx, s, xbuf[i], lambda rel, res=res: res.at[:, :, hcol(idx("x", rel))], None, none, 8, end, [over])

            def z_end(last, own, raws=raws):
                accumulate(last[0], [last[1], own])
                comm.start(*raws)

            all_done = [m for o in range(nx) for m in done(o)]
            raws = chain(("z", i), "z", nz, s, zbuf[i], lambda rel, a=a, u=u, n=n: dwp.at[a, pl.ds(u, n), idx("z", rel)],
                         P_Z, lambda rel, all_done=all_done: all_done, 9, z_end, raws, n)
            raw(11 + prio / 100, all_done, raws)

    groups = yo.shape[1]
    for a, out in enumerate((y_out, dx_out)):
        for sigma in range(2):
            s = sgn[sigma]
            half = pl.ds(sigma * (groups // 2), groups // 2)

            def y_end(last, own, a=a, half=half, sigma=sigma, out=out):
                def one(ix):
                    yo[(a, sigma * (groups // 2) + ix[0], ix[1])] = total([own, *last], ix).astype(BF16)

                each(own.shape, one)
                store(yo.at[a, half], out.at[half])

            raws = chain(("y", a, sigma), "y", ny, s, yr.at[a, sigma], lambda rel, a=a, half=half: yp.at[a, half, :, :, hcol(idx("y", rel))],
                         P_Y, lambda rel, a=a: [("Y", a, rel % ny)], 12, y_end, [])
            raw(11, [("Y", a, 2), ("Y", a, -s % ny)], raws)

    tile = 256

    def rows(o):
        return pl.ds(pl.multiple_of(idx("y", o) * hb, hb), hb)

    def arrive(key, prio=6):
        plan.msg(("got", *key), ("s", key), 0)
        plan.task(prio, [key], [("got", *key)], lambda: None, COST["go"])
        return ("got", *key)

    lhs_loads = [pltpu.make_async_copy(src, lhs.at[n], isem.at[n]) for n, src in enumerate((hid, dpre))]
    for n in (0, 1):
        plan.task(0, [], [mark(("T", n))], lhs_loads[n].wait, 0.3)

    others = pl.ds(pl.multiple_of((1 - c) * tk, tk), tk)
    own_rows = pl.ds(pl.multiple_of(c * tk, tk), tk)
    par_loads = []
    for n, (src, box) in enumerate(((hid, hx), (dpre, dx))):
        comm.msg(("hx", n), ("d", 0), lambda src=src: src.at[others], lambda box=box: box, partner)
        raw(1, [], [("hx", n)])
        par_loads.append(pltpu.make_async_copy(box, par.at[n], isem.at[2 + n]))
        plan.task(6, [("hx", n)], [mark(("P", n))], par_loads[n].start, 0.02)
    for a, o in Y_ORDER:
        if a == 0:
            comm.msg(("w", a, o), ("d", 0), lambda o=o: down.at[:, hcol(idx("y", o))], lambda o=o: wx2.at[:, hcol(idx("y", o))], partner)
        else:
            comm.msg(("w", a, o), ("d", 0), lambda o=o: up.at[rows(o)], lambda o=o: wx1.at[rows(o)], partner)
        raw(2, [], [("w", a, o)])

    par_seen = set()
    last_of, b = {}, 1
    for n, job in enumerate(JOBS):
        opens, closes = job[0] == "D" or job[3] == 0, job[0] == "D" or job[3] == 1
        b = 1 - b if opens else b
        keys = [("Y", job[1], job[2])] if job[0] == "Y" else [("D", job[1], job[2] % nx, v) for v in range(job[3], job[3] + job[4])]
        span = pl.ds(0, yo.shape[1] if job[0] == "Y" else job[4])
        waits = [("C", n - 1)] if n else []
        if opens and b in last_of:
            waits.append(("S", last_of[b]))
        if job[0] == "D":
            _, a, o, u, n_u = job
            waits.append(("T", 1 - a))
            ks = [stage(P_R, lambda a=a, o=o: (tok, grad)[a].at[:, hcol(idx("x", o))])]

            def value(cols, a=a, u=u, n_u=n_u, ks=ks):
                return mm_l(lhs[1 - a, :, u * nz * 8:(u + n_u) * nz * 8], slot(ks[0])[:, cols])

            dst = functools.partial(lambda a, o, u, n_u: dwp.at[a, pl.ds(u, n_u), :, :, hcol(idx("x", o))], a, o, u, n_u)
            cost = COST["D"][n_u]
        else:
            _, a, o, h = job
            waits.append(("T", a))
            marks = []
            if h:
                marks = [arrive(("w", a, o))]
                waits += [("P", a), *marks]
            if a == 0:
                ks = [stage(P_R, lambda o=o, w=(down, wx2)[h]: w.at[:, hcol(idx("y", o))], marks)]
            else:
                ks = [stage(P_W, lambda o=o, w=(up, wx1)[h]: w.at[rows(o)], marks)]

            def value(cols, a=a, h=h, ks=ks):
                left = par[a] if h else lhs[a, own_rows, :]
                return mm(left, slot(ks[0])[:, cols]) if a == 0 else mm_t(left, slot(ks[0])[cols, :])

            dst = functools.partial(lambda a, o: yp.at[a, :, :, :, hcol(idx("y", o))], a, o)
            cost = COST["Y"]

        def save(b=b, dst=dst, span=span):
            return pltpu.make_async_copy(tmp.at[b, span], dst(), tsem.at[b])

        def run(b=b, value=value, save=save, job=job, span=span, opens=opens, closes=closes):
            if job[0] == "Y" and job[3] and job[1] not in par_seen:
                par_loads[job[1]].wait()
                par_seen.add(job[1])

            @pl.loop(0, hb // tile)
            def _(t):
                cols = pl.ds(pl.multiple_of(t * tile, tile), tile)
                v = value(cols).reshape((span.size,) + tmp.shape[2:4] + (tile,))
                tmp[b, span, :, :, cols] = v if opens else tmp[b, span, :, :, cols] + v

            if closes:
                save().start()

        sends = [mark(("C", n))]
        if closes:
            plan.msg(("W", n), ("s", n), 0)
            sends.append(("W", n))
            last_of[b] = n
            plan.task(2, [("W", n)], [mark(("S", n)), *[mark(key) for key in keys]], lambda save=save: save().wait(), 0.03)
        plan.task(40, waits, sends, run, cost, stage=ks)

    order = plan.order()

    at = {}
    for n, i in enumerate(order):
        for w in plan.tasks[i][2]:
            at[w] = n
    uses = {p: [] for p in range(len(pools))}
    user = {}
    for n, i in enumerate(order):
        for k in plan.tasks[i][5]:
            uses[staged[k][0]].append(k)
            user[k] = n
    lbase, fill = 0, {}
    for p, ks in uses.items():
        depth = pools[p].shape[0]
        for n, k in enumerate(ks):
            box = pools[p].at[n % depth] if staged[k][3] is None else pools[p].at[n % depth, pl.ds(0, staged[k][3])]
            place[k] = (box, lsem.at[lbase + n % depth])
            when = -1 if n < depth else user[ks[n - depth]]
            for w in staged[k][2]:
                when = max(when, at[w])
            fill.setdefault(when, []).append(k)
        lbase += depth

    def load(k):
        return pltpu.make_async_copy(staged[k][1](), *place[k])

    for n in LHS_ORDER:
        lhs_loads[n].start()
    for k in fill.get(-1, ()):
        load(k).start()

    barrier = pltpu.get_barrier_semaphore()

    def tell(to):
        pl.semaphore_signal(barrier, inc=1, device_id=to, device_id_type=MESH)

    peers = [*[nb(axis, d) for axis in "zyx" for d in sgn], partner]
    for to in peers:
        tell(to)
    pl.when(x != y)(lambda: tell(across))
    pl.semaphore_wait(barrier, len(peers) + jnp.where(x != y, 1, 0))

    run_tasks(plan, comm, order, load, fill)
    for copy in stores:
        copy.wait()


def reduce(dims, tok, grad, up, down, hid, dpre):
    nz, ny, nx = dims
    rows2, hh = tok.shape
    fc = hid.shape[1]
    tk, hb = rows2 // 2, hh // ny
    hr = hb // 2
    nu = fc // (nz * SUB)
    g = tk // (SUB * SUB)
    vm = pltpu.VMEM

    def per(shape):
        return [vm(shape(axis, n), F32) for _, axis, _, _, n, *_ in CHUNKS]

    def fin(shape):
        return [vm((n, SUB, hr if a == 0 else hb), F32) for a, _, _, _, n, *_ in CHUNKS]

    n0 = max(chunk[4] for chunk in CHUNKS)
    scratch = [
        *per(lambda axis, n: (nx - 1, n, nz, SUB, hb) if axis == "x" else (nx - 1, n, SUB, hb)),
        *per(lambda axis, n: (nz - 1, n, SUB, hb) if axis == "x" else (nz - 1, n, SUB, hh)),
        *fin(0),
        vm((2, nu, nz, SUB, hr), F32),
        vm((nu, nz, SUB, hb), F32),
        vm((2, 2, ny - 1, g // 2, SUB, SUB, hb), F32),
        vm((2, g, SUB, SUB, hb), BF16),
        vm((2, rows2, fc), BF16),
        vm((2, tk, fc), BF16),
        vm((2, g, SUB, SUB, hb), F32),
        vm((3, n0, nz, SUB, hb), F32),
        vm((6, n0, SUB, hh), F32),
        vm((2, g // 2, SUB, SUB, hb), F32),
        vm((3, rows2, hb), BF16),
        vm((3, hb, fc), BF16),
        pltpu.SemaphoreType.DMA((340,)),
        pltpu.SemaphoreType.DMA((340,)),
        pltpu.SemaphoreType.DMA((18,)),
        pltpu.SemaphoreType.DMA((24,)),
        pltpu.SemaphoreType.DMA((6,)),
        pltpu.SemaphoreType.DMA((2,)),
    ]
    sds = jax.ShapeDtypeStruct
    outs = pl.pallas_call(
        functools.partial(reduce_kernel, dims),
        out_shape=[
            sds((g, SUB, SUB, hb), BF16),
            sds((g, SUB, SUB, hb), BF16),
            sds((2, nu, nz, SUB, hr), F32),
            sds((nu, nz, SUB, hb), F32),
            sds((2, nu, nz, SUB, hh), F32),
            sds((2, g, SUB, SUB, hh), F32),
            sds(up.shape, BF16),
            sds(down.shape, BF16),
            sds((tk, fc), BF16),
            sds((tk, fc), BF16),
        ],
        in_specs=[ANY] * 6,
        out_specs=[ANY] * 10,
        scratch_shapes=scratch,
        compiler_params=pltpu.CompilerParams(collective_id=1, has_side_effects=True, vmem_limit_bytes=VMEM_LIMIT),
        name="reduce",
    )(tok, grad, up, down, hid, dpre)
    y, dx, g1, g2 = outs[:4]
    return finish(y.reshape(tk, hb), dx.reshape(tk, hb), g1.reshape(2 * fc, hr), g2.reshape(fc, hb))


def finish_kernel(*refs):
    *arrays, turned, isem, osem = refs
    n, parts = isem.shape
    ins, outs, boxes = (arrays[k * n:(k + 1) * n] for k in range(3))

    def span(ref, k):
        size = ref.shape[0] // parts
        return pl.ds(k * size, size)

    def fetch(i, k):
        return pltpu.make_async_copy(ins[i].at[span(ins[i], k)], boxes[i].at[span(ins[i], k)], isem.at[i, k])

    def put(i, k):
        if i == 0:
            cols = span(ins[i], k)
            return pltpu.make_async_copy(turned.at[:, cols], outs[i].at[:, cols], osem.at[i, k])
        return pltpu.make_async_copy(boxes[i].at[span(ins[i], k)], outs[i].at[span(ins[i], k)], osem.at[i, k])

    todo = list(itertools.product(range(n), range(parts)))
    for i, k in todo:
        fetch(i, k).start()
    for i, k in todo:
        fetch(i, k).wait()
        if i == 0:
            rows = span(ins[i], k)
            turned[:, rows] = boxes[i][rows, :].T
        put(i, k).start()
    for i, k in todo:
        put(i, k).wait()


def finish(y, dx, g1, g2):
    ins = (g1, g2, y, dx)
    turned = jax.ShapeDtypeStruct(g1.shape[::-1], F32)
    parts = 4
    out = pl.pallas_call(
        finish_kernel,
        out_shape=[turned, *[jax.ShapeDtypeStruct(v.shape, v.dtype) for v in ins[1:]]],
        in_specs=[ANY] * len(ins),
        out_specs=[ANY] * len(ins),
        scratch_shapes=[*[pltpu.VMEM(v.shape, v.dtype) for v in ins], pltpu.VMEM(turned.shape, F32), *[pltpu.SemaphoreType.DMA((len(ins), parts))] * 2],
        compiler_params=pltpu.CompilerParams(vmem_limit_bytes=VMEM_LIMIT),
        name="finish",
    )(*ins)
    return out[2], out[3], out[0], out[1]


def solution(mesh):
    act_spec = P(("depth", "row"), "col")
    weight_spec = P("row", "col")
    dims = (mesh.shape["depth"], mesh.shape["col"], mesh.shape["row"] // 2)

    def local_block(tok_blk, up_blk, down_blk, grad_blk):
        return reduce(dims, *gather(dims, tok_blk, grad_blk, up_blk, down_blk))

    return jax.shard_map(local_block, mesh=mesh, in_specs=(act_spec, weight_spec, weight_spec, act_spec), out_specs=(act_spec, act_spec, weight_spec, weight_spec), check_vma=False)
```

```python
import functools
import itertools

import jax
import jax.numpy as jnp
from jax import lax
from jax.experimental import pallas as pl
from jax.experimental.pallas import tpu as pltpu
from jax.sharding import PartitionSpec as P

MESH = pl.DeviceIdType.MESH
ANY = pl.BlockSpec(memory_space=pl.ANY)
F32 = jnp.float32
SUB = 8
BF16 = jnp.bfloat16

TOP = (12, 10)
UNITS = 16


def chunk_list():
    def run(a, axis, lo, hi, rank):
        return [(a, axis, k % 2, u, min(2, hi - u), rank + k) for k, u in enumerate(range(lo, hi, 2))]

    first, last = TOP
    return [*run(1, "z", last, UNITS, 0), *run(0, "z", first, UNITS, 20), *run(0, "x", 0, first, 0), *run(1, "x", 0, last - 1, 6), (1, "x", 1, last - 1, 1, 11)]


CHUNKS = chunk_list()
FAR_FIRST = (2, 1, 3, 0)
Y_ORDER = [(a, o) for a in range(2) for o in FAR_FIRST]


def job_list():
    def block(a, lo, hi):
        return [("D", a, o, u, min(4, hi - u)) for u in range(lo, hi, 4) for o in FAR_FIRST]

    z_first = block(1, TOP[1], UNITS)
    rest = block(0, 0, TOP[0]) + block(1, 0, TOP[1])
    both = rest[:3] + z_first[:4] + rest[3:4] + z_first[4:] + rest[4:]
    half = len(both) // 2
    both[half:half] = block(0, TOP[0], UNITS)
    cut = int(0.7 * len(both))
    jobs, both = both[:cut], both[cut:]
    out = [[("Y", a, o, 0), ("Y", a, o, 1)] for a, o in Y_ORDER]
    while both or out:
        jobs, both = jobs + both[:3], both[3:]
        jobs += out.pop(0) if out else []
    return jobs


JOBS = job_list()
COST = {"D": (0.5, 0.15), "Y": 1.2, "fin": 0.1, "go": 0.03, "U": 4.0, "A": 0.8, "act": 3.0}
SLACK = 20.0
VMEM_LIMIT = 66_500_000


def gelu_fn(pre_act):
    return jax.nn.gelu(pre_act, approximate=True)


class Plan:
    def __init__(self, rates, window):
        self.rates, self.window = rates, window
        self.tasks, self.size, self.link = [], {}, {}

    def msg(self, key, link, nbytes):
        self.size[key], self.link[key] = nbytes, link

    def task(self, prio, waits, sends, run, cost=0.3, stage=(), raw=False):
        self.tasks.append((prio, tuple(waits), tuple(sends), run, cost, tuple(stage), raw))

    def order(self):
        free, arrive, out = {}, {}, []
        self.when, self.arrive = [], arrive
        now, left = 2.5, list(range(len(self.tasks)))
        while left:
            best = None
            for i in left:
                prio, waits, sends, _, _, _, raw = self.tasks[i]
                if any(w not in arrive for w in waits):
                    continue
                ready = max([arrive[w] for w in waits], default=0.0)
                if raw:
                    ready = max([ready] + [free.get(self.link[s], 0.0) - self.window for s in sends])
                key = (max(ready, now), prio, i)
                if best is None or key < best:
                    best = key
            at, _, i = best
            left.remove(i)
            out.append(i)
            now = at + self.tasks[i][4]
            self.when.append(now)
            for s in self.tasks[i][2]:
                rate, lat = self.rates[self.link[s][0]]
                took = self.size[s] / rate
                if self.link[s][0] in "to":
                    share = 0.5 if self.link[s][0] == "t" else 1.5
                    ways = [(axis, d) for axis in "xy" for d in (1, -1)]
                    done = max(now, *[free.get(way, 0.0) for way in ways]) + took
                    for way in ways:
                        free[way] = max(now, free.get(way, 0.0)) + took * share
                else:
                    done = max(now, free.get(self.link[s], 0.0)) + took
                    free[self.link[s]] = done
                arrive[s] = done + lat
        self.end = max(now, max(arrive.values()))
        return out


RATES = {axis: (45e3, 2.2) for axis in "xyz"}
RATES.update(d=(450e3, 3.0), t=(45e3, 5.0), o=(45e3, 7.0), l=(1e12, 0.0), s=(1e12, 2.0))
WINDOW = 8.0


class Comm:
    def __init__(self, plan, ssem, rsem):
        self.plan, self.ssem, self.rsem = plan, ssem, rsem
        self.make, self.meet, self.slot, self.remote_if, self.groups, self.grouped, self.flying = {}, {}, {}, {}, {}, set(), []

    def msg(self, key, link, src, dst, to, mail=None, group=None):
        i = len(self.slot)
        self.slot[key] = i
        there, here = mail or (i, i)
        name, ref = group or (key, None)
        g, _, _ = self.groups.setdefault(name, (len(self.groups), ref, to))
        if group:
            self.grouped.add(key)

        def make(r):
            return pltpu.make_async_remote_copy(
                src_ref=src(), dst_ref=dst(), send_sem=self.ssem.at[g], recv_sem=self.rsem.at[r], device_id=to, device_id_type=MESH)

        self.make[key] = lambda: make(there)
        self.meet[key] = lambda: make(here)
        shape = src().shape
        nbytes = functools.reduce(lambda a, b: a * b, shape, 1) * src().dtype.itemsize
        self.plan.msg(key, link, nbytes)

    def each(self, keys, make, act):
        for key in keys:
            if key in self.remote_if:
                pl.when(self.remote_if[key])(lambda key=key: act(make[key]()))
            elif key in make:
                act(make[key]())

    def start(self, *keys):
        self.flying.extend(key for key in keys if key not in self.grouped)
        self.each(keys, self.make, lambda copy: copy.start())

    def finish(self):
        self.sent(float("inf"))
        for g, ref, to in self.groups.values():
            if ref is not None:
                pltpu.make_async_remote_copy(src_ref=ref, dst_ref=ref, send_sem=self.ssem.at[g], recv_sem=self.rsem.at[g], device_id=to, device_id_type=MESH).wait_send()

    def wait(self, *keys):
        self.each(keys, self.meet, lambda copy: copy.wait_recv())

    def sent(self, before):
        keys = [key for key in self.flying if self.plan.arrive[key] <= before]
        self.flying = [key for key in self.flying if self.plan.arrive[key] > before]
        self.each(keys, self.make, lambda copy: copy.wait_send())


def run_tasks(plan, comm, order, ready, load=None, fill={}):
    heard = set()
    for n, i in enumerate(order):
        _, waits, sends, run, _, ks, _ = plan.tasks[i]
        if ready and any(key in comm.make for key in sends):
            ready()
            ready = None
        with jax.named_scope(f"w{n}"):
            comm.wait(*[w for w in waits if w not in heard])
            heard.update(waits)
        with jax.named_scope(f"l{n}"):
            for k in ks:
                load(k).wait()
        with jax.named_scope(f"r{n}"):
            run()
        for k in fill.get(n, ()):
            load(k).start()
        comm.sent(plan.when[n] - SLACK)
    comm.finish()


def where_am_i():
    z, y, r = lax.axis_index("depth"), lax.axis_index("col"), lax.axis_index("row")
    return z, y, lax.div(r, 2), lax.rem(r, 2)


def each(shape, fn):
    lead = shape[:-2]
    big = max(range(len(lead)), key=lambda d: lead[d])
    looped = lead[big] >= 8

    def rest(k):
        for ix in itertools.product(*[range(n) if not (looped and d == big) else (k,) for d, n in enumerate(lead)]):
            fn(ix)

    if looped:
        pl.loop(0, lead[big])(rest)
    else:
        rest(None)


def total(refs, ix):
    return functools.reduce(lambda a, b: a + b, [ref[ix] for ref in refs])


def accumulate(dst, others):
    def one(ix):
        dst[ix] = total([dst, *others], ix)

    each(dst.shape, one)


def mm(a, b):
    return jnp.dot(a, b, preferred_element_type=F32)


def mm_l(a, b):
    return lax.dot_general(a, b, (((0,), (0,)), ((), ())), preferred_element_type=F32)


def mm_t(a, b):
    return lax.dot_general(a, b, (((1,), (1,)), ((), ())), preferred_element_type=F32)


def gather_kernel(dims, x_ref, g_ref, w1_ref, w2_ref, xf, gf, w1f, w2f, hid, dpre,
                  bx, bg, bw1, bw2, vw2, u, da, ha, hd, ssem, rsem, lsem, osem, asem):
    nz, ny, nx = dims
    z, y, x, c = where_am_i()
    tk, hb = x_ref.shape
    fc = w2_ref.shape[0]
    hr, fz, half = hb // 2, fc // nz, tk // 2
    plan = Plan(RATES, WINDOW)
    comm = Comm(plan, ssem, rsem)
    ways = (1, -1)

    def idx(axis, d):
        at, n = {"z": (z, nz), "y": (y, ny), "x": (x, nx)}[axis]
        return lax.rem(at + (d % n), n)

    def nb(axis, d):
        i = idx(axis, d)
        return {"z": {"depth": i}, "y": {"col": i}, "x": {"row": 2 * i + c}}[axis]

    partner = {"row": 2 * x + (1 - c)}

    def at(i, size):
        return pl.ds(pl.multiple_of(i * size, size), size)

    def block(full, core, o, part=None):
        rows = at(core, tk) if part is None else pl.ds(pl.multiple_of(core * tk + part * half, half), half)
        return full.at[rows, at(idx("y", o), hb)]

    def wblock(o, core):
        return bw1.at[at(2 * idx("x", o) + core, hr), :]

    def piece(d, o):
        return bw2.at[at(idx("z", d), fz), at(idx("y", o), hb)]

    stores = []

    def store(src, dst):
        copy = pltpu.make_async_copy(src, dst, osem.at[len(stores)])
        stores.append(copy)
        copy.start()

    def mark(key):
        plan.msg(key, ("l", key), 0)
        return key

    loads = {}

    def load(name, src, dst):
        loads[name] = pltpu.make_async_copy(src, dst, lsem.at[len(loads)])
        plan.task(len(loads) / 10, [], [mark(name)], loads[name].wait, COST["go"])

    load("s", w2_ref.at[at(z, fz), :], vw2)
    load("w", w1_ref.at[:, at(c, fc)], wblock(0, c))
    load("x", x_ref, block(bx, c, 0))
    load("g", g_ref, block(bg, c, 0))
    self_copy = pltpu.make_async_copy(w2_ref.at[at(z, fz), :], piece(0, 0), lsem.at[len(loads)])

    def raw(prio, waits, keys):
        plan.task(prio, waits, keys, lambda: comm.start(*keys), COST["go"], raw=True)

    def passed(prio, wait, keys, key=None):
        plan.task(prio, [wait], [*keys, mark(("in", *wait) if key is None else key)], lambda: comm.start(*keys), COST["go"])

    for o in (1, -1, 2, 0):
        o = o % ny
        to = {"row": 2 * idx("x", o) + c, "col": x}
        comm.msg(("s", o), ("t", 0), lambda: vw2, lambda: piece(0, 0), to, mail=(y, idx("y", o)))
    comm.remote_if[("s", 0)] = x != y
    plan.task(1, ["s"], [("s", o) for o in range(ny)], lambda: comm.start(*[("s", o) for o in range(ny)]), COST["go"])
    whole = {d: [] for d in range(nz)}
    far = nz // 2
    for o in range(ny):
        for w in ways:
            steps = far if (w > 0) == (o % 2 == 0) else far - 1
            for t in range(steps):
                comm.msg(("z", o, w, t), ("z", w), lambda o=o, w=w, t=t: piece(-w * t, o), lambda o=o, w=w, t=t: piece(-w * t, o), nb("z", w))
                nxt = [("z", o, w, t + 1)] if t + 1 < steps else []
                key = ("w2", o, (-w * (t + 1)) % nz)
                passed(4, ("z", o, w, t), nxt, key)
                whole[key[2]].append(key)
        first = [("z", o, w, 0) for w in ways]

        def slice_in(o=o, first=first):
            if o == 0:
                pl.when(x == y)(self_copy.wait)
            comm.start(*first)

        plan.task(3, [("s", o)], [*first, mark(("w2", o, 0))], slice_in, COST["go"])
        whole[0].append(("w2", o, 0))

    comm.msg(("pw",), ("d", 0), lambda: w1_ref.at[:, at(1 - c, fc)], lambda: wblock(0, c), partner)
    raw(1.1, [], [("pw",)])
    w1_in = {0: ["w"], 1: [], -1: [], 2: []}
    for own in (True, False):
        core = c if own else 1 - c
        for w in ways:
            comm.msg(("wa", own, w), ("x", w), lambda core=core: wblock(0, core), lambda core=core: wblock(0, core), nb("x", w))
    raw(1.2, ["w"], [("wa", True, w) for w in ways])
    passed(5, ("pw",), [("wa", False, w) for w in ways])
    w1_in[0].append(("in", "pw"))
    for own, w in ((True, 1), (False, -1)):
        core = c if own else 1 - c
        comm.msg(("wf", w), ("x", w), lambda core=core, w=w: wblock(-w, core), lambda core=core, w=w: wblock(-w, core), nb("x", w))
        passed(6, ("wa", own, w), [("wf", w)])
        passed(6, ("wa", not own, w), [])
        passed(6, ("wf", w), [])
        w1_in[-w] += [("in", "wa", True, w), ("in", "wa", False, w)]
        w1_in[2].append(("in", "wf", w))

    arrived = {}
    for a, (full, name) in enumerate(((bx, "x"), (bg, "g"))):
        arrived[a] = [name]
        for w in ways:
            for p in range(2):
                comm.msg((name, w, p), ("y", w), lambda full=full, p=p: block(full, c, 0, p), lambda full=full, p=p: block(full, c, 0, p), nb("y", w))
            p = 0 if w > 0 else 1
            comm.msg((name, "f", w), ("y", w), lambda full=full, w=w, p=p: block(full, c, -w, p), lambda full=full, w=w, p=p: block(full, c, -w, p), nb("y", w))

        def share(key, o, p, full=full, name=name, a=a):
            comm.msg((name, "d", *key), ("d", 0), lambda: block(full, c, o, p), lambda: block(full, c, o, p), partner)
            passed(20, (name, "d", *key), [])
            arrived[a].append(("in", name, "d", *key))
            return (name, "d", *key)

        plan.task(2 + a, [name], [share((0,), 0, None)], lambda name=name: comm.start((name, "d", 0)), COST["go"])
        for w in ways:
            p = 0 if w > 0 else 1
            for q in range(2):
                keys = [share((-w, q), -w, q)] + ([(name, "f", w)] if q == p else [])
                passed(7, (name, w, q), keys)
                arrived[a].append(("in", name, w, q))
            passed(7, (name, "f", w), [share((2, p), 2, p)])
            arrived[a].append(("in", name, "f", w))
    for n, (name, late) in enumerate(itertools.product("gx", (False, True))):
        raw(1.3 + n / 100, [name], [(name, w, 1 if (w > 0) == late else 0) for w in ways])
    for name, here, src, dst in (("X", arrived[0], bx, xf), ("G", arrived[1], bg, gf), ("W2", [key for d in whole for key in whole[d]], bw2, w2f),
                                 ("W1", [key for o in w1_in for key in w1_in[o]], bw1, w1f)):
        plan.task(9, here, [mark(name)], functools.partial(store, src, dst), COST["go"])

    tile = 256

    e = lax.rem(y - x + ny, ny)
    early = lax.div(e, 2) * (3 - e), 1 + 2 * lax.div(e, 2)
    late = 2, 4 - early[0] - early[1]

    def up(ts, first):
        js = [lax.rem(x + t, nx) for t in ts]

        @pl.loop(0, fc // tile)
        def _(i):
            cols = at(i, tile)
            v = sum(mm(bx[:, at(j, hb)], bw1[at(j, hb), cols]) for j in js)
            u[:, cols] = v if first else u[:, cols] + v

    near = ["w", *[key for key in w1_in[0] + w1_in[1] + w1_in[-1]], *[key for key in arrived[0] if not (key[:3] == ("in", "x", "f") or key[:4] == ("in", "x", "d", 2))]]
    plan.task(30, near, [mark(("U", 0))], functools.partial(up, early, True), COST["U"])
    plan.task(30, [("U", 0), "X", "W1"], [mark(("U", 1))], functools.partial(up, late, False), COST["U"])

    def down(ds):
        spans = [at(idx("z", d), fz) for d in ds]

        @pl.loop(0, 2)
        def _(i):
            rows = at(i, tk)
            v = mm_t(bg[rows, :], jnp.concatenate([bw2[span, :] for span in spans]))
            for n, span in enumerate(spans):
                da[rows, span] = v[:, n * fz:(n + 1) * fz]

    for d in range(far + 1):
        ds = sorted({d, -d % nz})
        plan.task(31, ["G", *[key for e in ds for key in whole[e]]], [mark(("A", d))], functools.partial(down, ds), COST["A"] * len(ds) + 1)

    parts = 2 * tk // tile
    acts = [pltpu.make_async_copy(src, dst, asem.at[n]) for n, (src, dst) in enumerate(((ha, hid), (hd, dpre)))]

    def act():
        @pl.loop(0, parts * (fc // fz))
        def _(i):
            rows, cols = at(lax.rem(i, parts), tile), at(lax.div(i, parts), fz)
            h, vjp = jax.vjp(gelu_fn, u[rows, cols])
            ha[rows, cols] = h.astype(BF16)
            hd[rows, cols] = vjp(da[rows, cols])[0].astype(BF16)

        for copy in acts:
            copy.start()

    plan.task(32, [("U", 1), *[("A", d) for d in range(far + 1)]], [], act, COST["act"])

    order = plan.order()
    for copy in loads.values():
        copy.start()
    pl.when(x == y)(self_copy.start)

    barrier = pltpu.get_barrier_semaphore()

    def tell(to):
        pl.semaphore_signal(barrier, inc=1, device_id=to, device_id_type=MESH)

    for to in (*[nb(axis, d) for axis in "zyx" for d in ways], partner):
        tell(to)
    for o in range(1, ny):
        tell({"row": 2 * y + c, "col": idx("y", o)})
    pl.when(x != y)(lambda: tell({"row": 2 * y + c, "col": y}))
    run_tasks(plan, comm, order, lambda: pl.semaphore_wait(barrier, 6 + ny + jnp.where(x != y, 1, 0)))
    for copy in [*stores, *acts]:
        copy.wait()


def gather(dims, tok, grad, up, down):
    tk, hb = tok.shape
    fc = down.shape[0]
    nz, ny, nx = dims
    sds, vm = jax.ShapeDtypeStruct, pltpu.VMEM
    tokens, first, second, mid = (2 * tk, ny * hb), (nx * hb, fc), (fc, ny * hb), (2 * tk, fc)
    return pl.pallas_call(
        functools.partial(gather_kernel, dims),
        out_shape=[sds(shape, BF16) for shape in (tokens, tokens, first, second, mid, mid)],
        in_specs=[ANY] * 4,
        out_specs=[ANY] * 6,
        scratch_shapes=[
            *[vm(shape, BF16) for shape in (tokens, tokens, first, second, (fc // nz, hb))],
            vm(mid, F32),
            vm(mid, F32),
            vm(mid, BF16),
            vm(mid, BF16),
            pltpu.SemaphoreType.DMA((80,)),
            pltpu.SemaphoreType.DMA((80,)),
            pltpu.SemaphoreType.DMA((5,)),
            pltpu.SemaphoreType.DMA((9,)),
            pltpu.SemaphoreType.DMA((2,)),
        ],
        compiler_params=pltpu.CompilerParams(collective_id=0, has_side_effects=True, vmem_limit_bytes=VMEM_LIMIT),
        name="gather",
    )(tok, grad, up, down)


def reduce_kernel(dims, tok, grad, up, down, hid, dpre,
                  y_out, dx_out, g1_out, g2_out, dwp, yp, wx1, wx2, hx, dx, *scratch):
    nz, ny, nx = dims
    z, y, x, c = where_am_i()
    hb = y_out.shape[-1]
    tk = tok.shape[0] // 2
    hr = hb // 2
    fc = hid.shape[1]
    nu = fc // (nz * 8)
    sgn = (1, -1)
    scratch = list(scratch)

    def grab(n):
        return [scratch.pop(0) for _ in range(n)]

    nc = len(CHUNKS)
    xbuf, zbuf, tbuf = grab(nc), grab(nc), grab(nc)
    o1, o2, yr, yo, lhs, par, tmp = grab(7)
    pools = grab(5)
    ssem, rsem, lsem, osem, isem, tsem = grab(6)
    P_X, P_Z, P_Y, P_R, P_W = range(5)

    plan = Plan(RATES, WINDOW)
    comm = Comm(plan, ssem, rsem)

    def idx(axis, d):
        at, n = {"z": (z, nz), "y": (y, ny), "x": (x, nx)}[axis]
        return lax.rem(at + (d % n), n)

    def nb(axis, d):
        i = idx(axis, d)
        return {"z": {"depth": i}, "y": {"col": i}, "x": {"row": 2 * i + c}}[axis]

    partner = {"row": 2 * x + (1 - c)}
    across = {"row": 2 * y + c, "col": x}

    def hcol(j):
        return pl.ds(pl.multiple_of(j * hb, hb), hb)

    staged, stores, place = [], [], {}

    def stage(pool, src, marks=(), n=None):
        staged.append((pool, src, tuple(marks), n))
        return len(staged) - 1

    def slot(k):
        return place[k][0]

    def mark(key):
        plan.msg(key, ("l", key), 0)
        return key

    def chain(key, axis, n, s, buf, src, pool, marks, prio, end, end_sends, units=None):
        far, near = n // 2, n // 2 - 1
        for t in range(far):
            comm.msg((key, "F", t), (axis, s), (lambda: src(far * s)) if t == 0 else (lambda t=t: buf.at[t - 1]), lambda t=t: buf.at[t], nb(axis, s), group=(key, buf))
        for t in range(near):
            comm.msg((key, "N", t), (axis, -s), (lambda: src(-near * s)) if t == 0 else (lambda t=t: buf.at[far + t - 1]), lambda t=t: buf.at[far + t], nb(axis, -s), group=(key, buf))

        def own(rel):
            return [] if pool is None else [stage(pool, lambda: src(rel), marks(rel), units)]

        def mid(name, t, at, rel):
            ks = own(rel)

            def run():
                accumulate(buf.at[at], [slot(ks[0]) if ks else src(rel)])
                comm.start((key, name, t + 1))

            plan.task(prio, [(key, name, t), *marks(rel)], [(key, name, t + 1)], run, COST["go"], stage=ks)

        for t in range(far - 1):
            mid("F", t, t, (far - 1 - t) * s)
        for t in range(near - 1):
            mid("N", t, far + t, -(near - 1 - t) * s)
        ks = own(0)
        last = [buf.at[far - 1], buf.at[far + near - 1]]
        plan.task(prio, [(key, "F", far - 1), (key, "N", near - 1), *marks(0)], end_sends,
                  lambda: end(last, slot(ks[0]) if ks else src(0)), COST["fin"], stage=ks)
        return [(key, "F", 0), (key, "N", 0)]

    def raw(prio, marks, keys):
        plan.task(prio, marks, keys, lambda: comm.start(*keys), COST["go"], raw=True)

    def spread(key, s, region, finish, some):
        far, near = nz // 2, nz // 2 - 1
        for name, count, d in (("GF", far, s), ("GN", near, -s)):
            for t in range(count):
                def ref(t=t, d=d):
                    return region(idx("z", -t * d))
                comm.msg((key, name, t), ("z", d), ref, ref, nb("z", d), group=(key, some))
        for name, count in (("GF", far), ("GN", near)):
            for t in range(count - 1):
                plan.task(4, [(key, name, t)], [(key, name, t + 1)], lambda name=name, t=t: comm.start((key, name, t + 1)), COST["go"])
        plan.task(30, [(key, "GF", far - 1), (key, "GN", near - 1)], [], finish, COST["go"])
        return [(key, "GF", 0), (key, "GN", 0)]

    def store(src, dst):
        copy = pltpu.make_async_copy(src, dst, osem.at[len(stores)])
        stores.append(copy)
        copy.start()

    def none(rel):
        return ()

    for i, (a, first_axis, sigma, u, n, prio) in enumerate(CHUNKS):
        s = sgn[sigma]

        def done(o, a=a, u=u, n=n):
            return [("D", a, o % nx, v) for v in range(u, u + n)]

        if a == 0:
            def region(k, u=u, n=n):
                return o1.at[:, pl.ds(u, n), k]

            go = spread(("g", i), s, region, lambda u=u, n=n: store(o1.at[:, pl.ds(u, n)], g1_out.at[:, pl.ds(u, n)]), o1.at[:, pl.ds(0, n), pl.ds(0, nz - 1)])
            over = ("sw", i)
            comm.msg(over, ("d", 0), lambda i=i: tbuf[i], lambda u=u, n=n: o1.at[c, pl.ds(u, n), z], partner)

            def end(last, own, i=i, u=u, n=n, over=over):
                mine = pl.ds(pl.multiple_of(c * hr, hr), hr)
                other = pl.ds(pl.multiple_of((1 - c) * hr, hr), hr)
                for m in range(n):
                    tbuf[i][m] = total([own, *last], (m, slice(None), other))
                comm.start(over)
                for m in range(n):
                    o1[c, u + m, z] = total([own, *last], (m, slice(None), mine))
        else:
            def region(k, u=u, n=n):
                return o2.at[pl.ds(u, n), k]

            go = spread(("g", i), s, region, lambda u=u, n=n: store(o2.at[pl.ds(u, n)], g2_out.at[pl.ds(u, n)]), o2.at[pl.ds(0, n), pl.ds(0, nz - 1)])
            over = ("tr", i)
            comm.msg(over, ("o", 0), lambda i=i: tbuf[i], lambda region=region: region(z), across)
            comm.remote_if[over] = x != y

            def end(last, own, i=i, u=u, n=n, over=over):
                for m in range(n):
                    tbuf[i][m] = total([own, *last], m)
                comm.start(over)

                @pl.when(x == y)
                def _():
                    for m in range(n):
                        o2[u + m, z] = tbuf[i][m]

        plan.task(3, [over], go, lambda go=go: comm.start(*go), COST["go"])
        if first_axis == "x":
            res = xbuf[i].at[nx // 2 - 1]
            pieces = functools.partial(lambda res, rel: res.at[:, idx("z", rel)], res)
            raws = chain(("z", i), "z", nz, s, zbuf[i], pieces, None, none, 5, end, [over])

            def x_end(last, own, raws=raws):
                accumulate(last[0], [last[1], own])
                comm.start(*raws)

            raws = chain(("x", i), "x", nx, s, xbuf[i], lambda rel, a=a, u=u, n=n: dwp.at[a, pl.ds(u, n), :, :, hcol(idx("x", rel))],
                         P_X, lambda rel, done=done: done(rel), 10, x_end, raws, n)
            raw(11 + prio / 100, done(2) + done(-s), raws)
        else:
            res = zbuf[i].at[nz // 2 - 1]
            raws = chain(("x", i), "x", nx, s, xbuf[i], lambda rel, res=res: res.at[:, :, hcol(idx("x", rel))], None, none, 8, end, [over])

            def z_end(last, own, raws=raws):
                accumulate(last[0], [last[1], own])
                comm.start(*raws)

            all_done = [m for o in range(nx) for m in done(o)]
            raws = chain(("z", i), "z", nz, s, zbuf[i], lambda rel, a=a, u=u, n=n: dwp.at[a, pl.ds(u, n), idx("z", rel)],
                         P_Z, lambda rel, all_done=all_done: all_done, 9, z_end, raws, n)
            raw(11 + prio / 100, all_done, raws)

    groups = yo.shape[1]
    for a, out in enumerate((y_out, dx_out)):
        for sigma in range(2):
            s = sgn[sigma]
            half = pl.ds(sigma * (groups // 2), groups // 2)

            def y_end(last, own, a=a, half=half, sigma=sigma, out=out):
                def one(ix):
                    yo[(a, sigma * (groups // 2) + ix[0], ix[1])] = total([own, *last], ix).astype(BF16)

                each(own.shape, one)
                store(yo.at[a, half], out.at[half])

            raws = chain(("y", a, sigma), "y", ny, s, yr.at[a, sigma], lambda rel, a=a, half=half: yp.at[a, half, :, :, hcol(idx("y", rel))],
                         P_Y, lambda rel, a=a: [("Y", a, rel % ny)], 12, y_end, [])
            raw(11, [("Y", a, 2), ("Y", a, -s % ny)], raws)

    tile = 256

    def rows(o):
        return pl.ds(pl.multiple_of(idx("y", o) * hb, hb), hb)

    def arrive(key, prio=6):
        plan.msg(("got", *key), ("s", key), 0)
        plan.task(prio, [key], [("got", *key)], lambda: None, COST["go"])
        return ("got", *key)

    lhs_loads = [pltpu.make_async_copy(src, lhs.at[n], isem.at[n]) for n, src in enumerate((hid, dpre))]
    for n in (1, 0):
        plan.task(0, [], [mark(("T", n))], lhs_loads[n].wait, COST["fin"])

    others = pl.ds(pl.multiple_of((1 - c) * tk, tk), tk)
    own_rows = pl.ds(pl.multiple_of(c * tk, tk), tk)
    par_loads = []
    for n, (src, box) in enumerate(((hid, hx), (dpre, dx))):
        comm.msg(("hx", n), ("d", 0), lambda src=src: src.at[others], lambda box=box: box, partner)
        raw(1, [("C", 3)], [("hx", n)])
        par_loads.append(pltpu.make_async_copy(box, par.at[n], isem.at[2 + n]))
        plan.task(6, [("hx", n)], [mark(("P", n))], par_loads[n].start, COST["go"])
    for a, o in Y_ORDER:
        if a == 0:
            comm.msg(("w", a, o), ("d", 0), lambda o=o: down.at[:, hcol(idx("y", o))], lambda o=o: wx2.at[:, hcol(idx("y", o))], partner, group=("w2", wx2))
        else:
            comm.msg(("w", a, o), ("d", 0), lambda o=o: up.at[rows(o)], lambda o=o: wx1.at[rows(o)], partner, group=("w1", wx1))
        raw(2, [("C", 3)], [("w", a, o)])

    par_seen = set()
    last_of, b = {}, 1
    for n, job in enumerate(JOBS):
        opens, closes = job[0] == "D" or job[3] == 0, job[0] == "D" or job[3] == 1
        b = 1 - b if opens else b
        keys = [("Y", job[1], job[2])] if job[0] == "Y" else [("D", job[1], job[2] % nx, v) for v in range(job[3], job[3] + job[4])]
        span = pl.ds(0, yo.shape[1] if job[0] == "Y" else job[4])
        waits = [("C", n - 1)] if n else []
        if opens and b in last_of:
            waits.append(("S", last_of[b]))
        if job[0] == "D":
            _, a, o, u, n_u = job
            waits.append(("T", 1 - a))
            ks = [stage(P_R, lambda a=a, o=o: (tok, grad)[a].at[:, hcol(idx("x", o))])]

            def value(cols, a=a, u=u, n_u=n_u, ks=ks):
                return mm_l(lhs[1 - a, :, u * nz * 8:(u + n_u) * nz * 8], slot(ks[0])[:, cols])

            dst = functools.partial(lambda a, o, u, n_u: dwp.at[a, pl.ds(u, n_u), :, :, hcol(idx("x", o))], a, o, u, n_u)
            cost = COST["D"][0] + COST["D"][1] * n_u
        else:
            _, a, o, h = job
            waits.append(("T", a))
            marks = []
            if h:
                marks = [arrive(("w", a, o))]
                waits += [("P", a), *marks]
            if a == 0:
                ks = [stage(P_R, lambda o=o, w=(down, wx2)[h]: w.at[:, hcol(idx("y", o))], marks)]
            else:
                ks = [stage(P_W, lambda o=o, w=(up, wx1)[h]: w.at[rows(o)], marks)]

            def value(cols, a=a, h=h, ks=ks):
                left = par[a] if h else lhs[a, own_rows, :]
                return mm(left, slot(ks[0])[:, cols]) if a == 0 else mm_t(left, slot(ks[0])[cols, :])

            dst = functools.partial(lambda a, o: yp.at[a, :, :, :, hcol(idx("y", o))], a, o)
            cost = COST["Y"]

        def save(b=b, dst=dst, span=span):
            return pltpu.make_async_copy(tmp.at[b, span], dst(), tsem.at[b])

        def run(b=b, value=value, save=save, job=job, span=span, opens=opens, closes=closes):
            if job[0] == "Y" and job[3] and job[1] not in par_seen:
                par_loads[job[1]].wait()
                par_seen.add(job[1])

            @pl.loop(0, hb // tile)
            def _(t):
                cols = pl.ds(pl.multiple_of(t * tile, tile), tile)
                v = value(cols).reshape((span.size,) + tmp.shape[2:4] + (tile,))
                tmp[b, span, :, :, cols] = v if opens else tmp[b, span, :, :, cols] + v

            if closes:
                save().start()

        sends = [mark(("C", n))]
        if closes:
            plan.msg(("W", n), ("s", n), 0)
            sends.append(("W", n))
            last_of[b] = n
            plan.task(2, [("W", n)], [mark(("S", n)), *[mark(key) for key in keys]], lambda save=save: save().wait(), COST["go"])
        plan.task(40, waits, sends, run, cost, stage=ks)

    order = plan.order()

    at = {}
    for n, i in enumerate(order):
        for w in plan.tasks[i][2]:
            at[w] = n
    uses = {p: [] for p in range(len(pools))}
    user = {}
    for n, i in enumerate(order):
        for k in plan.tasks[i][5]:
            uses[staged[k][0]].append(k)
            user[k] = n
    lbase, fill = 0, {}
    for p, ks in uses.items():
        depth = pools[p].shape[0]
        for n, k in enumerate(ks):
            box = pools[p].at[n % depth] if staged[k][3] is None else pools[p].at[n % depth, pl.ds(0, staged[k][3])]
            place[k] = (box, lsem.at[lbase + n % depth])
            when = -1 if n < depth else user[ks[n - depth]]
            for w in staged[k][2]:
                when = max(when, at[w])
            fill.setdefault(when, []).append(k)
        lbase += depth

    def load(k):
        return pltpu.make_async_copy(staged[k][1](), *place[k])

    for copy in lhs_loads[::-1]:
        copy.start()
    for k in fill.get(-1, ()):
        load(k).start()

    barrier = pltpu.get_barrier_semaphore()

    def tell(to):
        pl.semaphore_signal(barrier, inc=1, device_id=to, device_id_type=MESH)

    peers = [*[nb(axis, d) for axis in "zyx" for d in sgn], partner]
    for to in peers:
        tell(to)
    pl.when(x != y)(lambda: tell(across))
    run_tasks(plan, comm, order, lambda: pl.semaphore_wait(barrier, len(peers) + jnp.where(x != y, 1, 0)), load, fill)
    for copy in stores:
        copy.wait()


def reduce(dims, tok, grad, up, down, hid, dpre):
    nz, ny, nx = dims
    rows2, hh = tok.shape
    fc = hid.shape[1]
    tk, hb = rows2 // 2, hh // ny
    hr = hb // 2
    nu = fc // (nz * SUB)
    g = tk // (SUB * SUB)
    vm = pltpu.VMEM

    def per(shape):
        return [vm(shape(axis, n), F32) for _, axis, _, _, n, *_ in CHUNKS]

    def fin(shape):
        return [vm((n, SUB, hr if a == 0 else hb), F32) for a, _, _, _, n, *_ in CHUNKS]

    n0 = max(chunk[4] for chunk in CHUNKS)
    scratch = [
        *per(lambda axis, n: (nx - 1, n, nz, SUB, hb) if axis == "x" else (nx - 1, n, SUB, hb)),
        *per(lambda axis, n: (nz - 1, n, SUB, hb) if axis == "x" else (nz - 1, n, SUB, hh)),
        *fin(0),
        vm((2, nu, nz, SUB, hr), F32),
        vm((nu, nz, SUB, hb), F32),
        vm((2, 2, ny - 1, g // 2, SUB, SUB, hb), F32),
        vm((2, g, SUB, SUB, hb), BF16),
        vm((2, rows2, fc), BF16),
        vm((2, tk, fc), BF16),
        vm((2, g, SUB, SUB, hb), F32),
        vm((3, n0, nz, SUB, hb), F32),
        vm((6, n0, SUB, hh), F32),
        vm((2, g // 2, SUB, SUB, hb), F32),
        vm((3, rows2, hb), BF16),
        vm((3, hb, fc), BF16),
        pltpu.SemaphoreType.DMA((80,)),
        pltpu.SemaphoreType.DMA((330,)),
        pltpu.SemaphoreType.DMA((18,)),
        pltpu.SemaphoreType.DMA((24,)),
        pltpu.SemaphoreType.DMA((6,)),
        pltpu.SemaphoreType.DMA((2,)),
    ]
    sds = jax.ShapeDtypeStruct
    outs = pl.pallas_call(
        functools.partial(reduce_kernel, dims),
        out_shape=[
            sds((g, SUB, SUB, hb), BF16),
            sds((g, SUB, SUB, hb), BF16),
            sds((2, nu, nz, SUB, hr), F32),
            sds((nu, nz, SUB, hb), F32),
            sds((2, nu, nz, SUB, hh), F32),
            sds((2, g, SUB, SUB, hh), F32),
            sds(up.shape, BF16),
            sds(down.shape, BF16),
            sds((tk, fc), BF16),
            sds((tk, fc), BF16),
        ],
        in_specs=[ANY] * 6,
        out_specs=[ANY] * 10,
        scratch_shapes=scratch,
        compiler_params=pltpu.CompilerParams(collective_id=1, has_side_effects=True, vmem_limit_bytes=VMEM_LIMIT),
        name="reduce",
    )(tok, grad, up, down, hid, dpre)
    y, dx, g1, g2 = outs[:4]
    return finish(y.reshape(tk, hb), dx.reshape(tk, hb), g1.reshape(2 * fc, hr), g2.reshape(fc, hb))


def finish_kernel(*refs):
    *arrays, turned, isem, osem = refs
    n, parts = isem.shape
    ins, outs, boxes = (arrays[k * n:(k + 1) * n] for k in range(3))

    def span(ref, k):
        size = ref.shape[0] // parts
        return pl.ds(k * size, size)

    def fetch(i, k):
        return pltpu.make_async_copy(ins[i].at[span(ins[i], k)], boxes[i].at[span(ins[i], k)], isem.at[i, k])

    def put(i, k):
        if i == 0:
            cols = span(ins[i], k)
            return pltpu.make_async_copy(turned.at[:, cols], outs[i].at[:, cols], osem.at[i, k])
        return pltpu.make_async_copy(boxes[i].at[span(ins[i], k)], outs[i].at[span(ins[i], k)], osem.at[i, k])

    todo = list(itertools.product(range(n), range(parts)))
    for i, k in todo:
        fetch(i, k).start()
    for i, k in todo:
        fetch(i, k).wait()
        if i == 0:
            rows = span(ins[i], k)
            turned[:, rows] = boxes[i][rows, :].T
        put(i, k).start()
    for i, k in todo:
        put(i, k).wait()


def finish(y, dx, g1, g2):
    ins = (g1, g2, y, dx)
    turned = jax.ShapeDtypeStruct(g1.shape[::-1], F32)
    parts = 4
    out = pl.pallas_call(
        finish_kernel,
        out_shape=[turned, *[jax.ShapeDtypeStruct(v.shape, v.dtype) for v in ins[1:]]],
        in_specs=[ANY] * len(ins),
        out_specs=[ANY] * len(ins),
        scratch_shapes=[*[pltpu.VMEM(v.shape, v.dtype) for v in ins], pltpu.VMEM(turned.shape, F32), *[pltpu.SemaphoreType.DMA((len(ins), parts))] * 2],
        compiler_params=pltpu.CompilerParams(vmem_limit_bytes=VMEM_LIMIT),
        name="finish",
    )(*ins)
    return out[2], out[3], out[0], out[1]


def solution(mesh):
    act_spec = P(("depth", "row"), "col")
    weight_spec = P("row", "col")
    dims = (mesh.shape["depth"], mesh.shape["col"], mesh.shape["row"] // 2)

    def local_block(tok_blk, up_blk, down_blk, grad_blk):
        return reduce(dims, *gather(dims, tok_blk, grad_blk, up_blk, down_blk))

    return jax.shard_map(local_block, mesh=mesh, in_specs=(act_spec, weight_spec, weight_spec, act_spec), out_specs=(act_spec, act_spec, weight_spec, weight_spec), check_vma=False)
```

```python
import functools
import itertools
import string

import jax
import jax.numpy as jnp
from jax import lax
from jax.experimental import pallas as pl
from jax.experimental.pallas import tpu as pltpu
from jax.sharding import PartitionSpec as P

MESH = pl.DeviceIdType.MESH
ANY = pl.BlockSpec(memory_space=pl.ANY)
F32 = jnp.float32
SUB = 8
BF16 = jnp.bfloat16

TOP = (12, 10)
UNITS = 16
FAR_FIRST = (2, 1, 3, 0)
Y_ORDER = [(a, o) for a in range(2) for o in FAR_FIRST]
DIGITS = string.digits + string.ascii_letters
JOB_ORDER = "10svut2y64z3w5x8rdho9b7AqcfamCBpilgFEnGejkDH"
RANKS = "107kl30b24216589a"
SIDES = "01010010101011001"


def chunk_list():
    def run(a, axis, lo, hi, n=2):
        return [(a, axis, u, min(n, hi - u)) for u in range(lo, hi, n)]

    first, last = TOP
    parts = run(1, "z", last, UNITS) + run(0, "z", first, UNITS) + run(0, "x", 0, first) + run(1, "x", 0, last - 2) + run(1, "x", last - 2, last, 1)
    return [(a, axis, int(side), u, n, DIGITS.index(rank)) for (a, axis, u, n), side, rank in zip(parts, SIDES, RANKS)]


CHUNKS = chunk_list()


def job_list():
    def block(a, lo, hi):
        return [[("D", a, o, u, min(4, hi - u))] for u in range(lo, hi, 4) for o in FAR_FIRST]

    first, last = TOP
    jobs = block(0, 0, first) + block(1, 0, last) + block(0, first, UNITS) + block(1, last, UNITS) + [[("Y", a, o, h) for h in range(2)] for a, o in Y_ORDER]
    return [job for c in JOB_ORDER for job in jobs[DIGITS.index(c)]]


JOBS = job_list()
COST = {"D": (0.5, 0.15), "Y": 1.2, "fin": 0.1, "go": 0.03, "U": 4.0, "A": 0.8, "act": 3.0}
SLACK = 20.0
VMEM_LIMIT = 66_500_000


def gelu_fn(pre_act):
    return jax.nn.gelu(pre_act, approximate=True)


class Plan:
    def __init__(self, rates, window):
        self.rates, self.window = rates, window
        self.tasks, self.size, self.link = [], {}, {}

    def msg(self, key, link, nbytes):
        self.size[key], self.link[key] = nbytes, link

    def task(self, prio, waits, sends, run, cost=0.3, stage=(), raw=False):
        self.tasks.append((prio, tuple(waits), tuple(sends), run, cost, tuple(stage), raw))

    def order(self):
        free, arrive, out = {}, {}, []
        self.when, self.arrive = [], arrive
        now, left = 2.5, list(range(len(self.tasks)))
        while left:
            best = None
            for i in left:
                prio, waits, sends, _, _, _, raw = self.tasks[i]
                if any(w not in arrive for w in waits):
                    continue
                ready = max([arrive[w] for w in waits], default=0.0)
                if raw:
                    ready = max([ready] + [free.get(self.link[s], 0.0) - self.window for s in sends])
                key = (max(ready, now), prio, i)
                if best is None or key < best:
                    best = key
            at, _, i = best
            left.remove(i)
            out.append(i)
            now = at + self.tasks[i][4]
            self.when.append(now)
            for s in self.tasks[i][2]:
                rate, lat = self.rates[self.link[s][0]]
                took = self.size[s] / rate
                if self.link[s][0] in "to":
                    share = 0.5 if self.link[s][0] == "t" else 1.5
                    ways = [(axis, d) for axis in "xy" for d in (1, -1)]
                    done = max(now, *[free.get(way, 0.0) for way in ways]) + took
                    for way in ways:
                        free[way] = max(now, free.get(way, 0.0)) + took * share
                else:
                    done = max(now, free.get(self.link[s], 0.0)) + took
                    free[self.link[s]] = done
                arrive[s] = done + lat
        self.end = max(now, max(arrive.values()))
        return out


RATES = {axis: (45e3, 2.2) for axis in "xyz"}
RATES.update(d=(450e3, 3.0), t=(45e3, 5.0), o=(45e3, 7.0), l=(1e12, 0.0), s=(1e12, 2.0))
WINDOW = 10.0


class Comm:
    def __init__(self, plan, ssem, rsem):
        self.plan, self.ssem, self.rsem = plan, ssem, rsem
        self.make, self.meet, self.slot, self.remote_if, self.groups, self.grouped, self.flying = {}, {}, {}, {}, {}, set(), []

    def msg(self, key, link, src, dst, to, mail=None, group=None):
        i = len(self.slot)
        self.slot[key] = i
        there, here = mail or (i, i)
        name, ref = group or (key, None)
        g, _, _ = self.groups.setdefault(name, (len(self.groups), ref, to))
        if group:
            self.grouped.add(key)

        def make(r):
            return pltpu.make_async_remote_copy(
                src_ref=src(), dst_ref=dst(), send_sem=self.ssem.at[g], recv_sem=self.rsem.at[r], device_id=to, device_id_type=MESH)

        self.make[key] = lambda: make(there)
        self.meet[key] = lambda: make(here)
        shape = src().shape
        nbytes = functools.reduce(lambda a, b: a * b, shape, 1) * src().dtype.itemsize
        self.plan.msg(key, link, nbytes)

    def each(self, keys, make, act):
        for key in keys:
            if key in self.remote_if:
                pl.when(self.remote_if[key])(lambda key=key: act(make[key]()))
            elif key in make:
                act(make[key]())

    def start(self, *keys):
        self.flying.extend(key for key in keys if key not in self.grouped)
        self.each(keys, self.make, lambda copy: copy.start())

    def finish(self):
        self.sent(float("inf"))
        for g, ref, to in self.groups.values():
            if ref is not None:
                pltpu.make_async_remote_copy(src_ref=ref, dst_ref=ref, send_sem=self.ssem.at[g], recv_sem=self.rsem.at[g], device_id=to, device_id_type=MESH).wait_send()

    def wait(self, *keys):
        self.each(keys, self.meet, lambda copy: copy.wait_recv())

    def sent(self, before):
        keys = [key for key in self.flying if self.plan.arrive[key] <= before]
        self.flying = [key for key in self.flying if self.plan.arrive[key] > before]
        self.each(keys, self.make, lambda copy: copy.wait_send())


def run_tasks(plan, comm, order, ready, load=None, fill={}):
    heard = set()
    for n, i in enumerate(order):
        _, waits, sends, run, _, ks, _ = plan.tasks[i]
        if ready and any(key in comm.make for key in sends):
            ready()
            ready = None
        with jax.named_scope(f"w{n}"):
            comm.wait(*[w for w in waits if w not in heard])
            heard.update(waits)
        with jax.named_scope(f"l{n}"):
            for k in ks:
                load(k).wait()
        with jax.named_scope(f"r{n}"):
            run()
        for k in fill.get(n, ()):
            load(k).start()
        comm.sent(plan.when[n] - SLACK)
    comm.finish()


def where_am_i():
    z, y, r = lax.axis_index("depth"), lax.axis_index("col"), lax.axis_index("row")
    return z, y, lax.div(r, 2), lax.rem(r, 2)


def each(shape, fn):
    lead = shape[:-2]
    big = max(range(len(lead)), key=lambda d: lead[d])
    looped = lead[big] >= 8

    def rest(k):
        for ix in itertools.product(*[range(n) if not (looped and d == big) else (k,) for d, n in enumerate(lead)]):
            fn(ix)

    if looped:
        pl.loop(0, lead[big])(rest)
    else:
        rest(None)


def total(refs, ix):
    return functools.reduce(lambda a, b: a + b, [ref[ix] for ref in refs])


def accumulate(dst, others):
    def one(ix):
        dst[ix] = total([dst, *others], ix)

    each(dst.shape, one)


def mm(a, b):
    return jnp.dot(a, b, preferred_element_type=F32)


def mm_l(a, b):
    return lax.dot_general(a, b, (((0,), (0,)), ((), ())), preferred_element_type=F32)


def mm_t(a, b):
    return lax.dot_general(a, b, (((1,), (1,)), ((), ())), preferred_element_type=F32)


def gather_kernel(dims, x_ref, g_ref, w1_ref, w2_ref, xf, gf, w1f, w2f, hid, dpre,
                  bx, bg, bw1, bw2, vw2, u, da, ha, hd, ssem, rsem, lsem, osem, asem):
    nz, ny, nx = dims
    z, y, x, c = where_am_i()
    tk, hb = x_ref.shape
    fc = w2_ref.shape[0]
    hr, fz, half = hb // 2, fc // nz, tk // 2
    plan = Plan(RATES, WINDOW)
    comm = Comm(plan, ssem, rsem)
    ways = (1, -1)

    def idx(axis, d):
        at, n = {"z": (z, nz), "y": (y, ny), "x": (x, nx)}[axis]
        return lax.rem(at + (d % n), n)

    def nb(axis, d):
        i = idx(axis, d)
        return {"z": {"depth": i}, "y": {"col": i}, "x": {"row": 2 * i + c}}[axis]

    partner = {"row": 2 * x + (1 - c)}

    def at(i, size):
        return pl.ds(pl.multiple_of(i * size, size), size)

    def block(full, core, o, part=None):
        rows = at(core, tk) if part is None else pl.ds(pl.multiple_of(core * tk + part * half, half), half)
        return full.at[rows, at(idx("y", o), hb)]

    def wblock(o, core):
        return bw1.at[at(2 * idx("x", o) + core, hr), :]

    def piece(d, o):
        return bw2.at[at(idx("z", d), fz), at(idx("y", o), hb)]

    stores = []

    def store(src, dst):
        copy = pltpu.make_async_copy(src, dst, osem.at[len(stores)])
        stores.append(copy)
        copy.start()

    def mark(key):
        plan.msg(key, ("l", key), 0)
        return key

    loads = {}

    def load(name, src, dst):
        loads[name] = pltpu.make_async_copy(src, dst, lsem.at[len(loads)])
        plan.task(len(loads) / 10, [], [mark(name)], loads[name].wait, COST["go"])

    load("s", w2_ref.at[at(z, fz), :], vw2)
    load("w", w1_ref.at[:, at(c, fc)], wblock(0, c))
    load("x", x_ref, block(bx, c, 0))
    load("g", g_ref, block(bg, c, 0))
    self_copy = pltpu.make_async_copy(w2_ref.at[at(z, fz), :], piece(0, 0), lsem.at[len(loads)])

    def raw(prio, waits, keys):
        plan.task(prio, waits, keys, lambda: comm.start(*keys), COST["go"], raw=True)

    def passed(prio, wait, keys, key=None):
        plan.task(prio, [wait], [*keys, mark(("in", *wait) if key is None else key)], lambda: comm.start(*keys), COST["go"])

    for o in (1, -1, 2, 0):
        o = o % ny
        to = {"row": 2 * idx("x", o) + c, "col": x}
        comm.msg(("s", o), ("t", 0), lambda: vw2, lambda: piece(0, 0), to, mail=(y, idx("y", o)))
    comm.remote_if[("s", 0)] = x != y
    plan.task(1, ["s"], [("s", o) for o in range(ny)], lambda: comm.start(*[("s", o) for o in range(ny)]), COST["go"])
    whole = {d: [] for d in range(nz)}
    far = nz // 2
    for o in range(ny):
        for w in ways:
            steps = far if (w > 0) == (o % 2 == 0) else far - 1
            for t in range(steps):
                comm.msg(("z", o, w, t), ("z", w), lambda o=o, w=w, t=t: piece(-w * t, o), lambda o=o, w=w, t=t: piece(-w * t, o), nb("z", w))
                nxt = [("z", o, w, t + 1)] if t + 1 < steps else []
                key = ("w2", o, (-w * (t + 1)) % nz)
                passed(4, ("z", o, w, t), nxt, key)
                whole[key[2]].append(key)
        first = [("z", o, w, 0) for w in ways]

        def slice_in(o=o, first=first):
            if o == 0:
                pl.when(x == y)(self_copy.wait)
            comm.start(*first)

        plan.task(3, [("s", o)], [*first, mark(("w2", o, 0))], slice_in, COST["go"])
        whole[0].append(("w2", o, 0))

    comm.msg(("pw",), ("d", 0), lambda: w1_ref.at[:, at(1 - c, fc)], lambda: wblock(0, c), partner)
    raw(1.1, [], [("pw",)])
    w1_in = {0: ["w"], 1: [], -1: [], 2: []}
    for own in (True, False):
        core = c if own else 1 - c
        for w in ways:
            comm.msg(("wa", own, w), ("x", w), lambda core=core: wblock(0, core), lambda core=core: wblock(0, core), nb("x", w))
    raw(1.2, ["w"], [("wa", True, w) for w in ways])
    passed(5, ("pw",), [("wa", False, w) for w in ways])
    w1_in[0].append(("in", "pw"))
    for own, w in ((True, 1), (False, -1)):
        core = c if own else 1 - c
        comm.msg(("wf", w), ("x", w), lambda core=core, w=w: wblock(-w, core), lambda core=core, w=w: wblock(-w, core), nb("x", w))
        passed(6, ("wa", own, w), [("wf", w)])
        passed(6, ("wa", not own, w), [])
        passed(6, ("wf", w), [])
        w1_in[-w] += [("in", "wa", True, w), ("in", "wa", False, w)]
        w1_in[2].append(("in", "wf", w))

    arrived = {}
    for a, (full, name) in enumerate(((bx, "x"), (bg, "g"))):
        arrived[a] = [name]
        for w in ways:
            for p in range(2):
                comm.msg((name, w, p), ("y", w), lambda full=full, p=p: block(full, c, 0, p), lambda full=full, p=p: block(full, c, 0, p), nb("y", w))
            p = 0 if w > 0 else 1
            comm.msg((name, "f", w), ("y", w), lambda full=full, w=w, p=p: block(full, c, -w, p), lambda full=full, w=w, p=p: block(full, c, -w, p), nb("y", w))

        def share(key, o, p, full=full, name=name, a=a):
            comm.msg((name, "d", *key), ("d", 0), lambda: block(full, c, o, p), lambda: block(full, c, o, p), partner)
            passed(20, (name, "d", *key), [])
            arrived[a].append(("in", name, "d", *key))
            return (name, "d", *key)

        plan.task(2 + a, [name], [share((0,), 0, None)], lambda name=name: comm.start((name, "d", 0)), COST["go"])
        for w in ways:
            p = 0 if w > 0 else 1
            for q in range(2):
                keys = [share((-w, q), -w, q)] + ([(name, "f", w)] if q == p else [])
                passed(7, (name, w, q), keys)
                arrived[a].append(("in", name, w, q))
            passed(7, (name, "f", w), [share((2, p), 2, p)])
            arrived[a].append(("in", name, "f", w))
    for n, (name, late) in enumerate(itertools.product("gx", (False, True))):
        raw(1.3 + n / 100, [name], [(name, w, 1 if (w > 0) == late else 0) for w in ways])
    for name, here, src, dst in (("X", arrived[0], bx, xf), ("G", arrived[1], bg, gf), ("W2", [key for d in whole for key in whole[d]], bw2, w2f),
                                 ("W1", [key for o in w1_in for key in w1_in[o]], bw1, w1f)):
        plan.task(9, here, [mark(name)], functools.partial(store, src, dst), COST["go"])

    tile = 256

    e = lax.rem(y - x + ny, ny)
    early = lax.div(e, 2) * (3 - e), 1 + 2 * lax.div(e, 2)
    late = 2, 4 - early[0] - early[1]

    def up(ts, first):
        js = [lax.rem(x + t, nx) for t in ts]

        @pl.loop(0, fc // tile)
        def _(i):
            cols = at(i, tile)
            v = sum(mm(bx[:, at(j, hb)], bw1[at(j, hb), cols]) for j in js)
            u[:, cols] = v if first else u[:, cols] + v

    near = ["w", *[key for key in w1_in[0] + w1_in[1] + w1_in[-1]], *[key for key in arrived[0] if not (key[:3] == ("in", "x", "f") or key[:4] == ("in", "x", "d", 2))]]
    plan.task(30, near, [mark(("U", 0))], functools.partial(up, early, True), COST["U"])
    plan.task(30, [("U", 0), "X", "W1"], [mark(("U", 1))], functools.partial(up, late, False), COST["U"])

    def down(ds):
        spans = [at(idx("z", d), fz) for d in ds]

        @pl.loop(0, 2)
        def _(i):
            rows = at(i, tk)
            v = mm_t(bg[rows, :], jnp.concatenate([bw2[span, :] for span in spans]))
            for n, span in enumerate(spans):
                da[rows, span] = v[:, n * fz:(n + 1) * fz]

    for d in range(far + 1):
        ds = sorted({d, -d % nz})
        plan.task(31, ["G", *[key for e in ds for key in whole[e]]], [mark(("A", d))], functools.partial(down, ds), COST["A"] * len(ds) + 1)

    parts = tk // tile
    acts = [[pltpu.make_async_copy(src.at[at(h, tk), :], dst.at[at(h, tk), :], asem.at[h, n]) for n, (src, dst) in enumerate(((ha, hid), (hd, dpre)))] for h in range(2)]

    def act():
        for half, copies in enumerate(acts):
            @pl.loop(0, parts * (fc // fz))
            def _(i):
                rows, cols = at(half * parts + lax.rem(i, parts), tile), at(lax.div(i, parts), fz)
                h, vjp = jax.vjp(gelu_fn, u[rows, cols])
                ha[rows, cols] = h.astype(BF16)
                hd[rows, cols] = vjp(da[rows, cols])[0].astype(BF16)

            for copy in copies:
                copy.start()

    plan.task(32, [("U", 1), *[("A", d) for d in range(far + 1)]], [], act, COST["act"])

    order = plan.order()
    for copy in loads.values():
        copy.start()
    pl.when(x == y)(self_copy.start)

    barrier = pltpu.get_barrier_semaphore()

    def tell(to):
        pl.semaphore_signal(barrier, inc=1, device_id=to, device_id_type=MESH)

    for to in (*[nb(axis, d) for axis in "zyx" for d in ways], partner):
        tell(to)
    for o in range(1, ny):
        tell({"row": 2 * y + c, "col": idx("y", o)})
    pl.when(x != y)(lambda: tell({"row": 2 * y + c, "col": y}))
    run_tasks(plan, comm, order, lambda: pl.semaphore_wait(barrier, 6 + ny + jnp.where(x != y, 1, 0)))
    for copy in [*stores, *sum(acts, [])]:
        copy.wait()


def gather(dims, tok, grad, up, down):
    tk, hb = tok.shape
    fc = down.shape[0]
    nz, ny, nx = dims
    sds, vm = jax.ShapeDtypeStruct, pltpu.VMEM
    tokens, first, second, mid = (2 * tk, ny * hb), (nx * hb, fc), (fc, ny * hb), (2 * tk, fc)
    return pl.pallas_call(
        functools.partial(gather_kernel, dims),
        out_shape=[sds(shape, BF16) for shape in (tokens, tokens, first, second, mid, mid)],
        in_specs=[ANY] * 4,
        out_specs=[ANY] * 6,
        scratch_shapes=[
            *[vm(shape, BF16) for shape in (tokens, tokens, first, second, (fc // nz, hb))],
            vm(mid, F32),
            vm(mid, F32),
            vm(mid, BF16),
            vm(mid, BF16),
            pltpu.SemaphoreType.DMA((80,)),
            pltpu.SemaphoreType.DMA((80,)),
            pltpu.SemaphoreType.DMA((5,)),
            pltpu.SemaphoreType.DMA((9,)),
            pltpu.SemaphoreType.DMA((2, 2)),
        ],
        compiler_params=pltpu.CompilerParams(collective_id=0, has_side_effects=True, vmem_limit_bytes=VMEM_LIMIT),
        name="gather",
    )(tok, grad, up, down)


def reduce_kernel(dims, tok, grad, up, down, hid, dpre,
                  y_out, dx_out, g1_out, g2_out, dwp, yp, wx1, wx2, hx, dx, *scratch):
    nz, ny, nx = dims
    z, y, x, c = where_am_i()
    hb = y_out.shape[-1]
    tk = tok.shape[0] // 2
    hr = hb // 2
    fc = hid.shape[1]
    nu = fc // (nz * 8)
    sgn = (1, -1)
    scratch = list(scratch)

    def grab(n):
        return [scratch.pop(0) for _ in range(n)]

    nc = len(CHUNKS)
    xbuf, zbuf, tbuf = grab(nc), grab(nc), grab(nc)
    o1, o2, yr, yo, lhs, par, tmp = grab(7)
    pools = grab(5)
    ssem, rsem, lsem, osem, isem, tsem = grab(6)
    P_X, P_Z, P_Y, P_R, P_W = range(5)

    plan = Plan(RATES, WINDOW)
    comm = Comm(plan, ssem, rsem)

    def idx(axis, d):
        at, n = {"z": (z, nz), "y": (y, ny), "x": (x, nx)}[axis]
        return lax.rem(at + (d % n), n)

    def nb(axis, d):
        i = idx(axis, d)
        return {"z": {"depth": i}, "y": {"col": i}, "x": {"row": 2 * i + c}}[axis]

    partner = {"row": 2 * x + (1 - c)}
    across = {"row": 2 * y + c, "col": x}

    def hcol(j):
        return pl.ds(pl.multiple_of(j * hb, hb), hb)

    staged, stores, place = [], [], {}

    def stage(pool, src, marks=(), n=None):
        staged.append((pool, src, tuple(marks), n))
        return len(staged) - 1

    def slot(k):
        return place[k][0]

    def mark(key):
        plan.msg(key, ("l", key), 0)
        return key

    def chain(key, axis, n, s, buf, src, pool, marks, prio, end, end_sends, units=None):
        far, near = n // 2, n // 2 - 1
        for t in range(far):
            comm.msg((key, "F", t), (axis, s), (lambda: src(far * s)) if t == 0 else (lambda t=t: buf.at[t - 1]), lambda t=t: buf.at[t], nb(axis, s), group=(key, buf))
        for t in range(near):
            comm.msg((key, "N", t), (axis, -s), (lambda: src(-near * s)) if t == 0 else (lambda t=t: buf.at[far + t - 1]), lambda t=t: buf.at[far + t], nb(axis, -s), group=(key, buf))

        def own(rel):
            return [] if pool is None else [stage(pool, lambda: src(rel), marks(rel), units)]

        def mid(name, t, at, rel):
            ks = own(rel)

            def run():
                accumulate(buf.at[at], [slot(ks[0]) if ks else src(rel)])
                comm.start((key, name, t + 1))

            plan.task(prio, [(key, name, t), *marks(rel)], [(key, name, t + 1)], run, COST["go"], stage=ks)

        for t in range(far - 1):
            mid("F", t, t, (far - 1 - t) * s)
        for t in range(near - 1):
            mid("N", t, far + t, -(near - 1 - t) * s)
        ks = own(0)
        last = [buf.at[far - 1], buf.at[far + near - 1]]
        plan.task(prio, [(key, "F", far - 1), (key, "N", near - 1), *marks(0)], end_sends,
                  lambda: end(last, slot(ks[0]) if ks else src(0)), COST["fin"], stage=ks)
        return [(key, "F", 0), (key, "N", 0)]

    def raw(prio, marks, keys):
        plan.task(prio, marks, keys, lambda: comm.start(*keys), COST["go"], raw=True)

    def spread(key, s, region, finish, some):
        far, near = nz // 2, nz // 2 - 1
        for name, count, d in (("GF", far, s), ("GN", near, -s)):
            for t in range(count):
                def ref(t=t, d=d):
                    return region(idx("z", -t * d))
                comm.msg((key, name, t), ("z", d), ref, ref, nb("z", d), group=(key, some))
        for name, count in (("GF", far), ("GN", near)):
            for t in range(count - 1):
                plan.task(4, [(key, name, t)], [(key, name, t + 1)], lambda name=name, t=t: comm.start((key, name, t + 1)), COST["go"])
        plan.task(30, [(key, "GF", far - 1), (key, "GN", near - 1)], [], finish, COST["go"])
        return [(key, "GF", 0), (key, "GN", 0)]

    def store(src, dst):
        copy = pltpu.make_async_copy(src, dst, osem.at[len(stores)])
        stores.append(copy)
        copy.start()

    def none(rel):
        return ()

    for i, (a, first_axis, sigma, u, n, prio) in enumerate(CHUNKS):
        s = sgn[sigma]

        def done(o, a=a, u=u, n=n):
            return [("D", a, o % nx, v) for v in range(u, u + n)]

        if a == 0:
            def region(k, u=u, n=n):
                return o1.at[:, pl.ds(u, n), k]

            go = spread(("g", i), s, region, lambda u=u, n=n: store(o1.at[:, pl.ds(u, n)], g1_out.at[:, pl.ds(u, n)]), o1.at[:, pl.ds(0, n), pl.ds(0, nz - 1)])
            over = ("sw", i)
            comm.msg(over, ("d", 0), lambda i=i: tbuf[i], lambda u=u, n=n: o1.at[c, pl.ds(u, n), z], partner)

            def end(last, own, i=i, u=u, n=n, over=over):
                mine = pl.ds(pl.multiple_of(c * hr, hr), hr)
                other = pl.ds(pl.multiple_of((1 - c) * hr, hr), hr)
                for m in range(n):
                    tbuf[i][m] = total([own, *last], (m, slice(None), other))
                comm.start(over)
                for m in range(n):
                    o1[c, u + m, z] = total([own, *last], (m, slice(None), mine))
        else:
            def region(k, u=u, n=n):
                return o2.at[pl.ds(u, n), k]

            go = spread(("g", i), s, region, lambda u=u, n=n: store(o2.at[pl.ds(u, n)], g2_out.at[pl.ds(u, n)]), o2.at[pl.ds(0, n), pl.ds(0, nz - 1)])
            over = ("tr", i)
            comm.msg(over, ("o", 0), lambda i=i: tbuf[i], lambda region=region: region(z), across)
            comm.remote_if[over] = x != y

            def end(last, own, i=i, u=u, n=n, over=over):
                for m in range(n):
                    tbuf[i][m] = total([own, *last], m)
                comm.start(over)

                @pl.when(x == y)
                def _():
                    for m in range(n):
                        o2[u + m, z] = tbuf[i][m]

        plan.task(3, [over], go, lambda go=go: comm.start(*go), COST["go"])
        if first_axis == "x":
            res = xbuf[i].at[nx // 2 - 1]
            pieces = functools.partial(lambda res, rel: res.at[:, idx("z", rel)], res)
            raws = chain(("z", i), "z", nz, s, zbuf[i], pieces, None, none, 5, end, [over])

            def x_end(last, own, raws=raws):
                accumulate(last[0], [last[1], own])
                comm.start(*raws)

            raws = chain(("x", i), "x", nx, s, xbuf[i], lambda rel, a=a, u=u, n=n: dwp.at[a, pl.ds(u, n), :, :, hcol(idx("x", rel))],
                         P_X, lambda rel, done=done: done(rel), 10, x_end, raws, n)
            raw(11 + prio / 100, done(2) + done(-s), raws)
        else:
            res = zbuf[i].at[nz // 2 - 1]
            raws = chain(("x", i), "x", nx, s, xbuf[i], lambda rel, res=res: res.at[:, :, hcol(idx("x", rel))], None, none, 8, end, [over])

            def z_end(last, own, raws=raws):
                accumulate(last[0], [last[1], own])
                comm.start(*raws)

            all_done = [m for o in range(nx) for m in done(o)]
            raws = chain(("z", i), "z", nz, s, zbuf[i], lambda rel, a=a, u=u, n=n: dwp.at[a, pl.ds(u, n), idx("z", rel)],
                         P_Z, lambda rel, all_done=all_done: all_done, 9, z_end, raws, n)
            raw(11 + prio / 100, all_done, raws)

    groups = yo.shape[1]
    for a, out in enumerate((y_out, dx_out)):
        for sigma in range(2):
            s = sgn[sigma]
            half = pl.ds(sigma * (groups // 2), groups // 2)

            def y_end(last, own, a=a, half=half, sigma=sigma, out=out):
                def one(ix):
                    yo[(a, sigma * (groups // 2) + ix[0], ix[1])] = total([own, *last], ix).astype(BF16)

                each(own.shape, one)
                store(yo.at[a, half], out.at[half])

            raws = chain(("y", a, sigma), "y", ny, s, yr.at[a, sigma], lambda rel, a=a, half=half: yp.at[a, half, :, :, hcol(idx("y", rel))],
                         P_Y, lambda rel, a=a: [("Y", a, rel % ny)], 12, y_end, [])
            raw(11, [("Y", a, 2), ("Y", a, -s % ny)], raws)

    tile = 256

    def rows(o):
        return pl.ds(pl.multiple_of(idx("y", o) * hb, hb), hb)

    def arrive(key, prio=6):
        plan.msg(("got", *key), ("s", key), 0)
        plan.task(prio, [key], [("got", *key)], lambda: None, COST["go"])
        return ("got", *key)

    lhs_loads = [pltpu.make_async_copy(src, lhs.at[n], isem.at[n]) for n, src in enumerate((hid, dpre))]
    for n in (1, 0):
        plan.task(0, [], [mark(("T", n))], lhs_loads[n].wait, COST["fin"])

    others = pl.ds(pl.multiple_of((1 - c) * tk, tk), tk)
    own_rows = pl.ds(pl.multiple_of(c * tk, tk), tk)
    par_loads = []
    for n, (src, box) in enumerate(((hid, hx), (dpre, dx))):
        comm.msg(("hx", n), ("d", 0), lambda src=src: src.at[others], lambda box=box: box, partner)
        raw(1, [("C", 3)], [("hx", n)])
        par_loads.append(pltpu.make_async_copy(box, par.at[n], isem.at[2 + n]))
        plan.task(6, [("hx", n)], [mark(("P", n))], par_loads[n].start, COST["go"])
    for a, o in Y_ORDER:
        if a == 0:
            comm.msg(("w", a, o), ("d", 0), lambda o=o: down.at[:, hcol(idx("y", o))], lambda o=o: wx2.at[:, hcol(idx("y", o))], partner, group=("w2", wx2))
        else:
            comm.msg(("w", a, o), ("d", 0), lambda o=o: up.at[rows(o)], lambda o=o: wx1.at[rows(o)], partner, group=("w1", wx1))
        raw(2, [("C", 3)], [("w", a, o)])

    par_seen = set()
    last_of, b = {}, 1
    for n, job in enumerate(JOBS):
        opens, closes = job[0] == "D" or job[3] == 0, job[0] == "D" or job[3] == 1
        b = 1 - b if opens else b
        keys = [("Y", job[1], job[2])] if job[0] == "Y" else [("D", job[1], job[2] % nx, v) for v in range(job[3], job[3] + job[4])]
        span = pl.ds(0, yo.shape[1] if job[0] == "Y" else job[4])
        waits = [("C", n - 1)] if n else []
        if opens and b in last_of:
            waits.append(("S", last_of[b]))
        if job[0] == "D":
            _, a, o, u, n_u = job
            waits.append(("T", 1 - a))
            ks = [stage(P_R, lambda a=a, o=o: (tok, grad)[a].at[:, hcol(idx("x", o))])]

            def value(cols, a=a, u=u, n_u=n_u, ks=ks):
                return mm_l(lhs[1 - a, :, u * nz * 8:(u + n_u) * nz * 8], slot(ks[0])[:, cols])

            dst = functools.partial(lambda a, o, u, n_u: dwp.at[a, pl.ds(u, n_u), :, :, hcol(idx("x", o))], a, o, u, n_u)
            cost = COST["D"][0] + COST["D"][1] * n_u
        else:
            _, a, o, h = job
            waits.append(("T", a))
            marks = []
            if h:
                marks = [arrive(("w", a, o))]
                waits += [("P", a), *marks]
            if a == 0:
                ks = [stage(P_R, lambda o=o, w=(down, wx2)[h]: w.at[:, hcol(idx("y", o))], marks)]
            else:
                ks = [stage(P_W, lambda o=o, w=(up, wx1)[h]: w.at[rows(o)], marks)]

            def value(cols, a=a, h=h, ks=ks):
                left = par[a] if h else lhs[a, own_rows, :]
                return mm(left, slot(ks[0])[:, cols]) if a == 0 else mm_t(left, slot(ks[0])[cols, :])

            dst = functools.partial(lambda a, o: yp.at[a, :, :, :, hcol(idx("y", o))], a, o)
            cost = COST["Y"]

        def save(b=b, dst=dst, span=span):
            return pltpu.make_async_copy(tmp.at[b, span], dst(), tsem.at[b])

        def run(b=b, value=value, save=save, job=job, span=span, opens=opens, closes=closes):
            if job[0] == "Y" and job[3] and job[1] not in par_seen:
                par_loads[job[1]].wait()
                par_seen.add(job[1])

            @pl.loop(0, hb // tile)
            def _(t):
                cols = pl.ds(pl.multiple_of(t * tile, tile), tile)
                v = value(cols).reshape((span.size,) + tmp.shape[2:4] + (tile,))
                tmp[b, span, :, :, cols] = v if opens else tmp[b, span, :, :, cols] + v

            if closes:
                save().start()

        sends = [mark(("C", n))]
        if closes:
            plan.msg(("W", n), ("s", n), 0)
            sends.append(("W", n))
            last_of[b] = n
            plan.task(2, [("W", n)], [mark(("S", n)), *[mark(key) for key in keys]], lambda save=save: save().wait(), COST["go"])
        plan.task(40, waits, sends, run, cost, stage=ks)

    order = plan.order()

    at = {}
    for n, i in enumerate(order):
        for w in plan.tasks[i][2]:
            at[w] = n
    uses = {p: [] for p in range(len(pools))}
    user = {}
    for n, i in enumerate(order):
        for k in plan.tasks[i][5]:
            uses[staged[k][0]].append(k)
            user[k] = n
    lbase, fill = 0, {}
    for p, ks in uses.items():
        depth = pools[p].shape[0]
        for n, k in enumerate(ks):
            box = pools[p].at[n % depth] if staged[k][3] is None else pools[p].at[n % depth, pl.ds(0, staged[k][3])]
            place[k] = (box, lsem.at[lbase + n % depth])
            when = -1 if n < depth else user[ks[n - depth]]
            for w in staged[k][2]:
                when = max(when, at[w])
            fill.setdefault(when, []).append(k)
        lbase += depth

    def load(k):
        return pltpu.make_async_copy(staged[k][1](), *place[k])

    for copy in lhs_loads[::-1]:
        copy.start()
    for k in fill.get(-1, ()):
        load(k).start()

    barrier = pltpu.get_barrier_semaphore()

    def tell(to):
        pl.semaphore_signal(barrier, inc=1, device_id=to, device_id_type=MESH)

    peers = [*[nb(axis, d) for axis in "zyx" for d in sgn], partner]
    for to in peers:
        tell(to)
    pl.when(x != y)(lambda: tell(across))
    run_tasks(plan, comm, order, lambda: pl.semaphore_wait(barrier, len(peers) + jnp.where(x != y, 1, 0)), load, fill)
    for copy in stores:
        copy.wait()


def reduce(dims, tok, grad, up, down, hid, dpre):
    nz, ny, nx = dims
    rows2, hh = tok.shape
    fc = hid.shape[1]
    tk, hb = rows2 // 2, hh // ny
    hr = hb // 2
    nu = fc // (nz * SUB)
    g = tk // (SUB * SUB)
    vm = pltpu.VMEM

    def per(shape):
        return [vm(shape(axis, n), F32) for _, axis, _, _, n, *_ in CHUNKS]

    def fin(shape):
        return [vm((n, SUB, hr if a == 0 else hb), F32) for a, _, _, _, n, *_ in CHUNKS]

    n0 = max(chunk[4] for chunk in CHUNKS)
    scratch = [
        *per(lambda axis, n: (nx - 1, n, nz, SUB, hb) if axis == "x" else (nx - 1, n, SUB, hb)),
        *per(lambda axis, n: (nz - 1, n, SUB, hb) if axis == "x" else (nz - 1, n, SUB, hh)),
        *fin(0),
        vm((2, nu, nz, SUB, hr), F32),
        vm((nu, nz, SUB, hb), F32),
        vm((2, 2, ny - 1, g // 2, SUB, SUB, hb), F32),
        vm((2, g, SUB, SUB, hb), BF16),
        vm((2, rows2, fc), BF16),
        vm((2, tk, fc), BF16),
        vm((2, g, SUB, SUB, hb), F32),
        vm((3, n0, nz, SUB, hb), F32),
        vm((6, n0, SUB, hh), F32),
        vm((2, g // 2, SUB, SUB, hb), F32),
        vm((3, rows2, hb), BF16),
        vm((3, hb, fc), BF16),
        pltpu.SemaphoreType.DMA((80,)),
        pltpu.SemaphoreType.DMA((330,)),
        pltpu.SemaphoreType.DMA((18,)),
        pltpu.SemaphoreType.DMA((24,)),
        pltpu.SemaphoreType.DMA((6,)),
        pltpu.SemaphoreType.DMA((2,)),
    ]
    sds = jax.ShapeDtypeStruct
    outs = pl.pallas_call(
        functools.partial(reduce_kernel, dims),
        out_shape=[
            sds((g, SUB, SUB, hb), BF16),
            sds((g, SUB, SUB, hb), BF16),
            sds((2, nu, nz, SUB, hr), F32),
            sds((nu, nz, SUB, hb), F32),
            sds((2, nu, nz, SUB, hh), F32),
            sds((2, g, SUB, SUB, hh), F32),
            sds(up.shape, BF16),
            sds(down.shape, BF16),
            sds((tk, fc), BF16),
            sds((tk, fc), BF16),
        ],
        in_specs=[ANY] * 6,
        out_specs=[ANY] * 10,
        scratch_shapes=scratch,
        compiler_params=pltpu.CompilerParams(collective_id=1, has_side_effects=True, vmem_limit_bytes=VMEM_LIMIT),
        name="reduce",
    )(tok, grad, up, down, hid, dpre)
    y, dx, g1, g2 = outs[:4]
    return finish(y.reshape(tk, hb), dx.reshape(tk, hb), g1.reshape(2 * fc, hr), g2.reshape(fc, hb))


def finish_kernel(*refs):
    *arrays, turned, isem, osem = refs
    n, parts = isem.shape
    ins, outs, boxes = (arrays[k * n:(k + 1) * n] for k in range(3))

    def span(ref, k):
        size = ref.shape[0] // parts
        return pl.ds(k * size, size)

    def fetch(i, k):
        return pltpu.make_async_copy(ins[i].at[span(ins[i], k)], boxes[i].at[span(ins[i], k)], isem.at[i, k])

    def put(i, k):
        if i == 0:
            cols = span(ins[i], k)
            return pltpu.make_async_copy(turned.at[:, cols], outs[i].at[:, cols], osem.at[i, k])
        return pltpu.make_async_copy(boxes[i].at[span(ins[i], k)], outs[i].at[span(ins[i], k)], osem.at[i, k])

    todo = list(itertools.product(range(n), range(parts)))
    for i, k in todo:
        fetch(i, k).start()
    for i, k in todo:
        fetch(i, k).wait()
        if i == 0:
            rows = span(ins[i], k)
            turned[:, rows] = boxes[i][rows, :].T
        put(i, k).start()
    for i, k in todo:
        put(i, k).wait()


def finish(y, dx, g1, g2):
    ins = (g1, g2, y, dx)
    turned = jax.ShapeDtypeStruct(g1.shape[::-1], F32)
    parts = 4
    out = pl.pallas_call(
        finish_kernel,
        out_shape=[turned, *[jax.ShapeDtypeStruct(v.shape, v.dtype) for v in ins[1:]]],
        in_specs=[ANY] * len(ins),
        out_specs=[ANY] * len(ins),
        scratch_shapes=[*[pltpu.VMEM(v.shape, v.dtype) for v in ins], pltpu.VMEM(turned.shape, F32), *[pltpu.SemaphoreType.DMA((len(ins), parts))] * 2],
        compiler_params=pltpu.CompilerParams(vmem_limit_bytes=VMEM_LIMIT),
        name="finish",
    )(*ins)
    return out[2], out[3], out[0], out[1]


def solution(mesh):
    act_spec = P(("depth", "row"), "col")
    weight_spec = P("row", "col")
    dims = (mesh.shape["depth"], mesh.shape["col"], mesh.shape["row"] // 2)

    def local_block(tok_blk, up_blk, down_blk, grad_blk):
        return reduce(dims, *gather(dims, tok_blk, grad_blk, up_blk, down_blk))

    return jax.shard_map(local_block, mesh=mesh, in_specs=(act_spec, weight_spec, weight_spec, act_spec), out_specs=(act_spec, act_spec, weight_spec, weight_spec), check_vma=False)
```

```python
import functools
import itertools
import string

import jax
import jax.numpy as jnp
from jax import lax
from jax.experimental import pallas as pl
from jax.experimental.pallas import tpu as pltpu
from jax.sharding import PartitionSpec as P

MESH = pl.DeviceIdType.MESH
ANY = pl.BlockSpec(memory_space=pl.ANY)
F32 = jnp.float32
SUB = 8
BF16 = jnp.bfloat16

TOP = (12, 10)
UNITS = 16
FAR_FIRST = (2, 1, 3, 0)
Y_ORDER = [(a, o) for a in range(2) for o in FAR_FIRST]
DIGITS = string.digits + string.ascii_letters
JOB_ORDER = "10svut2y64z3w5x8rdho9b7AqcfamCBpilgFEnGejkDH"
RANKS = "107kl30b24216589a"
SIDES = "01010010101011001"


def chunk_list():
    def run(a, axis, lo, hi, n=2):
        return [(a, axis, u, min(n, hi - u)) for u in range(lo, hi, n)]

    first, last = TOP
    parts = run(1, "z", last, UNITS) + run(0, "z", first, UNITS) + run(0, "x", 0, first) + run(1, "x", 0, last - 2) + run(1, "x", last - 2, last, 1)
    return [(a, axis, int(side), u, n, DIGITS.index(rank)) for (a, axis, u, n), side, rank in zip(parts, SIDES, RANKS)]


CHUNKS = chunk_list()


def job_list():
    def block(a, lo, hi):
        return [[("D", a, o, u, min(4, hi - u))] for u in range(lo, hi, 4) for o in FAR_FIRST]

    first, last = TOP
    jobs = block(0, 0, first) + block(1, 0, last) + block(0, first, UNITS) + block(1, last, UNITS) + [[("Y", a, o, h) for h in range(2)] for a, o in Y_ORDER]
    return [job for c in JOB_ORDER for job in jobs[DIGITS.index(c)]]


JOBS = job_list()
COST = {"D": (0.5, 0.15), "Y": 1.2, "fin": 0.1, "go": 0.03, "U": 4.0, "A": 0.8, "act": 3.0}
SLACK = 20.0
VMEM_LIMIT = 66_500_000


def gelu_fn(pre_act):
    return jax.nn.gelu(pre_act, approximate=True)


class Plan:
    def __init__(self, rates, window):
        self.rates, self.window = rates, window
        self.tasks, self.size, self.link = [], {}, {}

    def msg(self, key, link, nbytes):
        self.size[key], self.link[key] = nbytes, link

    def task(self, prio, waits, sends, run, cost=0.3, stage=(), raw=False):
        self.tasks.append((prio, tuple(waits), tuple(sends), run, cost, tuple(stage), raw))

    def order(self):
        free, arrive, out = {}, {}, []
        self.when, self.arrive = [], arrive
        now, left = 2.5, list(range(len(self.tasks)))
        while left:
            best = None
            for i in left:
                prio, waits, sends, _, _, _, raw = self.tasks[i]
                if any(w not in arrive for w in waits):
                    continue
                ready = max([arrive[w] for w in waits], default=0.0)
                if raw:
                    ready = max([ready] + [free.get(self.link[s], 0.0) - self.window for s in sends])
                key = (max(ready, now), prio, i)
                if best is None or key < best:
                    best = key
            at, _, i = best
            left.remove(i)
            out.append(i)
            now = at + self.tasks[i][4]
            self.when.append(now)
            for s in self.tasks[i][2]:
                rate, lat = self.rates[self.link[s][0]]
                took = self.size[s] / rate
                if self.link[s][0] in "to":
                    share = 0.5 if self.link[s][0] == "t" else 1.5
                    ways = [(axis, d) for axis in "xy" for d in (1, -1)]
                    done = max(now, *[free.get(way, 0.0) for way in ways]) + took
                    for way in ways:
                        free[way] = max(now, free.get(way, 0.0)) + took * share
                else:
                    done = max(now, free.get(self.link[s], 0.0)) + took
                    free[self.link[s]] = done
                arrive[s] = done + lat
        self.end = max(now, max(arrive.values()))
        return out


RATES = {axis: (45e3, 2.2) for axis in "xyz"}
RATES.update(d=(450e3, 3.0), t=(45e3, 5.0), o=(45e3, 7.0), l=(1e12, 0.0), s=(1e12, 2.0))
WINDOW = 10.0


class Comm:
    def __init__(self, plan, ssem, rsem):
        self.plan, self.ssem, self.rsem = plan, ssem, rsem
        self.make, self.meet, self.slot, self.remote_if, self.groups, self.grouped, self.flying = {}, {}, {}, {}, {}, set(), []

    def msg(self, key, link, src, dst, to, mail=None, group=None):
        i = len(self.slot)
        self.slot[key] = i
        there, here = mail or (i, i)
        name, ref = group or (key, None)
        g, _, _ = self.groups.setdefault(name, (len(self.groups), ref, to))
        if group:
            self.grouped.add(key)

        def make(r):
            return pltpu.make_async_remote_copy(
                src_ref=src(), dst_ref=dst(), send_sem=self.ssem.at[g], recv_sem=self.rsem.at[r], device_id=to, device_id_type=MESH)

        self.make[key] = lambda: make(there)
        self.meet[key] = lambda: make(here)
        shape = src().shape
        nbytes = functools.reduce(lambda a, b: a * b, shape, 1) * src().dtype.itemsize
        self.plan.msg(key, link, nbytes)

    def each(self, keys, make, act):
        for key in keys:
            if key in self.remote_if:
                pl.when(self.remote_if[key])(lambda key=key: act(make[key]()))
            elif key in make:
                act(make[key]())

    def start(self, *keys):
        self.flying.extend(key for key in keys if key not in self.grouped)
        self.each(keys, self.make, lambda copy: copy.start())

    def finish(self):
        self.sent(float("inf"))
        for g, ref, to in self.groups.values():
            if ref is not None:
                pltpu.make_async_remote_copy(src_ref=ref, dst_ref=ref, send_sem=self.ssem.at[g], recv_sem=self.rsem.at[g], device_id=to, device_id_type=MESH).wait_send()

    def wait(self, *keys):
        self.each(keys, self.meet, lambda copy: copy.wait_recv())

    def sent(self, before):
        keys = [key for key in self.flying if self.plan.arrive[key] <= before]
        self.flying = [key for key in self.flying if self.plan.arrive[key] > before]
        self.each(keys, self.make, lambda copy: copy.wait_send())


def run_tasks(plan, comm, order, ready, load=None, fill={}):
    heard = set()
    for n, i in enumerate(order):
        _, waits, sends, run, _, ks, _ = plan.tasks[i]
        if ready and any(key in comm.make for key in sends):
            ready()
            ready = None
        with jax.named_scope(f"w{n}"):
            comm.wait(*[w for w in waits if w not in heard])
            heard.update(waits)
        with jax.named_scope(f"l{n}"):
            for k in ks:
                load(k).wait()
        with jax.named_scope(f"r{n}"):
            run()
        for k in fill.get(n, ()):
            load(k).start()
        comm.sent(plan.when[n] - SLACK)
    comm.finish()


def where_am_i():
    z, y, r = lax.axis_index("depth"), lax.axis_index("col"), lax.axis_index("row")
    return z, y, lax.div(r, 2), lax.rem(r, 2)


def each(shape, fn):
    lead = shape[:-2]
    big = max(range(len(lead)), key=lambda d: lead[d])
    looped = lead[big] >= 8

    def rest(k):
        for ix in itertools.product(*[range(n) if not (looped and d == big) else (k,) for d, n in enumerate(lead)]):
            fn(ix)

    if looped:
        pl.loop(0, lead[big])(rest)
    else:
        rest(None)


def total(refs, ix):
    return functools.reduce(lambda a, b: a + b, [ref[ix] for ref in refs])


def accumulate(dst, others):
    def one(ix):
        dst[ix] = total([dst, *others], ix)

    each(dst.shape, one)


def mm(a, b):
    return jnp.dot(a, b, preferred_element_type=F32)


def mm_l(a, b):
    return lax.dot_general(a, b, (((0,), (0,)), ((), ())), preferred_element_type=F32)


def mm_t(a, b):
    return lax.dot_general(a, b, (((1,), (1,)), ((), ())), preferred_element_type=F32)


def gather_kernel(dims, x_ref, g_ref, w1_ref, w2_ref, xf, gf, w1f, w2f, hid, dpre,
                  bx, bg, bw1, bw2, vw2, u, da, ha, hd, ssem, rsem, lsem, osem, asem):
    nz, ny, nx = dims
    z, y, x, c = where_am_i()
    tk, hb = x_ref.shape
    fc = w2_ref.shape[0]
    hr, fz, half = hb // 2, fc // nz, tk // 2
    plan = Plan(RATES, WINDOW)
    comm = Comm(plan, ssem, rsem)
    ways = (1, -1)

    def idx(axis, d):
        at, n = {"z": (z, nz), "y": (y, ny), "x": (x, nx)}[axis]
        return lax.rem(at + (d % n), n)

    def nb(axis, d):
        i = idx(axis, d)
        return {"z": {"depth": i}, "y": {"col": i}, "x": {"row": 2 * i + c}}[axis]

    partner = {"row": 2 * x + (1 - c)}

    def at(i, size):
        return pl.ds(pl.multiple_of(i * size, size), size)

    def block(full, core, o, part=None):
        rows = at(core, tk) if part is None else pl.ds(pl.multiple_of(core * tk + part * half, half), half)
        return full.at[rows, at(idx("y", o), hb)]

    def wblock(o, core):
        return bw1.at[at(2 * idx("x", o) + core, hr), :]

    def piece(d, o):
        return bw2.at[at(idx("z", d), fz), at(idx("y", o), hb)]

    stores = []

    def store(src, dst):
        copy = pltpu.make_async_copy(src, dst, osem.at[len(stores)])
        stores.append(copy)
        copy.start()

    def mark(key):
        plan.msg(key, ("l", key), 0)
        return key

    loads = {}

    def load(name, src, dst):
        loads[name] = pltpu.make_async_copy(src, dst, lsem.at[len(loads)])
        plan.task(len(loads) / 10, [], [mark(name)], loads[name].wait, COST["go"])

    load("s", w2_ref.at[at(z, fz), :], vw2)
    load("w", w1_ref.at[:, at(c, fc)], wblock(0, c))
    load("x", x_ref, block(bx, c, 0))
    load("g", g_ref, block(bg, c, 0))
    self_copy = pltpu.make_async_copy(w2_ref.at[at(z, fz), :], piece(0, 0), lsem.at[len(loads)])

    def raw(prio, waits, keys):
        plan.task(prio, waits, keys, lambda: comm.start(*keys), COST["go"], raw=True)

    def passed(prio, wait, keys, key=None):
        plan.task(prio, [wait], [*keys, mark(("in", *wait) if key is None else key)], lambda: comm.start(*keys), COST["go"])

    for o in (1, -1, 2, 0):
        o = o % ny
        to = {"row": 2 * idx("x", o) + c, "col": x}
        comm.msg(("s", o), ("t", 0), lambda: vw2, lambda: piece(0, 0), to, mail=(y, idx("y", o)))
    comm.remote_if[("s", 0)] = x != y
    plan.task(1, ["s"], [("s", o) for o in range(ny)], lambda: comm.start(*[("s", o) for o in range(ny)]), COST["go"])
    whole = {d: [] for d in range(nz)}
    far = nz // 2
    for o in range(ny):
        for w in ways:
            steps = far if (w > 0) == (o % 2 == 0) else far - 1
            for t in range(steps):
                comm.msg(("z", o, w, t), ("z", w), lambda o=o, w=w, t=t: piece(-w * t, o), lambda o=o, w=w, t=t: piece(-w * t, o), nb("z", w))
                nxt = [("z", o, w, t + 1)] if t + 1 < steps else []
                key = ("w2", o, (-w * (t + 1)) % nz)
                passed(4, ("z", o, w, t), nxt, key)
                whole[key[2]].append(key)
        first = [("z", o, w, 0) for w in ways]

        def slice_in(o=o, first=first):
            if o == 0:
                pl.when(x == y)(self_copy.wait)
            comm.start(*first)

        plan.task(3, [("s", o)], [*first, mark(("w2", o, 0))], slice_in, COST["go"])
        whole[0].append(("w2", o, 0))

    comm.msg(("pw",), ("d", 0), lambda: w1_ref.at[:, at(1 - c, fc)], lambda: wblock(0, c), partner)
    raw(1.1, [], [("pw",)])
    w1_in = {0: ["w"], 1: [], -1: [], 2: []}
    for own in (True, False):
        core = c if own else 1 - c
        for w in ways:
            comm.msg(("wa", own, w), ("x", w), lambda core=core: wblock(0, core), lambda core=core: wblock(0, core), nb("x", w))
    raw(1.2, ["w"], [("wa", True, w) for w in ways])
    passed(5, ("pw",), [("wa", False, w) for w in ways])
    w1_in[0].append(("in", "pw"))
    for own, w in ((True, 1), (False, -1)):
        core = c if own else 1 - c
        comm.msg(("wf", w), ("x", w), lambda core=core, w=w: wblock(-w, core), lambda core=core, w=w: wblock(-w, core), nb("x", w))
        passed(6, ("wa", own, w), [("wf", w)])
        passed(6, ("wa", not own, w), [])
        passed(6, ("wf", w), [])
        w1_in[-w] += [("in", "wa", True, w), ("in", "wa", False, w)]
        w1_in[2].append(("in", "wf", w))

    arrived = {}
    for a, (full, name) in enumerate(((bx, "x"), (bg, "g"))):
        arrived[a] = [name]
        for w in ways:
            for p in range(2):
                comm.msg((name, w, p), ("y", w), lambda full=full, p=p: block(full, c, 0, p), lambda full=full, p=p: block(full, c, 0, p), nb("y", w))
            p = 0 if w > 0 else 1
            comm.msg((name, "f", w), ("y", w), lambda full=full, w=w, p=p: block(full, c, -w, p), lambda full=full, w=w, p=p: block(full, c, -w, p), nb("y", w))

        def share(key, o, p, full=full, name=name, a=a):
            comm.msg((name, "d", *key), ("d", 0), lambda: block(full, c, o, p), lambda: block(full, c, o, p), partner)
            passed(20, (name, "d", *key), [])
            arrived[a].append(("in", name, "d", *key))
            return (name, "d", *key)

        plan.task(2 + a, [name], [share((0,), 0, None)], lambda name=name: comm.start((name, "d", 0)), COST["go"])
        for w in ways:
            p = 0 if w > 0 else 1
            for q in range(2):
                keys = [share((-w, q), -w, q)] + ([(name, "f", w)] if q == p else [])
                passed(7, (name, w, q), keys)
                arrived[a].append(("in", name, w, q))
            passed(7, (name, "f", w), [share((2, p), 2, p)])
            arrived[a].append(("in", name, "f", w))
    for n, (name, late) in enumerate(itertools.product("gx", (False, True))):
        raw(1.3 + n / 100, [name], [(name, w, 1 if (w > 0) == late else 0) for w in ways])
    for name, here, src, dst in (("X", arrived[0], bx, xf), ("G", arrived[1], bg, gf), ("W2", [key for d in whole for key in whole[d]], bw2, w2f),
                                 ("W1", [key for o in w1_in for key in w1_in[o]], bw1, w1f)):
        plan.task(9, here, [mark(name)], functools.partial(store, src, dst), COST["go"])

    tile = 256

    e = lax.rem(y - x + ny, ny)
    early = lax.div(e, 2) * (3 - e), 1 + 2 * lax.div(e, 2)
    late = 2, 4 - early[0] - early[1]

    def up(ts, first):
        js = [lax.rem(x + t, nx) for t in ts]

        @pl.loop(0, fc // tile)
        def _(i):
            cols = at(i, tile)
            v = sum(mm(bx[:, at(j, hb)], bw1[at(j, hb), cols]) for j in js)
            u[:, cols] = v if first else u[:, cols] + v

    near = ["w", *[key for key in w1_in[0] + w1_in[1] + w1_in[-1]], *[key for key in arrived[0] if not (key[:3] == ("in", "x", "f") or key[:4] == ("in", "x", "d", 2))]]
    plan.task(30, near, [mark(("U", 0))], functools.partial(up, early, True), COST["U"])
    plan.task(30, [("U", 0), "X", "W1"], [mark(("U", 1))], functools.partial(up, late, False), COST["U"])

    def down(ds):
        spans = [at(idx("z", d), fz) for d in ds]

        @pl.loop(0, 2)
        def _(i):
            rows = at(i, tk)
            v = mm_t(bg[rows, :], jnp.concatenate([bw2[span, :] for span in spans]))
            for n, span in enumerate(spans):
                da[rows, span] = v[:, n * fz:(n + 1) * fz]

    for d in range(far + 1):
        ds = sorted({d, -d % nz})
        plan.task(31, ["G", *[key for e in ds for key in whole[e]]], [mark(("A", d))], functools.partial(down, ds), COST["A"] * len(ds) + 1)

    parts = tk // tile
    acts = [[pltpu.make_async_copy(src.at[at(h, tk), :], dst.at[at(h, tk), :], asem.at[h, n]) for n, (src, dst) in enumerate(((ha, hid), (hd, dpre)))] for h in range(2)]

    def act():
        for half, copies in enumerate(acts):
            @pl.loop(0, parts * (fc // fz))
            def _(i):
                rows, cols = at(half * parts + lax.rem(i, parts), tile), at(lax.div(i, parts), fz)
                h, vjp = jax.vjp(gelu_fn, u[rows, cols])
                ha[rows, cols] = h.astype(BF16)
                hd[rows, cols] = vjp(da[rows, cols])[0].astype(BF16)

            for copy in copies:
                copy.start()

    plan.task(32, [("U", 1), *[("A", d) for d in range(far + 1)]], [], act, COST["act"])

    order = plan.order()
    for copy in loads.values():
        copy.start()
    pl.when(x == y)(self_copy.start)

    barrier = pltpu.get_barrier_semaphore()

    def tell(to):
        pl.semaphore_signal(barrier, inc=1, device_id=to, device_id_type=MESH)

    for to in (*[nb(axis, d) for axis in "zyx" for d in ways], partner):
        tell(to)
    for o in range(1, ny):
        tell({"row": 2 * y + c, "col": idx("y", o)})
    pl.when(x != y)(lambda: tell({"row": 2 * y + c, "col": y}))
    run_tasks(plan, comm, order, lambda: pl.semaphore_wait(barrier, 6 + ny + jnp.where(x != y, 1, 0)))
    for copy in [*stores, *sum(acts, [])]:
        copy.wait()


def gather(dims, tok, grad, up, down):
    tk, hb = tok.shape
    fc = down.shape[0]
    nz, ny, nx = dims
    sds, vm = jax.ShapeDtypeStruct, pltpu.VMEM
    tokens, first, second, mid = (2 * tk, ny * hb), (nx * hb, fc), (fc, ny * hb), (2 * tk, fc)
    return pl.pallas_call(
        functools.partial(gather_kernel, dims),
        out_shape=[sds(shape, BF16) for shape in (tokens, tokens, first, second, mid, mid)],
        in_specs=[ANY] * 4,
        out_specs=[ANY] * 6,
        scratch_shapes=[
            *[vm(shape, BF16) for shape in (tokens, tokens, first, second, (fc // nz, hb))],
            vm(mid, F32),
            vm(mid, F32),
            vm(mid, BF16),
            vm(mid, BF16),
            pltpu.SemaphoreType.DMA((65,)),
            pltpu.SemaphoreType.DMA((65,)),
            pltpu.SemaphoreType.DMA((5,)),
            pltpu.SemaphoreType.DMA((9,)),
            pltpu.SemaphoreType.DMA((2, 2)),
        ],
        compiler_params=pltpu.CompilerParams(collective_id=0, has_side_effects=True, vmem_limit_bytes=VMEM_LIMIT),
        name="gather",
    )(tok, grad, up, down)


def reduce_kernel(dims, tok, grad, up, down, hid, dpre,
                  y_out, dx_out, g1_out, g2_out, dwp, yp, wx1, wx2, hx, dx, *scratch):
    nz, ny, nx = dims
    z, y, x, c = where_am_i()
    hb = y_out.shape[-1]
    tk = tok.shape[0] // 2
    hr = hb // 2
    fc = hid.shape[1]
    nu = fc // (nz * 8)
    sgn = (1, -1)
    scratch = list(scratch)

    def grab(n):
        return [scratch.pop(0) for _ in range(n)]

    nc = len(CHUNKS)
    xbuf, zbuf, tbuf = grab(nc), grab(nc), grab(nc)
    o1, o2, yr, yo, lhs, par, tmp = grab(7)
    pools = grab(5)
    ssem, rsem, lsem, osem, isem, tsem = grab(6)
    P_X, P_Z, P_Y, P_R, P_W = range(5)

    plan = Plan(RATES, WINDOW)
    comm = Comm(plan, ssem, rsem)

    def idx(axis, d):
        at, n = {"z": (z, nz), "y": (y, ny), "x": (x, nx)}[axis]
        return lax.rem(at + (d % n), n)

    def nb(axis, d):
        i = idx(axis, d)
        return {"z": {"depth": i}, "y": {"col": i}, "x": {"row": 2 * i + c}}[axis]

    partner = {"row": 2 * x + (1 - c)}
    across = {"row": 2 * y + c, "col": x}

    def hcol(j):
        return pl.ds(pl.multiple_of(j * hb, hb), hb)

    staged, stores, place = [], [], {}

    def stage(pool, src, marks=(), n=None):
        staged.append((pool, src, tuple(marks), n))
        return len(staged) - 1

    def slot(k):
        return place[k][0]

    def mark(key):
        plan.msg(key, ("l", key), 0)
        return key

    def chain(key, axis, n, s, buf, src, pool, marks, prio, end, end_sends, units=None):
        far, near = n // 2, n // 2 - 1
        for t in range(far):
            comm.msg((key, "F", t), (axis, s), (lambda: src(far * s)) if t == 0 else (lambda t=t: buf.at[t - 1]), lambda t=t: buf.at[t], nb(axis, s), group=(key, buf))
        for t in range(near):
            comm.msg((key, "N", t), (axis, -s), (lambda: src(-near * s)) if t == 0 else (lambda t=t: buf.at[far + t - 1]), lambda t=t: buf.at[far + t], nb(axis, -s), group=(key, buf))

        def own(rel):
            return [] if pool is None else [stage(pool, lambda: src(rel), marks(rel), units)]

        def mid(name, t, at, rel):
            ks = own(rel)

            def run():
                accumulate(buf.at[at], [slot(ks[0]) if ks else src(rel)])
                comm.start((key, name, t + 1))

            plan.task(prio, [(key, name, t), *marks(rel)], [(key, name, t + 1)], run, COST["go"], stage=ks)

        for t in range(far - 1):
            mid("F", t, t, (far - 1 - t) * s)
        for t in range(near - 1):
            mid("N", t, far + t, -(near - 1 - t) * s)
        ks = own(0)
        last = [buf.at[far - 1], buf.at[far + near - 1]]
        plan.task(prio, [(key, "F", far - 1), (key, "N", near - 1), *marks(0)], end_sends,
                  lambda: end(last, slot(ks[0]) if ks else src(0)), COST["fin"], stage=ks)
        return [(key, "F", 0), (key, "N", 0)]

    def raw(prio, marks, keys):
        plan.task(prio, marks, keys, lambda: comm.start(*keys), COST["go"], raw=True)

    def spread(key, s, region, finish, some):
        far, near = nz // 2, nz // 2 - 1
        for name, count, d in (("GF", far, s), ("GN", near, -s)):
            for t in range(count):
                def ref(t=t, d=d):
                    return region(idx("z", -t * d))
                comm.msg((key, name, t), ("z", d), ref, ref, nb("z", d), group=(key, some))
        for name, count in (("GF", far), ("GN", near)):
            for t in range(count - 1):
                plan.task(4, [(key, name, t)], [(key, name, t + 1)], lambda name=name, t=t: comm.start((key, name, t + 1)), COST["go"])
        plan.task(30, [(key, "GF", far - 1), (key, "GN", near - 1)], [], finish, COST["go"])
        return [(key, "GF", 0), (key, "GN", 0)]

    def store(src, dst):
        copy = pltpu.make_async_copy(src, dst, osem.at[len(stores)])
        stores.append(copy)
        copy.start()

    def none(rel):
        return ()

    for i, (a, first_axis, sigma, u, n, prio) in enumerate(CHUNKS):
        s = sgn[sigma]

        def done(o, a=a, u=u, n=n):
            return [("D", a, o % nx, v) for v in range(u, u + n)]

        if a == 0:
            def region(k, u=u, n=n):
                return o1.at[:, pl.ds(u, n), k]

            go = spread(("g", i), s, region, lambda u=u, n=n: store(o1.at[:, pl.ds(u, n)], g1_out.at[:, pl.ds(u, n)]), o1.at[:, pl.ds(0, n), pl.ds(0, nz - 1)])
            over = ("sw", i)
            comm.msg(over, ("d", 0), lambda i=i: tbuf[i], lambda u=u, n=n: o1.at[c, pl.ds(u, n), z], partner)

            def end(last, own, i=i, u=u, n=n, over=over):
                mine = pl.ds(pl.multiple_of(c * hr, hr), hr)
                other = pl.ds(pl.multiple_of((1 - c) * hr, hr), hr)
                for m in range(n):
                    tbuf[i][m] = total([own, *last], (m, slice(None), other))
                comm.start(over)
                for m in range(n):
                    o1[c, u + m, z] = total([own, *last], (m, slice(None), mine))
        else:
            def region(k, u=u, n=n):
                return o2.at[pl.ds(u, n), k]

            go = spread(("g", i), s, region, lambda u=u, n=n: store(o2.at[pl.ds(u, n)], g2_out.at[pl.ds(u, n)]), o2.at[pl.ds(0, n), pl.ds(0, nz - 1)])
            over = ("tr", i)
            comm.msg(over, ("o", 0), lambda i=i: tbuf[i], lambda region=region: region(z), across)
            comm.remote_if[over] = x != y

            def end(last, own, i=i, u=u, n=n, over=over):
                for m in range(n):
                    tbuf[i][m] = total([own, *last], m)
                comm.start(over)

                @pl.when(x == y)
                def _():
                    for m in range(n):
                        o2[u + m, z] = tbuf[i][m]

        plan.task(3, [over], go, lambda go=go: comm.start(*go), COST["go"])
        if first_axis == "x":
            res = xbuf[i].at[nx // 2 - 1]
            pieces = functools.partial(lambda res, rel: res.at[:, idx("z", rel)], res)
            raws = chain(("z", i), "z", nz, s, zbuf[i], pieces, None, none, 5, end, [over])

            def x_end(last, own, raws=raws):
                accumulate(last[0], [last[1], own])
                comm.start(*raws)

            raws = chain(("x", i), "x", nx, s, xbuf[i], lambda rel, a=a, u=u, n=n: dwp.at[a, pl.ds(u, n), :, :, hcol(idx("x", rel))],
                         P_X, lambda rel, done=done: done(rel), 10, x_end, raws, n)
            raw(11 + prio / 100, done(2) + done(-s), raws)
        else:
            res = zbuf[i].at[nz // 2 - 1]
            raws = chain(("x", i), "x", nx, s, xbuf[i], lambda rel, res=res: res.at[:, :, hcol(idx("x", rel))], None, none, 8, end, [over])

            def z_end(last, own, raws=raws):
                accumulate(last[0], [last[1], own])
                comm.start(*raws)

            all_done = [m for o in range(nx) for m in done(o)]
            raws = chain(("z", i), "z", nz, s, zbuf[i], lambda rel, a=a, u=u, n=n: dwp.at[a, pl.ds(u, n), idx("z", rel)],
                         P_Z, lambda rel, all_done=all_done: all_done, 9, z_end, raws, n)
            raw(11 + prio / 100, all_done, raws)

    groups = yo.shape[1]
    for a, out in enumerate((y_out, dx_out)):
        for sigma in range(2):
            s = sgn[sigma]
            half = pl.ds(sigma * (groups // 2), groups // 2)

            def y_end(last, own, a=a, half=half, sigma=sigma, out=out):
                def one(ix):
                    yo[(a, sigma * (groups // 2) + ix[0], ix[1])] = total([own, *last], ix).astype(BF16)

                each(own.shape, one)
                store(yo.at[a, half], out.at[half])

            raws = chain(("y", a, sigma), "y", ny, s, yr.at[a, sigma], lambda rel, a=a, half=half: yp.at[a, half, :, :, hcol(idx("y", rel))],
                         P_Y, lambda rel, a=a: [("Y", a, rel % ny)], 12, y_end, [])
            raw(11, [("Y", a, 2), ("Y", a, -s % ny)], raws)

    tile = 256

    def rows(o):
        return pl.ds(pl.multiple_of(idx("y", o) * hb, hb), hb)

    def arrive(key, prio=6):
        plan.msg(("got", *key), ("s", key), 0)
        plan.task(prio, [key], [("got", *key)], lambda: None, COST["go"])
        return ("got", *key)

    lhs_loads = [pltpu.make_async_copy(src, lhs.at[n], isem.at[n]) for n, src in enumerate((hid, dpre))]
    for n in (1, 0):
        plan.task(0, [], [mark(("T", n))], lhs_loads[n].wait, COST["fin"])

    others = pl.ds(pl.multiple_of((1 - c) * tk, tk), tk)
    own_rows = pl.ds(pl.multiple_of(c * tk, tk), tk)
    par_loads = []
    for n, (src, box) in enumerate(((hid, hx), (dpre, dx))):
        comm.msg(("hx", n), ("d", 0), lambda src=src: src.at[others], lambda box=box: box, partner)
        raw(1, [("C", 3)], [("hx", n)])
        par_loads.append(pltpu.make_async_copy(box, par.at[n], isem.at[2 + n]))
        plan.task(6, [("hx", n)], [mark(("P", n))], par_loads[n].start, COST["go"])
    for a, o in Y_ORDER:
        if a == 0:
            comm.msg(("w", a, o), ("d", 0), lambda o=o: down.at[:, hcol(idx("y", o))], lambda o=o: wx2.at[:, hcol(idx("y", o))], partner, group=("w2", wx2))
        else:
            comm.msg(("w", a, o), ("d", 0), lambda o=o: up.at[rows(o)], lambda o=o: wx1.at[rows(o)], partner, group=("w1", wx1))
        raw(2, [("C", 3)], [("w", a, o)])

    par_seen = set()
    last_of, b = {}, 1
    for n, job in enumerate(JOBS):
        opens, closes = job[0] == "D" or job[3] == 0, job[0] == "D" or job[3] == 1
        b = 1 - b if opens else b
        keys = [("Y", job[1], job[2])] if job[0] == "Y" else [("D", job[1], job[2] % nx, v) for v in range(job[3], job[3] + job[4])]
        span = pl.ds(0, yo.shape[1] if job[0] == "Y" else job[4])
        waits = [("C", n - 1)] if n else []
        if opens and b in last_of:
            waits.append(("S", last_of[b]))
        if job[0] == "D":
            _, a, o, u, n_u = job
            waits.append(("T", 1 - a))
            ks = [stage(P_R, lambda a=a, o=o: (tok, grad)[a].at[:, hcol(idx("x", o))])]

            def value(cols, a=a, u=u, n_u=n_u, ks=ks):
                return mm_l(lhs[1 - a, :, u * nz * 8:(u + n_u) * nz * 8], slot(ks[0])[:, cols])

            dst = functools.partial(lambda a, o, u, n_u: dwp.at[a, pl.ds(u, n_u), :, :, hcol(idx("x", o))], a, o, u, n_u)
            cost = COST["D"][0] + COST["D"][1] * n_u
        else:
            _, a, o, h = job
            waits.append(("T", a))
            marks = []
            if h:
                marks = [arrive(("w", a, o))]
                waits += [("P", a), *marks]
            if a == 0:
                ks = [stage(P_R, lambda o=o, w=(down, wx2)[h]: w.at[:, hcol(idx("y", o))], marks)]
            else:
                ks = [stage(P_W, lambda o=o, w=(up, wx1)[h]: w.at[rows(o)], marks)]

            def value(cols, a=a, h=h, ks=ks):
                left = par[a] if h else lhs[a, own_rows, :]
                return mm(left, slot(ks[0])[:, cols]) if a == 0 else mm_t(left, slot(ks[0])[cols, :])

            dst = functools.partial(lambda a, o: yp.at[a, :, :, :, hcol(idx("y", o))], a, o)
            cost = COST["Y"]

        def save(b=b, dst=dst, span=span):
            return pltpu.make_async_copy(tmp.at[b, span], dst(), tsem.at[b])

        def run(b=b, value=value, save=save, job=job, span=span, opens=opens, closes=closes):
            if job[0] == "Y" and job[3] and job[1] not in par_seen:
                par_loads[job[1]].wait()
                par_seen.add(job[1])

            @pl.loop(0, hb // tile)
            def _(t):
                cols = pl.ds(pl.multiple_of(t * tile, tile), tile)
                v = value(cols).reshape((span.size,) + tmp.shape[2:4] + (tile,))
                tmp[b, span, :, :, cols] = v if opens else tmp[b, span, :, :, cols] + v

            if closes:
                save().start()

        sends = [mark(("C", n))]
        if closes:
            plan.msg(("W", n), ("s", n), 0)
            sends.append(("W", n))
            last_of[b] = n
            plan.task(2, [("W", n)], [mark(("S", n)), *[mark(key) for key in keys]], lambda save=save: save().wait(), COST["go"])
        plan.task(40, waits, sends, run, cost, stage=ks)

    order = plan.order()

    at = {}
    for n, i in enumerate(order):
        for w in plan.tasks[i][2]:
            at[w] = n
    uses = {p: [] for p in range(len(pools))}
    user = {}
    for n, i in enumerate(order):
        for k in plan.tasks[i][5]:
            uses[staged[k][0]].append(k)
            user[k] = n
    lbase, fill = 0, {}
    for p, ks in uses.items():
        depth = pools[p].shape[0]
        for n, k in enumerate(ks):
            box = pools[p].at[n % depth] if staged[k][3] is None else pools[p].at[n % depth, pl.ds(0, staged[k][3])]
            place[k] = (box, lsem.at[lbase + n % depth])
            when = -1 if n < depth else user[ks[n - depth]]
            for w in staged[k][2]:
                when = max(when, at[w])
            fill.setdefault(when, []).append(k)
        lbase += depth

    def load(k):
        return pltpu.make_async_copy(staged[k][1](), *place[k])

    for copy in lhs_loads[::-1]:
        copy.start()
    for k in fill.get(-1, ()):
        load(k).start()

    barrier = pltpu.get_barrier_semaphore()

    def tell(to):
        pl.semaphore_signal(barrier, inc=1, device_id=to, device_id_type=MESH)

    peers = [*[nb(axis, d) for axis in "zyx" for d in sgn], partner]
    for to in peers:
        tell(to)
    pl.when(x != y)(lambda: tell(across))
    run_tasks(plan, comm, order, lambda: pl.semaphore_wait(barrier, len(peers) + jnp.where(x != y, 1, 0)), load, fill)
    for copy in stores:
        copy.wait()


def reduce(dims, tok, grad, up, down, hid, dpre):
    nz, ny, nx = dims
    rows2, hh = tok.shape
    fc = hid.shape[1]
    tk, hb = rows2 // 2, hh // ny
    hr = hb // 2
    nu = fc // (nz * SUB)
    g = tk // (SUB * SUB)
    vm = pltpu.VMEM

    def per(shape):
        return [vm(shape(axis, n), F32) for _, axis, _, _, n, *_ in CHUNKS]

    def fin(shape):
        return [vm((n, SUB, hr if a == 0 else hb), F32) for a, _, _, _, n, *_ in CHUNKS]

    n0 = max(chunk[4] for chunk in CHUNKS)
    scratch = [
        *per(lambda axis, n: (nx - 1, n, nz, SUB, hb) if axis == "x" else (nx - 1, n, SUB, hb)),
        *per(lambda axis, n: (nz - 1, n, SUB, hb) if axis == "x" else (nz - 1, n, SUB, hh)),
        *fin(0),
        vm((2, nu, nz, SUB, hr), F32),
        vm((nu, nz, SUB, hb), F32),
        vm((2, 2, ny - 1, g // 2, SUB, SUB, hb), F32),
        vm((2, g, SUB, SUB, hb), BF16),
        vm((2, rows2, fc), BF16),
        vm((2, tk, fc), BF16),
        vm((2, g, SUB, SUB, hb), F32),
        vm((3, n0, nz, SUB, hb), F32),
        vm((6, n0, SUB, hh), F32),
        vm((2, g // 2, SUB, SUB, hb), F32),
        vm((3, rows2, hb), BF16),
        vm((3, hb, fc), BF16),
        pltpu.SemaphoreType.DMA((80,)),
        pltpu.SemaphoreType.DMA((330,)),
        pltpu.SemaphoreType.DMA((18,)),
        pltpu.SemaphoreType.DMA((24,)),
        pltpu.SemaphoreType.DMA((6,)),
        pltpu.SemaphoreType.DMA((2,)),
    ]
    sds = jax.ShapeDtypeStruct
    outs = pl.pallas_call(
        functools.partial(reduce_kernel, dims),
        out_shape=[
            sds((g, SUB, SUB, hb), BF16),
            sds((g, SUB, SUB, hb), BF16),
            sds((2, nu, nz, SUB, hr), F32),
            sds((nu, nz, SUB, hb), F32),
            sds((2, nu, nz, SUB, hh), F32),
            sds((2, g, SUB, SUB, hh), F32),
            sds(up.shape, BF16),
            sds(down.shape, BF16),
            sds((tk, fc), BF16),
            sds((tk, fc), BF16),
        ],
        in_specs=[ANY] * 6,
        out_specs=[ANY] * 10,
        scratch_shapes=scratch,
        compiler_params=pltpu.CompilerParams(collective_id=1, has_side_effects=True, vmem_limit_bytes=VMEM_LIMIT),
        name="reduce",
    )(tok, grad, up, down, hid, dpre)
    y, dx, g1, g2 = outs[:4]
    return finish(y.reshape(tk, hb), dx.reshape(tk, hb), g1.reshape(2 * fc, hr), g2.reshape(fc, hb))


def finish_kernel(*refs):
    *arrays, turned, isem, osem = refs
    n, parts = isem.shape
    ins, outs, boxes = (arrays[k * n:(k + 1) * n] for k in range(3))

    def span(ref, k):
        size = ref.shape[0] // parts
        return pl.ds(k * size, size)

    def fetch(i, k):
        return pltpu.make_async_copy(ins[i].at[span(ins[i], k)], boxes[i].at[span(ins[i], k)], isem.at[i, k])

    def put(i, k):
        if i == 0:
            cols = span(ins[i], k)
            return pltpu.make_async_copy(turned.at[:, cols], outs[i].at[:, cols], osem.at[i, k])
        return pltpu.make_async_copy(boxes[i].at[span(ins[i], k)], outs[i].at[span(ins[i], k)], osem.at[i, k])

    todo = list(itertools.product(range(n), range(parts)))
    for i, k in todo:
        fetch(i, k).start()
    for i, k in todo:
        fetch(i, k).wait()
        if i == 0:
            rows = span(ins[i], k)
            turned[:, rows] = boxes[i][rows, :].T
        put(i, k).start()
    for i, k in todo:
        put(i, k).wait()


def finish(y, dx, g1, g2):
    ins = (g1, g2, y, dx)
    turned = jax.ShapeDtypeStruct(g1.shape[::-1], F32)
    parts = 2
    out = pl.pallas_call(
        finish_kernel,
        out_shape=[turned, *[jax.ShapeDtypeStruct(v.shape, v.dtype) for v in ins[1:]]],
        in_specs=[ANY] * len(ins),
        out_specs=[ANY] * len(ins),
        scratch_shapes=[*[pltpu.VMEM(v.shape, v.dtype) for v in ins], pltpu.VMEM(turned.shape, F32), *[pltpu.SemaphoreType.DMA((len(ins), parts))] * 2],
        compiler_params=pltpu.CompilerParams(vmem_limit_bytes=VMEM_LIMIT),
        name="finish",
    )(*ins)
    return out[2], out[3], out[0], out[1]


def solution(mesh):
    act_spec = P(("depth", "row"), "col")
    weight_spec = P("row", "col")
    dims = (mesh.shape["depth"], mesh.shape["col"], mesh.shape["row"] // 2)

    def local_block(tok_blk, up_blk, down_blk, grad_blk):
        return reduce(dims, *gather(dims, tok_blk, grad_blk, up_blk, down_blk))

    return jax.shard_map(local_block, mesh=mesh, in_specs=(act_spec, weight_spec, weight_spec, act_spec), out_specs=(act_spec, act_spec, weight_spec, weight_spec), check_vma=False)
```

```python
import functools
import itertools
import string

import jax
import jax.numpy as jnp
from jax import lax
from jax.experimental import pallas as pl
from jax.experimental.pallas import tpu as pltpu
from jax.sharding import PartitionSpec as P

MESH = pl.DeviceIdType.MESH
ANY = pl.BlockSpec(memory_space=pl.ANY)
F32 = jnp.float32
SUB = 8
BF16 = jnp.bfloat16

TOP = (12, 10)
UNITS = 16
FAR_FIRST = (2, 1, 3, 0)
Y_ORDER = [(a, o) for a in range(2) for o in FAR_FIRST]
DIGITS = string.digits + string.ascii_letters
JOB_ORDER = "01tvus25ywo84xcz7r9dhA6e3qpajbkfBiElCFGDgmHn"
RANKS = "73l204k52619810ab"
SIDES = "10010100110010101"


def chunk_list():
    def run(a, axis, lo, hi, n=2):
        return [(a, axis, u, min(n, hi - u)) for u in range(lo, hi, n)]

    first, last = TOP
    parts = run(1, "z", last, UNITS) + run(0, "z", first, UNITS) + run(0, "x", 0, first) + run(1, "x", 0, last - 2) + run(1, "x", last - 2, last, 1)
    return [(a, axis, int(side), u, n, DIGITS.index(rank)) for (a, axis, u, n), side, rank in zip(parts, SIDES, RANKS)]


CHUNKS = chunk_list()


def job_list():
    def block(a, lo, hi):
        return [[("D", a, o, u, min(4, hi - u))] for u in range(lo, hi, 4) for o in FAR_FIRST]

    first, last = TOP
    jobs = block(0, 0, first) + block(1, 0, last) + block(0, first, UNITS) + block(1, last, UNITS) + [[("Y", a, o, h) for h in range(2)] for a, o in Y_ORDER]
    return [job for c in JOB_ORDER for job in jobs[DIGITS.index(c)]]


JOBS = job_list()
COST = {"D": (0.5, 0.15), "Y": 1.2, "fin": 0.1, "go": 0.03, "U": 4.0, "A": 0.8, "act": 3.0}
SLACK = 20.0
VMEM_LIMIT = 66_500_000


def gelu_fn(pre_act):
    return jax.nn.gelu(pre_act, approximate=True)


class Plan:
    def __init__(self, rates, window):
        self.rates, self.window = rates, window
        self.tasks, self.size, self.link = [], {}, {}

    def msg(self, key, link, nbytes):
        self.size[key], self.link[key] = nbytes, link

    def task(self, prio, waits, sends, run, cost=0.3, stage=(), raw=False):
        self.tasks.append((prio, tuple(waits), tuple(sends), run, cost, tuple(stage), raw))

    def order(self):
        free, arrive, out = {}, {}, []
        self.when, self.arrive = [], arrive
        now, left = 2.5, list(range(len(self.tasks)))
        while left:
            best = None
            for i in left:
                prio, waits, sends, _, _, _, raw = self.tasks[i]
                if any(w not in arrive for w in waits):
                    continue
                ready = max([arrive[w] for w in waits], default=0.0)
                if raw:
                    ready = max([ready] + [free.get(self.link[s], 0.0) - self.window for s in sends])
                key = (max(ready, now), prio, i)
                if best is None or key < best:
                    best = key
            at, _, i = best
            left.remove(i)
            out.append(i)
            now = at + self.tasks[i][4]
            self.when.append(now)
            for s in self.tasks[i][2]:
                rate, lat = self.rates[self.link[s][0]]
                took = self.size[s] / rate
                if self.link[s][0] in "to":
                    share = 0.5 if self.link[s][0] == "t" else 1.5
                    ways = [(axis, d) for axis in "xy" for d in (1, -1)]
                    done = max(now, *[free.get(way, 0.0) for way in ways]) + took
                    for way in ways:
                        free[way] = max(now, free.get(way, 0.0)) + took * share
                else:
                    done = max(now, free.get(self.link[s], 0.0)) + took
                    free[self.link[s]] = done
                arrive[s] = done + lat
        self.end = max(now, max(arrive.values()))
        return out


RATES = {axis: (45e3, 2.2) for axis in "xyz"}
RATES.update(d=(450e3, 3.0), t=(45e3, 5.0), o=(45e3, 7.0), l=(1e12, 0.0), s=(1e12, 2.0))
WINDOW = 9.0


class Comm:
    def __init__(self, plan, ssem, rsem):
        self.plan, self.ssem, self.rsem = plan, ssem, rsem
        self.make, self.meet, self.slot, self.remote_if, self.groups, self.grouped, self.flying = {}, {}, {}, {}, {}, set(), []

    def msg(self, key, link, src, dst, to, mail=None, group=None):
        i = len(self.slot)
        self.slot[key] = i
        there, here = mail or (i, i)
        name, ref = group or (key, None)
        g, _, _ = self.groups.setdefault(name, (len(self.groups), ref, to))
        if group:
            self.grouped.add(key)

        def make(r):
            return pltpu.make_async_remote_copy(
                src_ref=src(), dst_ref=dst(), send_sem=self.ssem.at[g], recv_sem=self.rsem.at[r], device_id=to, device_id_type=MESH)

        self.make[key] = lambda: make(there)
        self.meet[key] = lambda: make(here)
        shape = src().shape
        nbytes = functools.reduce(lambda a, b: a * b, shape, 1) * src().dtype.itemsize
        self.plan.msg(key, link, nbytes)

    def each(self, keys, make, act):
        for key in keys:
            if key in self.remote_if:
                pl.when(self.remote_if[key])(lambda key=key: act(make[key]()))
            elif key in make:
                act(make[key]())

    def start(self, *keys):
        self.flying.extend(key for key in keys if key not in self.grouped)
        self.each(keys, self.make, lambda copy: copy.start())

    def finish(self):
        self.sent(float("inf"))
        for g, ref, to in self.groups.values():
            if ref is not None:
                pltpu.make_async_remote_copy(src_ref=ref, dst_ref=ref, send_sem=self.ssem.at[g], recv_sem=self.rsem.at[g], device_id=to, device_id_type=MESH).wait_send()

    def wait(self, *keys):
        self.each(keys, self.meet, lambda copy: copy.wait_recv())

    def sent(self, before):
        keys = [key for key in self.flying if self.plan.arrive[key] <= before]
        self.flying = [key for key in self.flying if self.plan.arrive[key] > before]
        self.each(keys, self.make, lambda copy: copy.wait_send())


def run_tasks(plan, comm, order, ready, load=None, fill={}):
    heard = set()
    for n, i in enumerate(order):
        _, waits, sends, run, _, ks, _ = plan.tasks[i]
        if ready and any(key in comm.make for key in sends):
            ready()
            ready = None
        with jax.named_scope(f"w{n}"):
            comm.wait(*[w for w in waits if w not in heard])
            heard.update(waits)
        with jax.named_scope(f"l{n}"):
            for k in ks:
                load(k).wait()
        with jax.named_scope(f"r{n}"):
            run()
        for k in fill.get(n, ()):
            load(k).start()
        comm.sent(plan.when[n] - SLACK)
    comm.finish()


def where_am_i():
    z, y, r = lax.axis_index("depth"), lax.axis_index("col"), lax.axis_index("row")
    return z, y, lax.div(r, 2), lax.rem(r, 2)


def each(shape, fn):
    lead = shape[:-2]
    big = max(range(len(lead)), key=lambda d: lead[d])
    looped = lead[big] >= 8

    def rest(k):
        for ix in itertools.product(*[range(n) if not (looped and d == big) else (k,) for d, n in enumerate(lead)]):
            fn(ix)

    if looped:
        pl.loop(0, lead[big])(rest)
    else:
        rest(None)


def total(refs, ix):
    return functools.reduce(lambda a, b: a + b, [ref[ix] for ref in refs])


def accumulate(dst, others):
    def one(ix):
        dst[ix] = total([dst, *others], ix)

    each(dst.shape, one)


def mm(a, b):
    return jnp.dot(a, b, preferred_element_type=F32)


def mm_l(a, b):
    return lax.dot_general(a, b, (((0,), (0,)), ((), ())), preferred_element_type=F32)


def mm_t(a, b):
    return lax.dot_general(a, b, (((1,), (1,)), ((), ())), preferred_element_type=F32)


def gather_kernel(dims, x_ref, g_ref, w1_ref, w2_ref, xf, gf, w1f, w2f, hid, dpre,
                  bx, bg, bw1, bw2, vw2, u, da, ha, hd, ssem, rsem, lsem, osem, asem):
    nz, ny, nx = dims
    z, y, x, c = where_am_i()
    tk, hb = x_ref.shape
    fc = w2_ref.shape[0]
    hr, fz, half = hb // 2, fc // nz, tk // 2
    plan = Plan(RATES, WINDOW)
    comm = Comm(plan, ssem, rsem)
    ways = (1, -1)

    def idx(axis, d):
        at, n = {"z": (z, nz), "y": (y, ny), "x": (x, nx)}[axis]
        return lax.rem(at + (d % n), n)

    def nb(axis, d):
        i = idx(axis, d)
        return {"z": {"depth": i}, "y": {"col": i}, "x": {"row": 2 * i + c}}[axis]

    partner = {"row": 2 * x + (1 - c)}

    def at(i, size):
        return pl.ds(pl.multiple_of(i * size, size), size)

    def block(full, core, o, part=None):
        rows = at(core, tk) if part is None else pl.ds(pl.multiple_of(core * tk + part * half, half), half)
        return full.at[rows, at(idx("y", o), hb)]

    def wblock(o, core):
        return bw1.at[at(2 * idx("x", o) + core, hr), :]

    def piece(d, o):
        return bw2.at[at(idx("z", d), fz), at(idx("y", o), hb)]

    stores = []

    def store(src, dst):
        copy = pltpu.make_async_copy(src, dst, osem.at[len(stores)])
        stores.append(copy)
        copy.start()

    def mark(key):
        plan.msg(key, ("l", key), 0)
        return key

    loads = {}

    def load(name, src, dst):
        loads[name] = pltpu.make_async_copy(src, dst, lsem.at[len(loads)])
        plan.task(len(loads) / 10, [], [mark(name)], loads[name].wait, COST["go"])

    load("s", w2_ref.at[at(z, fz), :], vw2)
    load("w", w1_ref.at[:, at(c, fc)], wblock(0, c))
    load("x", x_ref, block(bx, c, 0))
    load("g", g_ref, block(bg, c, 0))
    self_copy = pltpu.make_async_copy(w2_ref.at[at(z, fz), :], piece(0, 0), lsem.at[len(loads)])

    def raw(prio, waits, keys):
        plan.task(prio, waits, keys, lambda: comm.start(*keys), COST["go"], raw=True)

    def passed(prio, wait, keys, key=None):
        plan.task(prio, [wait], [*keys, mark(("in", *wait) if key is None else key)], lambda: comm.start(*keys), COST["go"])

    for o in (1, -1, 2, 0):
        o = o % ny
        to = {"row": 2 * idx("x", o) + c, "col": x}
        comm.msg(("s", o), ("t", 0), lambda: vw2, lambda: piece(0, 0), to, mail=(y, idx("y", o)))
    comm.remote_if[("s", 0)] = x != y
    plan.task(1, ["s"], [("s", o) for o in range(ny)], lambda: comm.start(*[("s", o) for o in range(ny)]), COST["go"])
    whole = {d: [] for d in range(nz)}
    far = nz // 2
    for o in range(ny):
        for w in ways:
            steps = far if (w > 0) == (o % 2 == 0) else far - 1
            for t in range(steps):
                comm.msg(("z", o, w, t), ("z", w), lambda o=o, w=w, t=t: piece(-w * t, o), lambda o=o, w=w, t=t: piece(-w * t, o), nb("z", w))
                nxt = [("z", o, w, t + 1)] if t + 1 < steps else []
                key = ("w2", o, (-w * (t + 1)) % nz)
                passed(4, ("z", o, w, t), nxt, key)
                whole[key[2]].append(key)
        first = [("z", o, w, 0) for w in ways]

        def slice_in(o=o, first=first):
            if o == 0:
                pl.when(x == y)(self_copy.wait)
            comm.start(*first)

        plan.task(3, [("s", o)], [*first, mark(("w2", o, 0))], slice_in, COST["go"])
        whole[0].append(("w2", o, 0))

    comm.msg(("pw",), ("d", 0), lambda: w1_ref.at[:, at(1 - c, fc)], lambda: wblock(0, c), partner)
    raw(1.1, [], [("pw",)])
    w1_in = {0: ["w"], 1: [], -1: [], 2: []}
    for own in (True, False):
        core = c if own else 1 - c
        for w in ways:
            comm.msg(("wa", own, w), ("x", w), lambda core=core: wblock(0, core), lambda core=core: wblock(0, core), nb("x", w))
    raw(1.2, ["w"], [("wa", True, w) for w in ways])
    passed(5, ("pw",), [("wa", False, w) for w in ways])
    w1_in[0].append(("in", "pw"))
    for own, w in ((True, 1), (False, -1)):
        core = c if own else 1 - c
        comm.msg(("wf", w), ("x", w), lambda core=core, w=w: wblock(-w, core), lambda core=core, w=w: wblock(-w, core), nb("x", w))
        passed(6, ("wa", own, w), [("wf", w)])
        passed(6, ("wa", not own, w), [])
        passed(6, ("wf", w), [])
        w1_in[-w] += [("in", "wa", True, w), ("in", "wa", False, w)]
        w1_in[2].append(("in", "wf", w))

    arrived = {}
    for a, (full, name) in enumerate(((bx, "x"), (bg, "g"))):
        arrived[a] = [name]
        for w in ways:
            for p in range(2):
                comm.msg((name, w, p), ("y", w), lambda full=full, p=p: block(full, c, 0, p), lambda full=full, p=p: block(full, c, 0, p), nb("y", w))
            p = 0 if w > 0 else 1
            comm.msg((name, "f", w), ("y", w), lambda full=full, w=w, p=p: block(full, c, -w, p), lambda full=full, w=w, p=p: block(full, c, -w, p), nb("y", w))

        def share(key, o, p, full=full, name=name, a=a):
            comm.msg((name, "d", *key), ("d", 0), lambda: block(full, c, o, p), lambda: block(full, c, o, p), partner)
            passed(20, (name, "d", *key), [])
            arrived[a].append(("in", name, "d", *key))
            return (name, "d", *key)

        plan.task(2 + a, [name], [share((0,), 0, None)], lambda name=name: comm.start((name, "d", 0)), COST["go"])
        for w in ways:
            p = 0 if w > 0 else 1
            for q in range(2):
                keys = [share((-w, q), -w, q)] + ([(name, "f", w)] if q == p else [])
                passed(7, (name, w, q), keys)
                arrived[a].append(("in", name, w, q))
            passed(7, (name, "f", w), [share((2, p), 2, p)])
            arrived[a].append(("in", name, "f", w))
    for n, (name, late) in enumerate(itertools.product("gx", (False, True))):
        raw(1.3 + n / 100, [name], [(name, w, 1 if (w > 0) == late else 0) for w in ways])
    for name, here, src, dst in (("X", arrived[0], bx, xf), ("G", arrived[1], bg, gf), ("W2", [key for d in whole for key in whole[d]], bw2, w2f),
                                 ("W1", [key for o in w1_in for key in w1_in[o]], bw1, w1f)):
        plan.task(9, here, [mark(name)], functools.partial(store, src, dst), COST["go"])

    tile = 256

    e = lax.rem(y - x + ny, ny)
    early = lax.div(e, 2) * (3 - e), 1 + 2 * lax.div(e, 2)
    late = 2, 4 - early[0] - early[1]

    def up(ts, first):
        js = [lax.rem(x + t, nx) for t in ts]

        @pl.loop(0, fc // tile)
        def _(i):
            cols = at(i, tile)
            v = sum(mm(bx[:, at(j, hb)], bw1[at(j, hb), cols]) for j in js)
            u[:, cols] = v if first else u[:, cols] + v

    near = ["w", *[key for key in w1_in[0] + w1_in[1] + w1_in[-1]], *[key for key in arrived[0] if not (key[:3] == ("in", "x", "f") or key[:4] == ("in", "x", "d", 2))]]
    plan.task(30, near, [mark(("U", 0))], functools.partial(up, early, True), COST["U"])
    plan.task(30, [("U", 0), "X", "W1"], [mark(("U", 1))], functools.partial(up, late, False), COST["U"])

    def down(ds):
        spans = [at(idx("z", d), fz) for d in ds]

        @pl.loop(0, 2)
        def _(i):
            rows = at(i, tk)
            v = mm_t(bg[rows, :], jnp.concatenate([bw2[span, :] for span in spans]))
            for n, span in enumerate(spans):
                da[rows, span] = v[:, n * fz:(n + 1) * fz]

    for d in range(far + 1):
        ds = sorted({d, -d % nz})
        plan.task(31, ["G", *[key for e in ds for key in whole[e]]], [mark(("A", d))], functools.partial(down, ds), COST["A"] * len(ds) + 1)

    parts = tk // tile
    acts = [[pltpu.make_async_copy(src.at[at(h, tk), :], dst.at[at(h, tk), :], asem.at[h, n]) for n, (src, dst) in enumerate(((ha, hid), (hd, dpre)))] for h in range(2)]

    def act():
        for half, copies in enumerate(acts):
            @pl.loop(0, parts * (fc // fz))
            def _(i):
                rows, cols = at(half * parts + lax.rem(i, parts), tile), at(lax.div(i, parts), fz)
                h, vjp = jax.vjp(gelu_fn, u[rows, cols])
                ha[rows, cols] = h.astype(BF16)
                hd[rows, cols] = vjp(da[rows, cols])[0].astype(BF16)

            for copy in copies:
                copy.start()

    plan.task(32, [("U", 1), *[("A", d) for d in range(far + 1)]], [], act, COST["act"])

    order = plan.order()
    for copy in loads.values():
        copy.start()
    pl.when(x == y)(self_copy.start)

    barrier = pltpu.get_barrier_semaphore()

    def tell(to):
        pl.semaphore_signal(barrier, inc=1, device_id=to, device_id_type=MESH)

    for to in (*[nb(axis, d) for axis in "zyx" for d in ways], partner):
        tell(to)
    for o in range(1, ny):
        tell({"row": 2 * y + c, "col": idx("y", o)})
    pl.when(x != y)(lambda: tell({"row": 2 * y + c, "col": y}))
    run_tasks(plan, comm, order, lambda: pl.semaphore_wait(barrier, 6 + ny + jnp.where(x != y, 1, 0)))
    for copy in [*stores, *sum(acts, [])]:
        copy.wait()


def gather(dims, tok, grad, up, down):
    tk, hb = tok.shape
    fc = down.shape[0]
    nz, ny, nx = dims
    sds, vm = jax.ShapeDtypeStruct, pltpu.VMEM
    tokens, first, second, mid = (2 * tk, ny * hb), (nx * hb, fc), (fc, ny * hb), (2 * tk, fc)
    return pl.pallas_call(
        functools.partial(gather_kernel, dims),
        out_shape=[sds(shape, BF16) for shape in (tokens, tokens, first, second, mid, mid)],
        in_specs=[ANY] * 4,
        out_specs=[ANY] * 6,
        scratch_shapes=[
            *[vm(shape, BF16) for shape in (tokens, tokens, first, second, (fc // nz, hb))],
            vm(mid, F32),
            vm(mid, F32),
            vm(mid, BF16),
            vm(mid, BF16),
            pltpu.SemaphoreType.DMA((65,)),
            pltpu.SemaphoreType.DMA((65,)),
            pltpu.SemaphoreType.DMA((5,)),
            pltpu.SemaphoreType.DMA((9,)),
            pltpu.SemaphoreType.DMA((2, 2)),
        ],
        compiler_params=pltpu.CompilerParams(collective_id=0, has_side_effects=True, vmem_limit_bytes=VMEM_LIMIT),
        name="gather",
    )(tok, grad, up, down)


def reduce_kernel(dims, tok, grad, up, down, hid, dpre,
                  y_out, dx_out, g1_out, g2_out, dwp, yp, wx1, wx2, hx, dx, *scratch):
    nz, ny, nx = dims
    z, y, x, c = where_am_i()
    hb = y_out.shape[-1]
    tk = tok.shape[0] // 2
    hr = hb // 2
    fc = hid.shape[1]
    nu = fc // (nz * 8)
    sgn = (1, -1)
    scratch = list(scratch)

    def grab(n):
        return [scratch.pop(0) for _ in range(n)]

    nc = len(CHUNKS)
    xbuf, zbuf, tbuf = grab(nc), grab(nc), grab(nc)
    o1, o2, yr, yo, lhs, par, tmp = grab(7)
    pools = grab(5)
    ssem, rsem, lsem, osem, isem, tsem = grab(6)
    P_X, P_Z, P_Y, P_R, P_W = range(5)

    plan = Plan(RATES, WINDOW)
    comm = Comm(plan, ssem, rsem)

    def idx(axis, d):
        at, n = {"z": (z, nz), "y": (y, ny), "x": (x, nx)}[axis]
        return lax.rem(at + (d % n), n)

    def nb(axis, d):
        i = idx(axis, d)
        return {"z": {"depth": i}, "y": {"col": i}, "x": {"row": 2 * i + c}}[axis]

    partner = {"row": 2 * x + (1 - c)}
    across = {"row": 2 * y + c, "col": x}

    def hcol(j):
        return pl.ds(pl.multiple_of(j * hb, hb), hb)

    staged, stores, place = [], [], {}

    def stage(pool, src, marks=(), n=None):
        staged.append((pool, src, tuple(marks), n))
        return len(staged) - 1

    def slot(k):
        return place[k][0]

    def mark(key):
        plan.msg(key, ("l", key), 0)
        return key

    def chain(key, axis, n, s, buf, src, pool, marks, prio, end, end_sends, units=None):
        far, near = n // 2, n // 2 - 1
        for t in range(far):
            comm.msg((key, "F", t), (axis, s), (lambda: src(far * s)) if t == 0 else (lambda t=t: buf.at[t - 1]), lambda t=t: buf.at[t], nb(axis, s), group=(key, buf))
        for t in range(near):
            comm.msg((key, "N", t), (axis, -s), (lambda: src(-near * s)) if t == 0 else (lambda t=t: buf.at[far + t - 1]), lambda t=t: buf.at[far + t], nb(axis, -s), group=(key, buf))

        def own(rel):
            return [] if pool is None else [stage(pool, lambda: src(rel), marks(rel), units)]

        def mid(name, t, at, rel):
            ks = own(rel)

            def run():
                accumulate(buf.at[at], [slot(ks[0]) if ks else src(rel)])
                comm.start((key, name, t + 1))

            plan.task(prio, [(key, name, t), *marks(rel)], [(key, name, t + 1)], run, COST["go"], stage=ks)

        for t in range(far - 1):
            mid("F", t, t, (far - 1 - t) * s)
        for t in range(near - 1):
            mid("N", t, far + t, -(near - 1 - t) * s)
        ks = own(0)
        last = [buf.at[far - 1], buf.at[far + near - 1]]
        plan.task(prio, [(key, "F", far - 1), (key, "N", near - 1), *marks(0)], end_sends,
                  lambda: end(last, slot(ks[0]) if ks else src(0)), COST["fin"], stage=ks)
        return [(key, "F", 0), (key, "N", 0)]

    def raw(prio, marks, keys):
        plan.task(prio, marks, keys, lambda: comm.start(*keys), COST["go"], raw=True)

    def spread(key, s, region, finish, some):
        far, near = nz // 2, nz // 2 - 1
        for name, count, d in (("GF", far, s), ("GN", near, -s)):
            for t in range(count):
                def ref(t=t, d=d):
                    return region(idx("z", -t * d))
                comm.msg((key, name, t), ("z", d), ref, ref, nb("z", d), group=(key, some))
        for name, count in (("GF", far), ("GN", near)):
            for t in range(count - 1):
                plan.task(4, [(key, name, t)], [(key, name, t + 1)], lambda name=name, t=t: comm.start((key, name, t + 1)), COST["go"])
        plan.task(30, [(key, "GF", far - 1), (key, "GN", near - 1)], [], finish, COST["go"])
        return [(key, "GF", 0), (key, "GN", 0)]

    def store(src, dst):
        copy = pltpu.make_async_copy(src, dst, osem.at[len(stores)])
        stores.append(copy)
        copy.start()

    def none(rel):
        return ()

    for i, (a, first_axis, sigma, u, n, prio) in enumerate(CHUNKS):
        s = sgn[sigma]

        def done(o, a=a, u=u, n=n):
            return [("D", a, o % nx, v) for v in range(u, u + n)]

        if a == 0:
            def region(k, u=u, n=n):
                return o1.at[:, pl.ds(u, n), k]

            go = spread(("g", i), s, region, lambda u=u, n=n: store(o1.at[:, pl.ds(u, n)], g1_out.at[:, pl.ds(u, n)]), o1.at[:, pl.ds(0, n), pl.ds(0, nz - 1)])
            over = ("sw", i)
            comm.msg(over, ("d", 0), lambda i=i: tbuf[i], lambda u=u, n=n: o1.at[c, pl.ds(u, n), z], partner)

            def end(last, own, i=i, u=u, n=n, over=over):
                mine = pl.ds(pl.multiple_of(c * hr, hr), hr)
                other = pl.ds(pl.multiple_of((1 - c) * hr, hr), hr)
                for m in range(n):
                    tbuf[i][m] = total([own, *last], (m, slice(None), other))
                comm.start(over)
                for m in range(n):
                    o1[c, u + m, z] = total([own, *last], (m, slice(None), mine))
        else:
            def region(k, u=u, n=n):
                return o2.at[pl.ds(u, n), k]

            go = spread(("g", i), s, region, lambda u=u, n=n: store(o2.at[pl.ds(u, n)], g2_out.at[pl.ds(u, n)]), o2.at[pl.ds(0, n), pl.ds(0, nz - 1)])
            over = ("tr", i)
            comm.msg(over, ("o", 0), lambda i=i: tbuf[i], lambda region=region: region(z), across)
            comm.remote_if[over] = x != y

            def end(last, own, i=i, u=u, n=n, over=over):
                for m in range(n):
                    tbuf[i][m] = total([own, *last], m)
                comm.start(over)

                @pl.when(x == y)
                def _():
                    for m in range(n):
                        o2[u + m, z] = tbuf[i][m]

        plan.task(3, [over], go, lambda go=go: comm.start(*go), COST["go"])
        if first_axis == "x":
            res = xbuf[i].at[nx // 2 - 1]
            pieces = functools.partial(lambda res, rel: res.at[:, idx("z", rel)], res)
            raws = chain(("z", i), "z", nz, s, zbuf[i], pieces, None, none, 5, end, [over])

            def x_end(last, own, raws=raws):
                accumulate(last[0], [last[1], own])
                comm.start(*raws)

            raws = chain(("x", i), "x", nx, s, xbuf[i], lambda rel, a=a, u=u, n=n: dwp.at[a, pl.ds(u, n), :, :, hcol(idx("x", rel))],
                         P_X, lambda rel, done=done: done(rel), 10, x_end, raws, n)
            raw(11 + prio / 100, done(2) + done(-s), raws)
        else:
            res = zbuf[i].at[nz // 2 - 1]
            raws = chain(("x", i), "x", nx, s, xbuf[i], lambda rel, res=res: res.at[:, :, hcol(idx("x", rel))], None, none, 8, end, [over])

            def z_end(last, own, raws=raws):
                accumulate(last[0], [last[1], own])
                comm.start(*raws)

            all_done = [m for o in range(nx) for m in done(o)]
            raws = chain(("z", i), "z", nz, s, zbuf[i], lambda rel, a=a, u=u, n=n: dwp.at[a, pl.ds(u, n), idx("z", rel)],
                         P_Z, lambda rel, all_done=all_done: all_done, 9, z_end, raws, n)
            raw(11 + prio / 100, all_done, raws)

    groups = yo.shape[1]
    for a, out in enumerate((y_out, dx_out)):
        for sigma in range(2):
            s = sgn[sigma]
            half = pl.ds(sigma * (groups // 2), groups // 2)

            def y_end(last, own, a=a, half=half, sigma=sigma, out=out):
                def one(ix):
                    yo[(a, sigma * (groups // 2) + ix[0], ix[1])] = total([own, *last], ix).astype(BF16)

                each(own.shape, one)
                store(yo.at[a, half], out.at[half])

            raws = chain(("y", a, sigma), "y", ny, s, yr.at[a, sigma], lambda rel, a=a, half=half: yp.at[a, half, :, :, hcol(idx("y", rel))],
                         P_Y, lambda rel, a=a: [("Y", a, rel % ny)], 12, y_end, [])
            raw(11, [("Y", a, 2), ("Y", a, -s % ny)], raws)

    tile = 256

    def rows(o):
        return pl.ds(pl.multiple_of(idx("y", o) * hb, hb), hb)

    def arrive(key, prio=6):
        plan.msg(("got", *key), ("s", key), 0)
        plan.task(prio, [key], [("got", *key)], lambda: None, COST["go"])
        return ("got", *key)

    lhs_loads = [pltpu.make_async_copy(src, lhs.at[n], isem.at[n]) for n, src in enumerate((hid, dpre))]
    for n in (1, 0):
        plan.task(0, [], [mark(("T", n))], lhs_loads[n].wait, COST["fin"])

    others = pl.ds(pl.multiple_of((1 - c) * tk, tk), tk)
    own_rows = pl.ds(pl.multiple_of(c * tk, tk), tk)
    par_loads = []
    for n, (src, box) in enumerate(((hid, hx), (dpre, dx))):
        comm.msg(("hx", n), ("d", 0), lambda src=src: src.at[others], lambda box=box: box, partner)
        raw(1, [("C", 3)], [("hx", n)])
        par_loads.append(pltpu.make_async_copy(box, par.at[n], isem.at[2 + n]))
        plan.task(6, [("hx", n)], [mark(("P", n))], par_loads[n].start, COST["go"])
    for a, o in Y_ORDER:
        if a == 0:
            comm.msg(("w", a, o), ("d", 0), lambda o=o: down.at[:, hcol(idx("y", o))], lambda o=o: wx2.at[:, hcol(idx("y", o))], partner, group=("w2", wx2))
        else:
            comm.msg(("w", a, o), ("d", 0), lambda o=o: up.at[rows(o)], lambda o=o: wx1.at[rows(o)], partner, group=("w1", wx1))
        raw(2, [("C", 3)], [("w", a, o)])

    par_seen = set()
    last_of, b = {}, 1
    for n, job in enumerate(JOBS):
        opens, closes = job[0] == "D" or job[3] == 0, job[0] == "D" or job[3] == 1
        b = 1 - b if opens else b
        keys = [("Y", job[1], job[2])] if job[0] == "Y" else [("D", job[1], job[2] % nx, v) for v in range(job[3], job[3] + job[4])]
        span = pl.ds(0, yo.shape[1] if job[0] == "Y" else job[4])
        waits = [("C", n - 1)] if n else []
        if opens and b in last_of:
            waits.append(("S", last_of[b]))
        if job[0] == "D":
            _, a, o, u, n_u = job
            waits.append(("T", 1 - a))
            ks = [stage(P_R, lambda a=a, o=o: (tok, grad)[a].at[:, hcol(idx("x", o))])]

            def value(cols, a=a, u=u, n_u=n_u, ks=ks):
                return mm_l(lhs[1 - a, :, u * nz * 8:(u + n_u) * nz * 8], slot(ks[0])[:, cols])

            dst = functools.partial(lambda a, o, u, n_u: dwp.at[a, pl.ds(u, n_u), :, :, hcol(idx("x", o))], a, o, u, n_u)
            cost = COST["D"][0] + COST["D"][1] * n_u
        else:
            _, a, o, h = job
            waits.append(("T", a))
            marks = []
            if h:
                marks = [arrive(("w", a, o))]
                waits += [("P", a), *marks]
            if a == 0:
                ks = [stage(P_R, lambda o=o, w=(down, wx2)[h]: w.at[:, hcol(idx("y", o))], marks)]
            else:
                ks = [stage(P_W, lambda o=o, w=(up, wx1)[h]: w.at[rows(o)], marks)]

            def value(cols, a=a, h=h, ks=ks):
                left = par[a] if h else lhs[a, own_rows, :]
                return mm(left, slot(ks[0])[:, cols]) if a == 0 else mm_t(left, slot(ks[0])[cols, :])

            dst = functools.partial(lambda a, o: yp.at[a, :, :, :, hcol(idx("y", o))], a, o)
            cost = COST["Y"]

        def save(b=b, dst=dst, span=span):
            return pltpu.make_async_copy(tmp.at[b, span], dst(), tsem.at[b])

        def run(b=b, value=value, save=save, job=job, span=span, opens=opens, closes=closes):
            if job[0] == "Y" and job[3] and job[1] not in par_seen:
                par_loads[job[1]].wait()
                par_seen.add(job[1])

            @pl.loop(0, hb // tile)
            def _(t):
                cols = pl.ds(pl.multiple_of(t * tile, tile), tile)
                v = value(cols).reshape((span.size,) + tmp.shape[2:4] + (tile,))
                tmp[b, span, :, :, cols] = v if opens else tmp[b, span, :, :, cols] + v

            if closes:
                save().start()

        sends = [mark(("C", n))]
        if closes:
            plan.msg(("W", n), ("s", n), 0)
            sends.append(("W", n))
            last_of[b] = n
            plan.task(2, [("W", n)], [mark(("S", n)), *[mark(key) for key in keys]], lambda save=save: save().wait(), COST["go"])
        plan.task(40, waits, sends, run, cost, stage=ks)

    order = plan.order()

    at = {}
    for n, i in enumerate(order):
        for w in plan.tasks[i][2]:
            at[w] = n
    uses = {p: [] for p in range(len(pools))}
    user = {}
    for n, i in enumerate(order):
        for k in plan.tasks[i][5]:
            uses[staged[k][0]].append(k)
            user[k] = n
    lbase, fill = 0, {}
    for p, ks in uses.items():
        depth = pools[p].shape[0]
        for n, k in enumerate(ks):
            box = pools[p].at[n % depth] if staged[k][3] is None else pools[p].at[n % depth, pl.ds(0, staged[k][3])]
            place[k] = (box, lsem.at[lbase + n % depth])
            when = -1 if n < depth else user[ks[n - depth]]
            for w in staged[k][2]:
                when = max(when, at[w])
            fill.setdefault(when, []).append(k)
        lbase += depth

    def load(k):
        return pltpu.make_async_copy(staged[k][1](), *place[k])

    for copy in lhs_loads[::-1]:
        copy.start()
    for k in fill.get(-1, ()):
        load(k).start()

    barrier = pltpu.get_barrier_semaphore()

    def tell(to):
        pl.semaphore_signal(barrier, inc=1, device_id=to, device_id_type=MESH)

    peers = [*[nb(axis, d) for axis in "zyx" for d in sgn], partner]
    for to in peers:
        tell(to)
    pl.when(x != y)(lambda: tell(across))
    run_tasks(plan, comm, order, lambda: pl.semaphore_wait(barrier, len(peers) + jnp.where(x != y, 1, 0)), load, fill)
    for copy in stores:
        copy.wait()


def reduce(dims, tok, grad, up, down, hid, dpre):
    nz, ny, nx = dims
    rows2, hh = tok.shape
    fc = hid.shape[1]
    tk, hb = rows2 // 2, hh // ny
    hr = hb // 2
    nu = fc // (nz * SUB)
    g = tk // (SUB * SUB)
    vm = pltpu.VMEM

    def per(shape):
        return [vm(shape(axis, n), F32) for _, axis, _, _, n, *_ in CHUNKS]

    def fin(shape):
        return [vm((n, SUB, hr if a == 0 else hb), F32) for a, _, _, _, n, *_ in CHUNKS]

    n0 = max(chunk[4] for chunk in CHUNKS)
    scratch = [
        *per(lambda axis, n: (nx - 1, n, nz, SUB, hb) if axis == "x" else (nx - 1, n, SUB, hb)),
        *per(lambda axis, n: (nz - 1, n, SUB, hb) if axis == "x" else (nz - 1, n, SUB, hh)),
        *fin(0),
        vm((2, nu, nz, SUB, hr), F32),
        vm((nu, nz, SUB, hb), F32),
        vm((2, 2, ny - 1, g // 2, SUB, SUB, hb), F32),
        vm((2, g, SUB, SUB, hb), BF16),
        vm((2, rows2, fc), BF16),
        vm((2, tk, fc), BF16),
        vm((2, g, SUB, SUB, hb), F32),
        vm((3, n0, nz, SUB, hb), F32),
        vm((6, n0, SUB, hh), F32),
        vm((2, g // 2, SUB, SUB, hb), F32),
        vm((3, rows2, hb), BF16),
        vm((3, hb, fc), BF16),
        pltpu.SemaphoreType.DMA((80,)),
        pltpu.SemaphoreType.DMA((330,)),
        pltpu.SemaphoreType.DMA((18,)),
        pltpu.SemaphoreType.DMA((24,)),
        pltpu.SemaphoreType.DMA((6,)),
        pltpu.SemaphoreType.DMA((2,)),
    ]
    sds = jax.ShapeDtypeStruct
    outs = pl.pallas_call(
        functools.partial(reduce_kernel, dims),
        out_shape=[
            sds((g, SUB, SUB, hb), BF16),
            sds((g, SUB, SUB, hb), BF16),
            sds((2, nu, nz, SUB, hr), F32),
            sds((nu, nz, SUB, hb), F32),
            sds((2, nu, nz, SUB, hh), F32),
            sds((2, g, SUB, SUB, hh), F32),
            sds(up.shape, BF16),
            sds(down.shape, BF16),
            sds((tk, fc), BF16),
            sds((tk, fc), BF16),
        ],
        in_specs=[ANY] * 6,
        out_specs=[ANY] * 10,
        scratch_shapes=scratch,
        compiler_params=pltpu.CompilerParams(collective_id=1, has_side_effects=True, vmem_limit_bytes=VMEM_LIMIT),
        name="reduce",
    )(tok, grad, up, down, hid, dpre)
    y, dx, g1, g2 = outs[:4]
    return finish(y.reshape(tk, hb), dx.reshape(tk, hb), g1.reshape(2 * fc, hr), g2.reshape(fc, hb))


def finish_kernel(*refs):
    *arrays, turned, isem, osem = refs
    n, parts = isem.shape
    ins, outs, boxes = (arrays[k * n:(k + 1) * n] for k in range(3))

    def span(ref, k):
        size = ref.shape[0] // parts
        return pl.ds(k * size, size)

    def fetch(i, k):
        return pltpu.make_async_copy(ins[i].at[span(ins[i], k)], boxes[i].at[span(ins[i], k)], isem.at[i, k])

    def put(i, k):
        if i == 0:
            cols = span(ins[i], k)
            return pltpu.make_async_copy(turned.at[:, cols], outs[i].at[:, cols], osem.at[i, k])
        return pltpu.make_async_copy(boxes[i].at[span(ins[i], k)], outs[i].at[span(ins[i], k)], osem.at[i, k])

    todo = list(itertools.product(range(n), range(parts)))
    for i, k in todo:
        fetch(i, k).start()
    for i, k in todo:
        fetch(i, k).wait()
        if i == 0:
            rows = span(ins[i], k)
            turned[:, rows] = boxes[i][rows, :].T
        put(i, k).start()
    for i, k in todo:
        put(i, k).wait()


def finish(y, dx, g1, g2):
    ins = (g1, g2, y, dx)
    turned = jax.ShapeDtypeStruct(g1.shape[::-1], F32)
    parts = 2
    out = pl.pallas_call(
        finish_kernel,
        out_shape=[turned, *[jax.ShapeDtypeStruct(v.shape, v.dtype) for v in ins[1:]]],
        in_specs=[ANY] * len(ins),
        out_specs=[ANY] * len(ins),
        scratch_shapes=[*[pltpu.VMEM(v.shape, v.dtype) for v in ins], pltpu.VMEM(turned.shape, F32), *[pltpu.SemaphoreType.DMA((len(ins), parts))] * 2],
        compiler_params=pltpu.CompilerParams(vmem_limit_bytes=VMEM_LIMIT),
        name="finish",
    )(*ins)
    return out[2], out[3], out[0], out[1]


def solution(mesh):
    act_spec = P(("depth", "row"), "col")
    weight_spec = P("row", "col")
    dims = (mesh.shape["depth"], mesh.shape["col"], mesh.shape["row"] // 2)

    def local_block(tok_blk, up_blk, down_blk, grad_blk):
        return reduce(dims, *gather(dims, tok_blk, grad_blk, up_blk, down_blk))

    return jax.shard_map(local_block, mesh=mesh, in_specs=(act_spec, weight_spec, weight_spec, act_spec), out_specs=(act_spec, act_spec, weight_spec, weight_spec), check_vma=False)
```
